32 devices in a mesh: rep: 8 (over y, x, core), shard: 4 (over z).
Axes of the slice: x: 2, y: 2, z: 4, core: 2. Of those that a mesh axis runs over, the one named last changes fastest.
Arguments:
- tokens: bfloat16 [8192, 1024], P(('rep', 'shard')), may hold values from -6 to 6
- in_proj: bfloat16 [1024, 3072], P('shard'), may hold values from -0.1875 to 0.1875
- in_bias: bfloat16 [3072], P('shard'), may hold values from -3 to 3
- out_proj: bfloat16 [1024, 1024], P('shard'), may hold values from -1.5 to 1.5
- out_bias: bfloat16 [1024], P('shard'), may hold values from -3 to 3
- up_proj: bfloat16 [1024, 4096], P('shard'), may hold values from -0.1875 to 0.1875
- up_bias: bfloat16 [4096], P('shard'), may hold values from -3 to 3
- down_proj: bfloat16 [4096, 1024], P('shard'), may hold values from -0.09375 to 0.09375
- down_bias: bfloat16 [1024], P('shard'), may hold values from -3 to 3
- first_gain: bfloat16 [1024], P('shard'), may hold values from 0.5 to 1.5
- first_shift: bfloat16 [1024], P('shard'), may hold values from -3 to 3
- second_gain: bfloat16 [1024], P('shard'), may hold values from 0.5 to 1.5
- second_shift: bfloat16 [1024], P('shard'), may hold values from -3 to 3
- cotangent: bfloat16 [8192, 1024], P(('rep', 'shard')), may hold values from -6 to 6
Outputs:
- mixed: bfloat16 [8192, 1024], P(('rep', 'shard'))
- tokens_grad: float32 [8192, 1024], P(('rep', 'shard'))
- in_proj_grad: float32 [1024, 3072], P('shard')
- in_bias_grad: float32 [3072], P('shard')
- out_proj_grad: float32 [1024, 1024], P('shard')
- out_bias_grad: float32 [1024], P('shard')
- up_proj_grad: float32 [1024, 4096], P('shard')
- up_bias_grad: float32 [4096], P('shard')
- down_proj_grad: float32 [4096, 1024], P('shard')
- down_bias_grad: float32 [1024], P('shard')
- first_gain_grad: float32 [1024], P('shard')
- first_shift_grad: float32 [1024], P('shard')
- second_gain_grad: float32 [1024], P('shard')
- second_shift_grad: float32 [1024], P('shard')
The draws below stay inside these ranges and needn't reach their ends.
All inputs are finite; a program needn't handle non-finite values.
Results may differ from the reference program's by a relative error of at most 0.012.
Values may be sent and summed in bfloat16 or wider, within the bound.
A program may use at most 192 MiB of HBM per device.

```python
import jax
import jax.numpy as jnp
from jax import lax

D = 1024
FF = 4096
HEADS = 16
HEAD_DIM = 64
ROT = 16
LEN = 256
SEQS = 32
TOKENS = 8192


def with_spikes(drawn, stream_key, source, target, blocks, factor):
    owner, partner = [(jnp.arange(drawn.shape[position]) // (drawn.shape[position] // blocks)).reshape([-1 if axis == position else 1 for axis in range(drawn.ndim)]) for position in (source, target)]
    chosen = jax.random.permutation(stream_key, blocks)[partner]
    strong = (owner == chosen) | (owner == (partner + blocks // 2) % blocks)
    return jnp.where(strong, factor * drawn, drawn)


def block_scale(own_key, shape, pieces, least, largest):
    level, own = 1.0, jax.random.fold_in(own_key, 6)
    for dim, parts in pieces:
        draws = jnp.exp(jax.random.uniform(jax.random.fold_in(own, dim), (parts,), jnp.float32, least / len(pieces), largest / len(pieces)))
        level = level * jnp.repeat(draws, shape[dim] // parts).reshape([-1 if axis == dim else 1 for axis in range(len(shape))])
    return level


def scatter_about(stream_key, dims, deviation, most, split=(), held_as=jnp.bfloat16):
    entries = jax.random.normal(stream_key, dims, jnp.float32) * deviation
    if len(split) > 0:
        entries = block_scale(stream_key, dims, split, -0.22, 0.18) * entries
    return jnp.clip(entries, min=-most, max=most).astype(held_as)


def gaussian_with(key, dims, width, reach, shards, heavy, held_as=jnp.bfloat16):
    values = width * jax.random.normal(key, dims, jnp.float32)
    if shards:
        values = values * block_scale(key, dims, shards, -0.22, 0.18)
    return jnp.clip(with_spikes(values, jax.random.fold_in(key, 3), *heavy), -reach, reach).astype(held_as)


def setup_inputs(seed: int = 0) -> dict:
    streams_of = jax.random.split(jax.random.key(seed), 15)
    return {
        "tokens": gaussian_with(streams_of[0], (TOKENS, D), 1.0, 6.0, ((0, 32),), (0, 1, 32, 2.75)),
        "in_proj": scatter_about(streams_of[1], (D, 3 * D), D ** -0.5, 0.1875, ((0, 4),)),
        "in_bias": scatter_about(streams_of[2], (3 * D,), 0.5, 3.0, ((0, 4),)),
        "out_proj": scatter_about(streams_of[3], (D, D), (D // 64) ** -0.5, 1.5, ((0, 4),)),
        "out_bias": scatter_about(streams_of[4], (D,), 0.5, 3.0, ((0, 4),)),
        "up_proj": scatter_about(streams_of[5], (D, FF), D ** -0.5, 0.1875, ((0, 4),)),
        "up_bias": scatter_about(streams_of[6], (FF,), 0.5, 3.0, ((0, 4),)),
        "down_proj": scatter_about(streams_of[7], (FF, D), FF ** -0.5, 0.09375, ((0, 4),)),
        "down_bias": scatter_about(streams_of[8], (D,), 0.5, 3.0, ((0, 4),)),
        "first_gain": jnp.clip(1.0 + 0.1 * jax.random.normal(streams_of[9], (D,), jnp.float32), 0.5, 1.5).astype(jnp.bfloat16),
        "first_shift": scatter_about(streams_of[10], (D,), 0.5, 3.0, ((0, 4),)),
        "second_gain": jnp.clip(1.0 + 0.1 * jax.random.normal(streams_of[11], (D,), jnp.float32), 0.5, 1.5).astype(jnp.bfloat16),
        "second_shift": scatter_about(streams_of[12], (D,), 0.5, 3.0, ((0, 4),)),
        "cotangent": gaussian_with(streams_of[13], (TOKENS, D), 1.0, 6.0, ((0, 32),), (0, 1, 32, 2.75)),
    }


@jax.custom_vjp
def low(v):
    return lax.optimization_barrier(v.astype(jnp.bfloat16)).astype(jnp.float32)

@jax.custom_vjp
def low_back(v):
    return v

def low_keep(v):
    return (low(v), None)

def low_pass(kept, grad):
    return (grad,)

def back_keep(v):
    return (v, None)

def back_low(kept, grad):
    return (low(grad),)
low.defvjp(low_keep, low_pass)
low_back.defvjp(back_keep, back_low)
highest = lax.Precision.HIGHEST

def product(left, right):
    return jnp.dot(left, right, precision=highest, preferred_element_type=jnp.float32)

def layer_norm(values, gain, shift):
    average = lax.optimization_barrier(jnp.mean(values, axis=-1, keepdims=True))
    centred = values - average
    spread = lax.optimization_barrier(jnp.mean(centred * centred, axis=-1, keepdims=True))
    return centred * lax.rsqrt(spread + 1e-05) * gain + shift

def rotary_tables(length):
    half = ROT // 2
    inverse = jnp.exp(-jnp.log(10000.0) * (2.0 * jnp.arange(half, dtype=jnp.float32) / ROT))
    angles = jnp.arange(length, dtype=jnp.float32)[:, None] * inverse[None, :]
    return (jnp.cos(angles)[:, None, :], jnp.sin(angles)[:, None, :])

def rotate(values, cosine, sine):
    half = ROT // 2
    first = values[..., :half]
    second = values[..., half:ROT]
    return jnp.concatenate([first * cosine - second * sine, second * cosine + first * sine, values[..., ROT:]], axis=-1)

def one_sequence(block_inputs, in_proj, in_bias, out_proj, out_bias, up_proj, up_bias, down_proj, down_bias, first_gain, first_shift, second_gain, second_shift):
    length = block_inputs.shape[0]
    attn_in = low(layer_norm(block_inputs, first_gain, first_shift))
    mlp_in = low(layer_norm(block_inputs, second_gain, second_shift))
    qkv = low_back(product(attn_in, in_proj) + in_bias).reshape(length, 3, HEADS, HEAD_DIM)
    cosine, sine = rotary_tables(length)
    query = low(rotate(qkv[:, 0], cosine, sine))
    keys = low(rotate(qkv[:, 1], cosine, sine))
    values = low(qkv[:, 2])
    raw = jnp.einsum('qhd,khd->hqk', query, keys, precision=highest)
    scores = low_back(raw * HEAD_DIM ** (-0.5))
    causal = jnp.arange(length)[:, None] >= jnp.arange(length)[None, :]
    scores = jnp.where(causal[None], scores, -1e+30)
    expo = jnp.exp(scores)
    probs = low(expo / lax.optimization_barrier(jnp.sum(expo, axis=-1, keepdims=True)))
    attended = jnp.einsum('hqk,khd->qhd', probs, values, precision=highest).reshape(length, D)
    attended = low(low_back(attended))
    up = low_back(product(mlp_in, up_proj) + up_bias)
    activated = low(jax.nn.gelu(up, approximate=False))
    return block_inputs + product(attended, out_proj) + out_bias + product(activated, down_proj) + down_bias

def reference(tokens, in_proj, in_bias, out_proj, out_bias, up_proj, up_bias, down_proj, down_bias, first_gain, first_shift, second_gain, second_shift, cotangent):
    params = tuple((p.astype(jnp.float32) for p in (in_proj, in_bias, out_proj, out_bias, up_proj, up_bias, down_proj, down_bias, first_gain, first_shift, second_gain, second_shift)))
    sequences = tokens.astype(jnp.float32).reshape(SEQS, LEN, D)

    def forward(seqs, *weights):

        def single(seq):
            return one_sequence(seq, *weights)
        return lax.map(jax.checkpoint(single), seqs)
    outputs, pull = jax.vjp(forward, sequences, *params)
    grads = pull(cotangent.astype(jnp.float32).reshape(SEQS, LEN, D))
    mixed = outputs.reshape(TOKENS, D).astype(jnp.bfloat16)
    tokens_grad = grads[0].reshape(TOKENS, D)
    return (mixed, tokens_grad, grads[1], grads[2], grads[3], grads[4], grads[5], grads[6], grads[7], grads[8], grads[9], grads[10], grads[11], grads[12])
```

```python
import jax
import jax.numpy as jnp
from jax import lax
from jax.sharding import PartitionSpec as P

HEAD_DIM = 64
ROT = 16
EPS = 1e-05
MASKED = -1e30


def rotary_tables(length):
    half = ROT // 2
    inverse = jnp.exp(-jnp.log(10000.0) * (2.0 * jnp.arange(half, dtype=jnp.float32) / ROT))
    angles = jnp.arange(length, dtype=jnp.float32)[:, None] * inverse[None, :]
    return (jnp.cos(angles)[:, None, :], jnp.sin(angles)[:, None, :])


def rotate(values, cosine, sine, sign):
    half = ROT // 2
    first = values[..., :half]
    second = values[..., half:ROT]
    return jnp.concatenate(
        [
            first * cosine - sign * second * sine,
            second * cosine + sign * first * sine,
            values[..., ROT:],
        ],
        axis=-1,
    )


def mm(left, right, dims=((1,), (0,))):
    return lax.dot_general(left, right, (dims, ((), ())), preferred_element_type=jnp.float32)


def make_body(parts):
    def body(
        tokens,
        in_proj,
        in_bias,
        out_proj,
        out_bias,
        up_proj,
        up_bias,
        down_proj,
        down_bias,
        first_gain,
        first_shift,
        second_gain,
        second_shift,
        cotangent,
    ):
        length, width = tokens.shape
        me = lax.axis_index("shard")
        heads = width // parts // HEAD_DIM
        span = width // parts
        rows = in_proj.shape[0]
        hidden = up_bias.shape[0]
        scale = HEAD_DIM ** (-0.5)
        vectors = jnp.concatenate(
            [in_bias, out_bias, down_bias, first_gain, first_shift, second_gain, second_shift]
        )
        vectors = lax.all_gather(vectors, "shard", axis=0).astype(jnp.float32)
        cuts = [in_bias.shape[0]] + [span] * 6
        offsets = [sum(cuts[:i]) for i in range(len(cuts))]
        whole = [vectors[:, o : o + c].reshape(-1) for o, c in zip(offsets, cuts)]
        in_b, out_b, down_b, gain1, shift1, gain2, shift2 = whole
        both = lax.all_gather(jnp.stack([tokens, cotangent]), "shard", axis=1, tiled=True)
        x_all, g_all = both[0], both[1]
        w_in = lax.all_to_all(
            in_proj.reshape(rows, 3, parts, span), "shard", 2, 0, tiled=True
        ).reshape(parts * rows, 3 * span)
        w_up = lax.all_to_all(up_proj, "shard", 1, 0, tiled=True)
        b_in = lax.dynamic_slice_in_dim(in_b.reshape(3, parts, span), me, 1, axis=1).reshape(-1)
        x = x_all.astype(jnp.float32)
        mean = jnp.mean(x, axis=1, keepdims=True)
        cen = x - mean
        inv = lax.rsqrt(jnp.mean(cen * cen, axis=1, keepdims=True) + EPS)
        xhat = cen * inv
        attn_in = (xhat * gain1 + shift1).astype(jnp.bfloat16)
        mlp_in = (xhat * gain2 + shift2).astype(jnp.bfloat16)
        total_rows = x.shape[0]
        qkv = (mm(attn_in, w_in) + b_in).reshape(parts, length, 3, heads, HEAD_DIM)
        cosine, sine = rotary_tables(length)
        query = rotate(qkv[:, :, 0], cosine, sine, 1.0).astype(jnp.bfloat16)
        keys = rotate(qkv[:, :, 1], cosine, sine, 1.0).astype(jnp.bfloat16)
        values = qkv[:, :, 2].astype(jnp.bfloat16)
        causal = jnp.arange(length)[:, None] >= jnp.arange(length)[None, :]

        def ein(eq, a, b):
            return jnp.einsum(eq, a, b, preferred_element_type=jnp.float32)

        scores = jnp.where(causal, ein("sqhd,skhd->shqk", query, keys) * scale, MASKED)
        expo = jnp.exp(scores)
        probs_full = expo / jnp.sum(expo, axis=-1, keepdims=True)
        probs = probs_full.astype(jnp.bfloat16)
        attended = ein("shqk,skhd->sqhd", probs, values).astype(jnp.bfloat16)
        attended = attended.reshape(total_rows, span)
        up = mm(mlp_in, w_up) + up_bias.astype(jnp.float32)
        activated, pull = jax.vjp(lambda t: jax.nn.gelu(t, approximate=False), up)
        activated = activated.astype(jnp.bfloat16)
        partial = mm(attended, out_proj) + mm(activated, down_proj)
        branch = lax.psum_scatter(
            partial.astype(jnp.bfloat16), "shard", scatter_dimension=0, tiled=True
        )
        mixed = (tokens.astype(jnp.float32) + branch.astype(jnp.float32) + out_b + down_b).astype(
            jnp.bfloat16
        )
        grad_att = mm(g_all, out_proj, ((1,), (1,))).astype(jnp.bfloat16)
        grad_att = grad_att.reshape(parts, length, heads, HEAD_DIM)
        grad_act = mm(g_all, down_proj, ((1,), (1,)))
        grad_up = pull(grad_act)[0].astype(jnp.bfloat16)
        d_probs = ein("sqhd,skhd->shqk", grad_att, values)
        d_values = ein("shqk,sqhd->skhd", probs, grad_att)
        inner = jnp.sum(d_probs * probs_full, axis=-1, keepdims=True)
        d_scores = (probs_full * (d_probs - inner)).astype(jnp.bfloat16)
        d_query = ein("shqk,skhd->sqhd", d_scores, keys) * scale
        d_keys = ein("shqk,sqhd->skhd", d_scores, query) * scale
        d_query = rotate(d_query, cosine, sine, -1.0)
        d_keys = rotate(d_keys, cosine, sine, -1.0)
        grad_qkv = jnp.stack([d_query, d_keys, d_values], axis=2).astype(jnp.bfloat16)
        grad_qkv = grad_qkv.reshape(total_rows, 3 * span)
        d1 = mm(grad_qkv, w_in, ((1,), (1,)))
        d2 = mm(grad_up, w_up, ((1,), (1,)))
        scaled = (d1 * gain1 + d2 * gain2).astype(jnp.bfloat16)
        e = lax.psum_scatter(scaled, "shard", scatter_dimension=0, tiled=True).astype(jnp.float32)
        own = lambda a: lax.dynamic_slice_in_dim(a, me * length, length, axis=0)
        xh, rv = own(xhat), own(inv)
        tokens_grad = cotangent.astype(jnp.float32) + rv * (
            e - jnp.mean(e, axis=1, keepdims=True) - xh * jnp.mean(e * xh, axis=1, keepdims=True)
        )
        left = ((0,), (0,))
        dw_in = mm(attn_in, grad_qkv, left).astype(jnp.bfloat16)
        dw_up = mm(mlp_in, grad_up, left).astype(jnp.bfloat16)
        dw_out = mm(attended, g_all, left).astype(jnp.bfloat16)
        dw_down = mm(activated, g_all, left).astype(jnp.bfloat16)
        dw_in, dw_up, dw_out, dw_down = lax.psum((dw_in, dw_up, dw_out, dw_down), "rep")
        dw_in = lax.all_to_all(
            dw_in.reshape(parts * rows, 3, 1, span), "shard", 0, 2, tiled=True
        ).reshape(rows, 3 * width)
        dw_up = lax.all_to_all(dw_up, "shard", 0, 1, tiled=True)
        f32 = jnp.float32
        place = lambda v: lax.dynamic_update_slice_in_dim(
            jnp.zeros((3, parts, span), f32), v.reshape(3, 1, span), me, axis=1
        ).reshape(-1)
        vec = [
            place(jnp.sum(grad_qkv, axis=0, dtype=f32)),
            jnp.sum(cotangent.astype(f32), axis=0),
            jnp.sum(d1 * xhat, axis=0),
            jnp.sum(d1, axis=0),
            jnp.sum(d2 * xhat, axis=0),
            jnp.sum(d2, axis=0),
        ]
        vec = jnp.concatenate([v.reshape(parts, -1) for v in vec], axis=1)
        vec = lax.psum_scatter(vec, "shard", scatter_dimension=0, tiled=True)[0]
        vec, up_vec = lax.psum((vec, jnp.sum(grad_up, axis=0, dtype=f32)), "rep")
        o = in_bias.shape[0]
        bias_grad = vec[o : o + span]
        rest = [vec[o + span * i : o + span * (i + 1)] for i in range(1, 5)]
        return (
            mixed,
            tokens_grad,
            dw_in.astype(f32),
            vec[:o],
            dw_out.astype(f32),
            bias_grad,
            dw_up.astype(f32),
            up_vec,
            dw_down.astype(f32),
            bias_grad,
            *rest,
        )

    return body


def solution(mesh):
    rows = P(("rep", "shard"), None)
    mat = P("shard", None)
    vec = P("shard")
    in_specs = (rows, mat, vec, mat, vec, mat, vec, mat, vec, vec, vec, vec, vec, rows)
    out_specs = (rows, rows, mat, vec, mat, vec, mat, vec, mat, vec, vec, vec, vec, vec)
    return jax.shard_map(
        make_body(mesh.shape["shard"]),
        mesh=mesh,
        in_specs=in_specs,
        out_specs=out_specs,
        check_vma=False,
    )
```

```python
import functools

import jax
import jax.numpy as jnp
import numpy as np
from jax import lax
from jax.experimental import pallas as pl
from jax.experimental.pallas import tpu as pltpu
from jax.sharding import PartitionSpec as P

HEAD_DIM = 64
ROT = 16
EPS = 1e-05
MASKED = -1e30


def rotary_tables(length):
    half = ROT // 2
    inverse = jnp.exp(-jnp.log(10000.0) * (2.0 * jnp.arange(half, dtype=jnp.float32) / ROT))
    angles = jnp.arange(length, dtype=jnp.float32)[:, None] * inverse[None, :]
    return (jnp.cos(angles)[:, None, :], jnp.sin(angles)[:, None, :])


def rotate(values, cosine, sine, sign):
    half = ROT // 2
    first = values[..., :half]
    second = values[..., half:ROT]
    return jnp.concatenate(
        [
            first * cosine - sign * second * sine,
            second * cosine + sign * first * sine,
            values[..., ROT:],
        ],
        axis=-1,
    )


def mm(left, right, dims=((1,), (0,))):
    return lax.dot_general(left, right, (dims, ((), ())), preferred_element_type=jnp.float32)


def make_body(parts):
    def body(
        tokens,
        in_proj,
        in_bias,
        out_proj,
        out_bias,
        up_proj,
        up_bias,
        down_proj,
        down_bias,
        first_gain,
        first_shift,
        second_gain,
        second_shift,
        cotangent,
    ):
        length, width = tokens.shape
        me = lax.axis_index("shard")
        heads = width // parts // HEAD_DIM
        span = width // parts
        rows = in_proj.shape[0]
        hidden = up_bias.shape[0]
        scale = HEAD_DIM ** (-0.5)
        vectors = jnp.concatenate(
            [in_bias, out_bias, down_bias, first_gain, first_shift, second_gain, second_shift]
        )
        vectors = lax.all_gather(vectors, "shard", axis=0).astype(jnp.float32)
        cuts = [in_bias.shape[0]] + [span] * 6
        offsets = [sum(cuts[:i]) for i in range(len(cuts))]
        whole = [vectors[:, o : o + c].reshape(-1) for o, c in zip(offsets, cuts)]
        in_b, out_b, down_b, gain1, shift1, gain2, shift2 = whole
        both = lax.all_gather(jnp.stack([tokens, cotangent]), "shard", axis=1, tiled=True)
        x_all, g_all = both[0], both[1]
        w_in = lax.all_to_all(
            in_proj.reshape(rows, 3, parts, span), "shard", 2, 0, tiled=True
        ).reshape(parts * rows, 3 * span)
        w_up = lax.all_to_all(up_proj, "shard", 1, 0, tiled=True)
        b_in = lax.dynamic_slice_in_dim(in_b.reshape(3, parts, span), me, 1, axis=1).reshape(-1)
        x = x_all.astype(jnp.float32)
        mean = jnp.mean(x, axis=1, keepdims=True)
        cen = x - mean
        inv = lax.rsqrt(jnp.mean(cen * cen, axis=1, keepdims=True) + EPS)
        xhat = cen * inv
        attn_in = (xhat * gain1 + shift1).astype(jnp.bfloat16)
        mlp_in = (xhat * gain2 + shift2).astype(jnp.bfloat16)
        total_rows = x.shape[0]
        qkv = (mm(attn_in, w_in) + b_in).reshape(parts, length, 3, heads, HEAD_DIM)
        cosine, sine = rotary_tables(length)
        query = rotate(qkv[:, :, 0], cosine, sine, 1.0).astype(jnp.bfloat16)
        keys = rotate(qkv[:, :, 1], cosine, sine, 1.0).astype(jnp.bfloat16)
        values = qkv[:, :, 2].astype(jnp.bfloat16)
        causal = jnp.arange(length)[:, None] >= jnp.arange(length)[None, :]

        def ein(eq, a, b):
            return jnp.einsum(eq, a, b, preferred_element_type=jnp.float32)

        scores = jnp.where(causal, ein("sqhd,skhd->shqk", query, keys) * scale, MASKED)
        expo = jnp.exp(scores)
        probs_full = expo / jnp.sum(expo, axis=-1, keepdims=True)
        probs = probs_full.astype(jnp.bfloat16)
        attended = ein("shqk,skhd->sqhd", probs, values).astype(jnp.bfloat16)
        attended = attended.reshape(total_rows, span)
        up = mm(mlp_in, w_up) + up_bias.astype(jnp.float32)
        activated, pull = jax.vjp(lambda t: jax.nn.gelu(t, approximate=False), up)
        activated = activated.astype(jnp.bfloat16)
        partial = mm(attended, out_proj) + mm(activated, down_proj)
        branch = lax.psum_scatter(
            partial.astype(jnp.bfloat16), "shard", scatter_dimension=0, tiled=True
        )
        mixed = (tokens.astype(jnp.float32) + branch.astype(jnp.float32) + out_b + down_b).astype(
            jnp.bfloat16
        )
        grad_att = mm(g_all, out_proj, ((1,), (1,))).astype(jnp.bfloat16)
        grad_att = grad_att.reshape(parts, length, heads, HEAD_DIM)
        grad_act = mm(g_all, down_proj, ((1,), (1,)))
        grad_up = pull(grad_act)[0].astype(jnp.bfloat16)
        d_probs = ein("sqhd,skhd->shqk", grad_att, values)
        d_values = ein("shqk,sqhd->skhd", probs, grad_att)
        inner = jnp.sum(d_probs * probs_full, axis=-1, keepdims=True)
        d_scores = (probs_full * (d_probs - inner)).astype(jnp.bfloat16)
        d_query = ein("shqk,skhd->sqhd", d_scores, keys) * scale
        d_keys = ein("shqk,sqhd->skhd", d_scores, query) * scale
        d_query = rotate(d_query, cosine, sine, -1.0)
        d_keys = rotate(d_keys, cosine, sine, -1.0)
        grad_qkv = jnp.stack([d_query, d_keys, d_values], axis=2).astype(jnp.bfloat16)
        grad_qkv = grad_qkv.reshape(total_rows, 3 * span)
        d1 = mm(grad_qkv, w_in, ((1,), (1,)))
        d2 = mm(grad_up, w_up, ((1,), (1,)))
        scaled = (d1 * gain1 + d2 * gain2).astype(jnp.bfloat16)
        e = lax.psum_scatter(scaled, "shard", scatter_dimension=0, tiled=True).astype(jnp.float32)
        own = lambda a: lax.dynamic_slice_in_dim(a, me * length, length, axis=0)
        xh, rv = own(xhat), own(inv)
        tokens_grad = cotangent.astype(jnp.float32) + rv * (
            e - jnp.mean(e, axis=1, keepdims=True) - xh * jnp.mean(e * xh, axis=1, keepdims=True)
        )
        left = ((0,), (0,))
        dw_in = mm(attn_in, grad_qkv, left).astype(jnp.bfloat16)
        dw_up = mm(mlp_in, grad_up, left).astype(jnp.bfloat16)
        dw_out = mm(attended, g_all, left).astype(jnp.bfloat16)
        dw_down = mm(activated, g_all, left).astype(jnp.bfloat16)
        dw_in, dw_up, dw_out, dw_down = lax.psum((dw_in, dw_up, dw_out, dw_down), "rep")
        dw_in = lax.all_to_all(
            dw_in.reshape(parts * rows, 3, 1, span), "shard", 0, 2, tiled=True
        ).reshape(rows, 3 * width)
        dw_up = lax.all_to_all(dw_up, "shard", 0, 1, tiled=True)
        f32 = jnp.float32
        place = lambda v: lax.dynamic_update_slice_in_dim(
            jnp.zeros((3, parts, span), f32), v.reshape(3, 1, span), me, axis=1
        ).reshape(-1)
        vec = [
            place(jnp.sum(grad_qkv, axis=0, dtype=f32)),
            jnp.sum(cotangent.astype(f32), axis=0),
            jnp.sum(d1 * xhat, axis=0),
            jnp.sum(d1, axis=0),
            jnp.sum(d2 * xhat, axis=0),
            jnp.sum(d2, axis=0),
        ]
        vec = jnp.concatenate([v.reshape(parts, -1) for v in vec], axis=1)
        vec = lax.psum_scatter(vec, "shard", scatter_dimension=0, tiled=True)[0]
        vec, up_vec = lax.psum((vec, jnp.sum(grad_up, axis=0, dtype=f32)), "rep")
        o = in_bias.shape[0]
        bias_grad = vec[o : o + span]
        rest = [vec[o + span * i : o + span * (i + 1)] for i in range(1, 5)]
        return (
            mixed,
            tokens_grad,
            dw_in.astype(f32),
            vec[:o],
            dw_out.astype(f32),
            bias_grad,
            dw_up.astype(f32),
            up_vec,
            dw_down.astype(f32),
            bias_grad,
            *rest,
        )

    return body


BF = jnp.bfloat16
F32 = jnp.float32
MESH = pl.DeviceIdType.MESH
VMEM_LIMIT = 67_000_000
NN = ((1,), (0,))
NT = ((1,), (1,))
TN = ((0,), (0,))


class Sizes:
    def __init__(self, mesh_shape, length, width, hidden):
        self.copies = mesh_shape["rep"]
        self.n = self.copies // 2
        self.s = mesh_shape["shard"]
        self.l = length
        self.d = width
        self.ff = hidden
        self.span = width // self.n
        self.hid = hidden // self.n
        self.rs = width // self.s
        self.hb = hidden // self.s // self.n
        self.rows = self.n * length

    def fits(self):
        return (
            self.copies % 2 == 0
            and self.n == self.s
            and self.span % 256 == 0
            and self.hb % 256 == 0
            and self.rs == 256
            and self.span == 256
            and self.hb == 256
        )


def rotary_lanes(length):
    half = ROT // 2
    inverse = np.exp(-np.log(10000.0) * (2.0 * np.arange(half) / ROT))
    angles = np.arange(length)[:, None] * inverse[None, :]
    cosine, sine = np.cos(angles), np.sin(angles)
    table = np.zeros((3, length, 128), np.float32)
    table[0] = 1.0
    for start in (0, HEAD_DIM):
        table[0, :, start : start + half] = cosine
        table[0, :, start + half : start + ROT] = cosine
        table[1, :, start : start + half] = -sine
        table[2, :, start + half : start + ROT] = sine
    return table


def dot(left, right, dims=NN):
    return lax.dot_general(left, right, (dims, ((), ())), preferred_element_type=F32)


def fused(z, *refs):
    (tok, cot, inp, upp, outp, downp, vec, rot) = refs[:8]
    (mixed_o, tgrad_o, gin_o, gup_o, gdown_o, gout_o, vec_o) = refs[8:15]
    (
        x_all, g_all, a1, a2, w1, wo, wd, qkv, pt, der, act, att, gatt, gup, gqkv,
        msend, mrecv, mown, esend, erecv, eown,
        dwi, dwu, dwd, dwo, xri, xru, xrd, xro, zri, zru, zrd, zro, fi, fu, fd, fo,
        va, inb, vfull, vz, vu, vr, mean_r, inv_r, vacc, bin_r, bup_r,
        loc, v_s, v_r, x_s, x_r, g_s, g_r, w_s, w_r, wc_s, wc_r, d_s, d_r, dc_s, dc_r,
        o_s, o_r, oc_s, oc_r, m_s, m_r, e_s, e_r, xs_s, xs_r, zs_s, zs_r,
        agx_s, agx_r, agc_s, agc_r, agl, v1_s, v1_r, v2_s, v2_r,
    ) = refs[15:]
    n, s_n, length, width = z.n, z.s, z.l, z.d
    span, hid, rs, hb = z.span, z.hid, z.rs, z.hb
    iw = 3 * span
    heads = span // HEAD_DIM
    scale = HEAD_DIM**-0.5
    r = lax.axis_index("rep")
    zz = lax.axis_index("shard")
    p = lax.div(r, 2)
    c = lax.rem(r, 2)
    other = 1 - c
    partner = (2 * p + other, zz)

    def rc(src, dst, ss, rr, dev):
        return pltpu.make_async_remote_copy(
            src_ref=src, dst_ref=dst, send_sem=ss, recv_sem=rr, device_id=dev, device_id_type=MESH
        )

    def mo(value, m):
        return pl.multiple_of(value, m)

    def seq(ref, s):
        return ref.at[pl.ds(mo(s * length, length), length)]

    sends = []

    def start(copy, cond=None):
        if cond is None:
            copy.start()
        else:
            pl.when(cond)(copy.start)
        sends.append((cond, copy))

    own_rows = pl.ds(mo(zz * rs, rs), rs)
    own_hb = pl.ds(mo(zz * hb, hb), hb)
    locals_w = []
    for i in range(3):
        locals_w.append(
            pltpu.make_async_copy(
                inp.at[:, pl.ds(mo(i * width + p * span, span), span)],
                w1.at[own_rows, pl.ds(i * span, span)],
                loc.at[i],
            )
        )
    for i in range(s_n):
        locals_w.append(
            pltpu.make_async_copy(
                upp.at[:, pl.ds(mo(i * (hb * n) + p * hb, hb), hb)],
                w1.at[own_rows, pl.ds(iw + i * hb, hb)],
                loc.at[3 + i],
            )
        )
    local_d = pltpu.make_async_copy(
        downp.at[pl.ds(mo(p * hb, hb), hb)], wd.at[own_hb], loc.at[3 + s_n]
    )
    local_x = pltpu.make_async_copy(tok, seq(x_all, p), loc.at[4 + s_n])
    local_g = pltpu.make_async_copy(cot, seq(g_all, p), loc.at[5 + s_n])
    local_v = pltpu.make_async_copy(vec, va.at[zz], loc.at[6 + s_n])
    local_o = pltpu.make_async_copy(outp, wo, loc.at[7 + s_n])
    for cp in [local_v, local_x] + locals_w + [local_g, local_d]:
        cp.start()
    pl.when(zz == p)(local_o.start)

    barrier = pltpu.get_barrier_semaphore()
    for i in range(1, 2 * n):
        pl.semaphore_signal(
            barrier, 1, device_id=(lax.rem(r + i, 2 * n), zz), device_id_type=MESH
        )
    for i in range(1, s_n):
        pl.semaphore_signal(barrier, 1, device_id=(r, lax.rem(zz + i, s_n)), device_id_type=MESH)
    pl.semaphore_wait(barrier, 2 * n - 1 + s_n - 1)

    def plane(i):
        q = lax.rem(p + i, n)
        return q, (2 * q + c, zz)

    def line(i):
        q = lax.rem(zz + i, s_n)
        return q, (r, q)

    left, right = (r, zz - 1), (r, zz + 1)
    has_left, has_right = zz > 0, zz < s_n - 1

    for i in range(1, s_n):
        q, dev = line(i)
        start(rc(vec, va.at[zz], v_s.at[i], v_r.at[zz], dev))
    for i in range(1, n):
        q, dev = plane(i)
        start(rc(tok, seq(x_all, p), x_s.at[i], x_r.at[p], dev))
    half = rs // 2

    def w_piece(q):
        return w1.at[pl.ds(mo(q * rs + c * half, half), half)]

    def w_other(q):
        return w1.at[pl.ds(mo(q * rs + other * half, half), half)]

    for cp in locals_w:
        cp.wait()
    start(rc(w_piece(zz), w_piece(zz), w_s.at[0], w_r.at[zz], left), has_left)
    start(rc(w_piece(zz), w_piece(zz), w_s.at[1], w_r.at[zz], right), has_right)
    for i in range(1, n):
        q, dev = plane(i)
        start(rc(cot, seq(g_all, p), g_s.at[i], g_r.at[p], dev))

    def relay(piece, ss, rr, cs, cr, d):
        def take(q, has, onward, more, slot):
            @pl.when(has)
            def _():
                rc(piece(q), piece(q), ss.at[slot], rr.at[q], partner).wait_recv()

            start(
                rc(piece(q), piece(q), ss.at[slot], rr.at[q], onward),
                jnp.logical_and(has, more),
            )
            start(rc(piece(q), piece(q), cs.at[slot], cr.at[q], partner), has)

        take(zz - d, zz - d >= 0, right, has_right, 2 * d)
        take(zz + d, zz + d <= s_n - 1, left, has_left, 2 * d + 1)

    def relay_done(piece_other, cs, cr):
        for i in range(1, s_n):
            q, _ = line(i)
            rc(piece_other(q), piece_other(q), cs.at[0], cr.at[q], partner).wait_recv()

    local_v.wait()
    for i in range(1, s_n):
        q, dev = line(i)
        rc(vec, va.at[q], v_s.at[i], v_r.at[q], dev).wait_recv()
    n_in = 3 * width // s_n
    n_up = hb * n
    at_up = n_in
    at_rest = n_in + n_up

    def vector(i):
        off = at_rest + i * rs
        return jnp.concatenate([va[q, :, off : off + rs] for q in range(s_n)], axis=1)

    out_b, down_b, gain1, shift1, gain2, shift2 = [vector(i) for i in range(6)]
    for q in range(s_n):
        inb[:, q * n_in : (q + 1) * n_in] = va[q, :, :n_in]

    def norm(s):
        step = 32

        def body(i, carry):
            row = pl.ds(mo(s * length + i * step, step), step)
            xv = x_all[row, :].astype(F32)
            mu = jnp.mean(xv, axis=1, keepdims=True)
            cen = xv - mu
            inv = lax.rsqrt(jnp.mean(cen * cen, axis=1, keepdims=True) + EPS)
            xh = cen * inv
            a1[row, :] = (xh * gain1 + shift1).astype(BF)
            a2[row, :] = (xh * gain2 + shift2).astype(BF)
            mean_r[row, :] = mu
            inv_r[row, :] = inv
            return carry

        lax.fori_loop(0, length // step, body, 0)

    local_x.wait()
    norm(p)
    relay(w_piece, w_s, w_r, wc_s, wc_r, 1)
    for d in range(2, s_n):
        if d == s_n - 1:
            for i in range(1, n):
                q, dev = plane(i)
                rc(tok, seq(x_all, q), x_s.at[i], x_r.at[q], dev).wait_recv()
                norm(q)
        relay(w_piece, w_s, w_r, wc_s, wc_r, d)

    hhalf = hb // 2

    def d_piece(q):
        return wd.at[pl.ds(mo(q * hb + c * hhalf, hhalf), hhalf)]

    def d_other(q):
        return wd.at[pl.ds(mo(q * hb + other * hhalf, hhalf), hhalf)]

    ohalf = span // 2
    o_piece = wo.at[pl.ds(mo(c * ohalf, ohalf), ohalf)]
    o_other = wo.at[pl.ds(mo(other * ohalf, ohalf), ohalf)]
    local_d.wait()
    pl.when(zz == p)(local_o.wait)
    start(rc(d_piece(zz), d_piece(zz), d_s.at[0], d_r.at[zz], left), has_left)
    start(rc(d_piece(zz), d_piece(zz), d_s.at[1], d_r.at[zz], right), has_right)
    at_home = zz == p
    start(rc(o_piece, o_piece, o_s.at[0], o_r.at[0], left), jnp.logical_and(at_home, has_left))
    start(rc(o_piece, o_piece, o_s.at[1], o_r.at[0], right), jnp.logical_and(at_home, has_right))
    relay_done(w_other, wc_s, wc_r)

    def up_block(s):
        row = pl.ds(mo(s * length, length), length)
        left_a = a2[row, :]
        for j in range(s_n):
            col = pl.ds(j * hb, hb)
            bias = va[j, :, pl.ds(mo(at_up + p * hb, hb), hb)]
            u = dot(left_a, w1[:, iw + j * hb : iw + (j + 1) * hb]) + bias
            phi = 0.5 * (1.0 + lax.erf(u * 0.7071067811865476))
            act[row, col] = (u * phi).astype(BF)
            der[row, col] = phi + u * (0.3989422804014327 * jnp.exp(-0.5 * u * u))

    lax.fori_loop(0, n, lambda s, _: (up_block(s), 0)[1], 0)
    relay(d_piece, d_s, d_r, dc_s, dc_r, 1)

    def exchange(t, dw, xr, block_half):
        src = dw.at[:, pl.ds(mo(other * block_half, block_half), block_half)]
        start(rc(src, xr, xs_s.at[t], xs_r.at[t], partner))

    def pair_sum(t, dw, xr, zr, block_half, blocks):
        mine = pl.ds(mo(c * block_half, block_half), block_half)
        src = dw.at[:, mine]
        rc(src, xr, xs_s.at[t], xs_r.at[t], partner).wait_recv()

        def body(q, carry):
            xr[q] = (dw[q, mine].astype(F32) + xr[q].astype(F32)).astype(BF)
            return carry

        lax.fori_loop(0, blocks, body, 0)
        for i in range(1, s_n):
            q, dev = line(i)
            start(rc(xr.at[q], zr.at[zz], zs_s.at[t, i], zs_r.at[t, zz], dev))

    def line_sum(t, xr, zr, fin):
        total = xr[zz].astype(F32)
        for i in range(1, s_n):
            q, dev = line(i)
            rc(xr.at[q], zr.at[q], zs_s.at[t, i], zs_r.at[t, q], dev).wait_recv()
            total = total + zr[q].astype(F32)
        fin[...] = total.astype(BF)

    def areas(t, q, core):
        if t == 0:
            row = pl.ds(mo(core * half, half), half)
            return [
                (k, gin_o.at[row, pl.ds(mo(k * width + q * span, span), span)], fi.at[:, pl.ds(k * span, span)])
                for k in range(3)
            ]
        if t == 1:
            row = pl.ds(mo(core * half, half), half)
            return [
                (3 + k, gup_o.at[row, pl.ds(mo(k * (hb * n) + q * hb, hb), hb)], fu.at[:, pl.ds(k * hb, hb)])
                for k in range(s_n)
            ]
        if t == 2:
            row = pl.ds(mo(q * hb + core * hhalf, hhalf), hhalf)
            return [(3 + s_n, gdown_o.at[row], fd)]
        row = pl.ds(mo(core * ohalf, ohalf), ohalf)
        return [(4 + s_n, gout_o.at[row], fo)]

    local_out = []

    def spread(t, cond=None):
        for k, area, fin in areas(t, p, c):
            for i in range(1, n):
                q, dev = plane(i)
                start(rc(fin, area, agx_s.at[k, i], agx_r.at[k, p], dev), cond)
            start(rc(fin, area, agc_s.at[k, 0], agc_r.at[k, p], partner), cond)
            cp = pltpu.make_async_copy(fin, area, agl.at[k])
            if cond is None:
                cp.start()
            else:
                pl.when(cond)(cp.start)
            local_out.append((cond, cp))

    def spread_on(t):
        for i in range(1, n):
            q, dev = plane(i)
            for k, area, fin in areas(t, q, c):
                rc(fin, area, agx_s.at[k, i], agx_r.at[k, q], dev).wait_recv()
                start(rc(area, area, agc_s.at[k, i], agc_r.at[k, q], partner))

    def spread_end(t):
        for i in range(n):
            q = lax.rem(p + i, n)
            for k, area, fin in areas(t, q, other):
                rc(fin, area, agc_s.at[k, 0], agc_r.at[k, q], partner).wait_recv()

    local_g.wait()
    for i in range(1, n):
        q, dev = plane(i)
        rc(cot, seq(g_all, q), g_s.at[i], g_r.at[q], dev).wait_recv()

    for j in range(s_n):
        dwd[j] = dot(act[:, j * hb : (j + 1) * hb], g_all[...], TN).astype(BF)
    exchange(2, dwd, xrd, hhalf)

    table = [rot[i] for i in range(3)]

    def turn(t, sign):
        fwd = pltpu.roll(t, 128 - ROT // 2, 1)
        back = pltpu.roll(t, ROT // 2, 1)
        return t * table[0] + (fwd * table[1] + back * table[2]) * sign

    def qkv_block(s):
        row = pl.ds(mo(s * length, length), length)
        left_a = a1[row, :]
        for i in range(3):
            bias = inb[:, pl.ds(mo(i * width + p * span, span), span)]
            v = dot(left_a, w1[:, i * span : (i + 1) * span]) + bias
            for h in range(span // 128):
                part = v[:, h * 128 : (h + 1) * 128]
                if i < 2:
                    part = turn(part, 1.0)
                qkv[row, i * span + h * 128 : i * span + (h + 1) * 128] = part.astype(BF)

    relay(d_piece, d_s, d_r, dc_s, dc_r, 2)
    lax.fori_loop(0, n, lambda s, _: (qkv_block(s), 0)[1], 0)
    pair_sum(2, dwd, xrd, zrd, hhalf, s_n)

    lane = lax.broadcasted_iota(jnp.int32, (1, 128), 1)
    first = lane < HEAD_DIM
    masks = [first.astype(F32).astype(BF), (1.0 - first.astype(F32)).astype(BF)]
    pairs = span // 128

    def att_forward(idx, carry):
        s = lax.div(idx, pairs)
        pr = lax.rem(idx, pairs)
        row = pl.ds(mo(s * length, length), length)
        q2 = qkv[row, pl.ds(mo(pr * 128, 128), 128)]
        k2 = qkv[row, pl.ds(mo(span + pr * 128, 128), 128)]
        v2 = qkv[row, pl.ds(mo(2 * span + pr * 128, 128), 128)]
        key_i = lax.broadcasted_iota(jnp.int32, (length, length), 0)
        query_i = lax.broadcasted_iota(jnp.int32, (length, length), 1)
        got = []
        for h in range(2):
            st = dot(k2, q2 * masks[h], NT) * scale
            ex = jnp.exp(jnp.where(key_i <= query_i, st, MASKED))
            pr_t = ex / jnp.sum(ex, axis=0, keepdims=True)
            pt[idx * 2 + h] = pr_t
            got.append(dot(pr_t.astype(BF), v2, TN))
        att[row, pl.ds(mo(pr * 128, 128), 128)] = jnp.where(first, got[0], got[1]).astype(BF)
        return carry

    lax.fori_loop(0, n * pairs, att_forward, 0)
    relay(d_piece, d_s, d_r, dc_s, dc_r, 3)
    dwo[0] = dot(att[...], g_all[...], TN).astype(BF)
    exchange(3, dwo, xro, ohalf)

    def o_relay():
        away_left = zz < p
        away_right = zz > p

        @pl.when(jnp.logical_not(at_home))
        def _():
            rc(o_piece, o_piece, o_s.at[0], o_r.at[0], partner).wait_recv()

        start(
            rc(o_piece, o_piece, o_s.at[2], o_r.at[0], left), jnp.logical_and(away_left, has_left)
        )
        start(
            rc(o_piece, o_piece, o_s.at[3], o_r.at[0], right),
            jnp.logical_and(away_right, has_right),
        )
        start(
            rc(o_piece, o_piece, oc_s.at[0], oc_r.at[0], partner), jnp.logical_not(at_home)
        )

        @pl.when(jnp.logical_not(at_home))
        def _():
            rc(o_other, o_other, oc_s.at[0], oc_r.at[0], partner).wait_recv()

    o_relay()
    relay_done(d_other, dc_s, dc_r)

    bup_r[...] = jnp.zeros_like(bup_r)
    bin_r[...] = jnp.zeros_like(bin_r)

    def grad_block(s):
        row = pl.ds(mo(s * length, length), length)
        gs = g_all[row, :]
        gatt[row, :] = dot(gs, wo[...], NT).astype(BF)
        for j in range(s_n):
            col = pl.ds(j * hb, hb)
            gu = (dot(gs, wd[j * hb : (j + 1) * hb, :], NT) * der[row, col]).astype(BF)
            gup[row, col] = gu
            bup_r[:, col] += jnp.sum(gu.astype(F32), axis=0, keepdims=True)

    lax.fori_loop(0, n, lambda s, _: (grad_block(s), 0)[1], 0)

    for j in range(s_n):
        dwu[j] = dot(a2[:, j * rs : (j + 1) * rs], gup[...], TN).astype(BF)
    exchange(1, dwu, xru, half)

    own_half = pl.ds(mo(c * ohalf, ohalf), ohalf)
    rc(dwo.at[:, own_half], xro, xs_s.at[3], xs_r.at[3], partner).wait_recv()
    xro[0] = (dwo[0, own_half].astype(F32) + xro[0].astype(F32)).astype(BF)
    start(
        rc(xro.at[0], zro.at[zz], zs_s.at[3, 0], zs_r.at[3, zz], (r, p)), jnp.logical_not(at_home)
    )

    def out_block(k, carry):
        s = lax.rem(p + 1 + k, n)
        row = pl.ds(mo(s * length, length), length)
        for j in range(width // 256):
            col = slice(j * 256, (j + 1) * 256)
            v = dot(att[row, :], wo[:, col]) + dot(act[row, :], wd[:, col])
            msend[k, :, col] = v.astype(BF)
            mown[:, col] = v

        @pl.when(k < n - 1)
        def _():
            rc(msend.at[k], mrecv.at[p], m_s.at[k], m_r.at[p], (2 * s + c, zz)).start()

        return carry

    lax.fori_loop(0, n, out_block, 0)
    pair_sum(1, dwu, xru, zru, half, s_n)
    line_sum(2, xrd, zrd, fd)
    spread(2)

    def att_backward(idx, carry):
        s = lax.div(idx, pairs)
        pr = lax.rem(idx, pairs)
        row = pl.ds(mo(s * length, length), length)
        q_col = pl.ds(mo(pr * 128, 128), 128)
        k_col = pl.ds(mo(span + pr * 128, 128), 128)
        v_col = pl.ds(mo(2 * span + pr * 128, 128), 128)
        q2, k2, v2 = qkv[row, q_col], qkv[row, k_col], qkv[row, v_col]
        g2 = gatt[row, q_col]
        dq, dk, dv = [], [], []
        for h in range(2):
            pr_t = pt[idx * 2 + h]
            dp = dot(v2, g2 * masks[h], NT)
            inner = jnp.sum(dp * pr_t, axis=0, keepdims=True)
            ds = (pr_t * (dp - inner)).astype(BF)
            dv.append(dot(pr_t.astype(BF), g2))
            dk.append(dot(ds, q2))
            dq.append(dot(ds, k2, TN))
        dqv = turn(jnp.where(first, dq[0], dq[1]) * scale, -1.0).astype(BF)
        dkv = turn(jnp.where(first, dk[0], dk[1]) * scale, -1.0).astype(BF)
        dvv = jnp.where(first, dv[0], dv[1]).astype(BF)
        for col, val in ((q_col, dqv), (k_col, dkv), (v_col, dvv)):
            gqkv[row, col] = val
            bin_r[:, col] += jnp.sum(val.astype(F32), axis=0, keepdims=True)
        return carry

    lax.fori_loop(0, n * pairs, att_backward, 0)
    for j in range(s_n):
        dwi[j] = dot(a1[:, j * rs : (j + 1) * rs], gqkv[...], TN).astype(BF)
    exchange(0, dwi, xri, half)

    @pl.when(at_home)
    def _():
        total = xro[0].astype(F32)
        for i in range(1, s_n):
            q, dev = line(i)
            rc(xro.at[0], zro.at[q], zs_s.at[3, 0], zs_r.at[3, q], dev).wait_recv()
            total = total + zro[q].astype(F32)
        fo[...] = total.astype(BF)

    spread(3, at_home)
    spread_on(2)

    vacc[...] = jnp.zeros_like(vacc)

    def in_block(k, carry):
        s = lax.rem(p + 1 + k, n)
        row = pl.ds(mo(s * length, length), length)
        gq = gqkv[row, :]
        gu = gup[row, :]
        mu = mean_r[row, :]
        inv = inv_r[row, :]
        for j in range(s_n):
            col = slice(j * rs, (j + 1) * rs)
            d1 = dot(gq, w1[col, :iw], NT)
            d2 = dot(gu, w1[col, iw:], NT)
            xh = (x_all[row, col].astype(F32) - mu) * inv
            vacc[0, :, col] += jnp.sum(d1 * xh, axis=0, keepdims=True)
            vacc[1, :, col] += jnp.sum(d1, axis=0, keepdims=True)
            vacc[2, :, col] += jnp.sum(d2 * xh, axis=0, keepdims=True)
            vacc[3, :, col] += jnp.sum(d2, axis=0, keepdims=True)
            e = d1 * gain1[:, col] + d2 * gain2[:, col]
            esend[k, :, col] = e.astype(BF)
            eown[:, col] = e

        @pl.when(k < n - 1)
        def _():
            rc(esend.at[k], erecv.at[p], e_s.at[k], e_r.at[p], (2 * s + c, zz)).start()

        return carry

    pair_sum(0, dwi, xri, zri, half, s_n)
    lax.fori_loop(0, n, in_block, 0)

    slots = vfull.shape[0] // s_n
    vfull[...] = jnp.zeros_like(vfull)
    per = n_in // span
    for i in range(3):
        b = i * n + p
        vfull[lax.div(b, per) * slots + lax.rem(b, per)] = bin_r[:, i * span : (i + 1) * span]
    for q in range(s_n):
        vfull[q * slots + per + p] = bup_r[:, q * hb : (q + 1) * hb]
        col = slice(q * rs, (q + 1) * rs)
        g_own = g_all[pl.ds(mo(p * length, length), length), col].astype(F32)
        vfull[q * slots + per + n] = jnp.sum(g_own, axis=0, keepdims=True)
        for i in range(4):
            vfull[q * slots + per + n + 1 + i] = vacc[i, :, col]
    for i in range(1, s_n):
        q, dev = line(i)
        start(rc(vfull.at[pl.ds(q * slots, slots)], vz.at[zz], v1_s.at[i], v1_r.at[zz], dev))

    line_sum(1, xru, zru, fu)
    spread(1)

    for i in range(1, n):
        q, dev = plane(i)
        rc(msend.at[0], mrecv.at[q], m_s.at[0], m_r.at[q], dev).wait_recv()

    def mixed_rows(i, carry):
        step = 32
        row = pl.ds(mo(i * step, step), step)
        xv = x_all[pl.ds(mo(p * length + i * step, step), step), :].astype(F32)
        t = mown[row, :]
        for k in range(1, n):
            t = t + mrecv[lax.rem(p + k, n), row, :].astype(F32)
        mixed_o[row, :] = (xv + t + out_b + down_b).astype(BF)
        return carry

    lax.fori_loop(0, length // 32, mixed_rows, 0)

    line_sum(0, xri, zri, fi)
    spread(0)

    total = [vfull[zz * slots + k] for k in range(slots)]
    for i in range(1, s_n):
        q, dev = line(i)
        rc(vfull.at[pl.ds(0, slots)], vz.at[q], v1_s.at[i], v1_r.at[q], dev).wait_recv()
        total = [t + vz[q, k] for k, t in enumerate(total)]
    for k in range(slots):
        vu[k] = total[k]
        vr[r, k] = total[k]
    for i in range(1, 2 * n):
        start(rc(vu, vr.at[r], v2_s.at[i], v2_r.at[r], (lax.rem(r + i, 2 * n), zz)))

    spread_on(1)

    @pl.when(jnp.logical_not(at_home))
    def _():
        k, area, fin = areas(3, zz, c)[0]
        rc(fin, area, agx_s.at[k, 0], agx_r.at[k, zz], partner).wait_recv()

    k_o, area_o, _ = areas(3, zz, c)[0]
    start(
        rc(area_o, area_o, agc_s.at[k_o, 1], agc_r.at[k_o, zz], partner),
        jnp.logical_not(at_home),
    )

    for i in range(1, n):
        q, dev = plane(i)
        rc(esend.at[0], erecv.at[q], e_s.at[0], e_r.at[q], dev).wait_recv()

    def tgrad_rows(i, carry):
        step = 32
        row = pl.ds(mo(i * step, step), step)
        far = pl.ds(mo(p * length + i * step, step), step)
        inv = inv_r[far, :]
        xh = (x_all[far, :].astype(F32) - mean_r[far, :]) * inv
        e = eown[row, :]
        for k in range(1, n):
            e = e + erecv[lax.rem(p + k, n), row, :].astype(F32)
        m0 = jnp.mean(e, axis=1, keepdims=True)
        m1 = jnp.mean(e * xh, axis=1, keepdims=True)
        tgrad_o[row, :] = g_all[far, :].astype(F32) + inv * (e - m0 - xh * m1)
        return carry

    lax.fori_loop(0, length // 32, tgrad_rows, 0)

    for i in range(1, 2 * n):
        q = lax.rem(r + i, 2 * n)
        rc(vu, vr.at[q], v2_s.at[i], v2_r.at[q], (q, zz)).wait_recv()
    for k in range(slots):
        t = vr[0, k]
        for q in range(1, 2 * n):
            t = t + vr[q, k]
        vec_o[k] = t

    spread_on(0)
    for t in (2, 1, 0):
        spread_end(t)
    k, area, fin = areas(3, zz, other)[0]
    rc(fin, area, agc_s.at[k, 0], agc_r.at[k, zz], partner).wait_recv()

    for cond, cp in local_out:
        if cond is None:
            cp.wait()
        else:
            pl.when(cond)(cp.wait)
    for k in range(n - 1):
        rc(msend.at[k], mrecv.at[p], m_s.at[k], m_r.at[p], partner).wait_send()
        rc(esend.at[k], erecv.at[p], e_s.at[k], e_r.at[p], partner).wait_send()
    for cond, cp in sends:
        if cond is None:
            cp.wait_send()
        else:
            pl.when(cond)(cp.wait_send)


def fused_call(z, tok, cot, inp, upp, outp, downp, vec):
    n, s_n, length, width, span, hid = z.n, z.s, z.l, z.d, z.span, z.hid
    rs, hb, rows = z.rs, z.hb, z.rows
    iw = 3 * span
    nv = vec.shape[-1]
    slots = 3 * width // s_n // span + n + 5
    kinds = 5 + s_n
    V = pltpu.VMEM
    dma = lambda *shape: pltpu.SemaphoreType.DMA(shape)
    scratch = [
        *[V((rows, width), BF)] * 4,
        V((width, iw + hid), BF), V((span, width), BF), V((hid, width), BF),
        V((rows, iw), BF), V((n * span // HEAD_DIM, length, length), F32),
        V((rows, hid), F32), V((rows, hid), BF), V((rows, span), BF),
        V((rows, span), BF), V((rows, hid), BF), V((rows, iw), BF),
        *[V((n, length, width), BF), V((n, length, width), BF), V((length, width), F32)] * 2,
        V((s_n, rs, iw), BF), V((s_n, rs, hid), BF), V((s_n, hb, width), BF), V((1, span, width), BF),
        V((s_n, rs // 2, iw), BF), V((s_n, rs // 2, hid), BF), V((s_n, hb // 2, width), BF), V((1, span // 2, width), BF),
        V((s_n, rs // 2, iw), BF), V((s_n, rs // 2, hid), BF), V((s_n, hb // 2, width), BF), V((s_n, span // 2, width), BF),
        V((rs // 2, iw), BF), V((rs // 2, hid), BF), V((hb // 2, width), BF), V((span // 2, width), BF),
        V((s_n, 1, nv), F32), V((1, 3 * width), F32), V((s_n * slots, 1, 256), F32),
        V((s_n, slots, 1, 256), F32), V((slots, 1, 256), F32), V((2 * n, slots, 1, 256), F32),
        V((rows, 1), F32), V((rows, 1), F32), V((4, 1, width), F32), V((1, iw), F32), V((1, hid), F32),
        dma(8 + s_n), dma(s_n), dma(s_n), dma(n), dma(n), dma(n), dma(n),
        dma(2 * s_n), dma(s_n), dma(2 * s_n), dma(s_n),
        dma(2 * s_n), dma(s_n), dma(2 * s_n), dma(s_n),
        dma(4), dma(1), dma(1), dma(1),
        dma(n), dma(n), dma(n), dma(n), dma(4), dma(4), dma(4, s_n), dma(4, s_n),
        dma(kinds, n), dma(kinds, n), dma(kinds, n), dma(kinds, n), dma(kinds),
        dma(s_n), dma(s_n), dma(2 * n), dma(2 * n),
    ]
    any_ = pl.BlockSpec(memory_space=pl.ANY)
    vm = pl.BlockSpec(memory_space=pltpu.VMEM)
    outs = [
        jax.ShapeDtypeStruct((length, width), BF),
        jax.ShapeDtypeStruct((length, width), F32),
        jax.ShapeDtypeStruct((rs, 3 * width), BF),
        jax.ShapeDtypeStruct((rs, z.ff), BF),
        jax.ShapeDtypeStruct((hb * n, width), BF),
        jax.ShapeDtypeStruct((span, width), BF),
        jax.ShapeDtypeStruct((slots, 1, 256), F32),
    ]
    return pl.pallas_call(
        functools.partial(fused, z),
        out_shape=outs,
        in_specs=[any_] * 7 + [vm],
        out_specs=[vm, vm, any_, any_, any_, any_, vm],
        scratch_shapes=scratch,
        compiler_params=pltpu.CompilerParams(
            collective_id=0, has_side_effects=True, vmem_limit_bytes=VMEM_LIMIT
        ),
        name="block_step",
    )(tok, cot, inp, upp, outp, downp, vec, jnp.asarray(rotary_lanes(length)))


def make_fused_body(z):
    def body(
        tokens, in_proj, in_bias, out_proj, out_bias, up_proj, up_bias, down_proj, down_bias,
        first_gain, first_shift, second_gain, second_shift, cotangent,
    ):
        vec = jnp.concatenate(
            [in_bias, up_bias, out_bias, down_bias, first_gain, first_shift, second_gain, second_shift]
        ).astype(F32)[None]
        mixed, tgrad, g_in, g_up, g_down, g_out, vg = fused_call(
            z, tokens, cotangent, in_proj, up_proj, out_proj, down_proj, vec
        )
        per = in_bias.shape[0] // z.span
        flat = vg.reshape(-1)
        cut = lambda a, b: flat[a * 256 : b * 256]
        at = per + z.n
        bias = cut(at, at + 1)
        return (
            mixed, tgrad, g_in.astype(F32), cut(0, per), g_out.astype(F32), bias, g_up.astype(F32),
            cut(per, at), g_down.astype(F32), bias,
            cut(at + 1, at + 2), cut(at + 2, at + 3), cut(at + 3, at + 4), cut(at + 4, at + 5),
        )

    return body


def solution(mesh):
    rows = P(("rep", "shard"), None)
    mat = P("shard", None)
    vec = P("shard")
    in_specs = (rows, mat, vec, mat, vec, mat, vec, mat, vec, vec, vec, vec, vec, rows)
    out_specs = (rows, rows, mat, vec, mat, vec, mat, vec, mat, vec, vec, vec, vec, vec)
    shape = dict(mesh.shape)

    def step(*args):
        tokens, up_proj = args[0], args[5]
        devices = shape["rep"] * shape["shard"]
        z = Sizes(shape, tokens.shape[0] // devices, tokens.shape[1], up_proj.shape[1])
        body = make_fused_body(z) if z.fits() else make_body(shape["shard"])
        return jax.shard_map(
            body, mesh=mesh, in_specs=in_specs, out_specs=out_specs, check_vma=False
        )(*args)

    return step
```

```python
import functools

import jax
import jax.numpy as jnp
import numpy as np
from jax import lax
from jax.experimental import pallas as pl
from jax.experimental.pallas import tpu as pltpu
from jax.sharding import PartitionSpec as P

HEAD_DIM = 64
ROT = 16
EPS = 1e-05
MASKED = -1e30


def rotary_tables(length):
    half = ROT // 2
    inverse = jnp.exp(-jnp.log(10000.0) * (2.0 * jnp.arange(half, dtype=jnp.float32) / ROT))
    angles = jnp.arange(length, dtype=jnp.float32)[:, None] * inverse[None, :]
    return (jnp.cos(angles)[:, None, :], jnp.sin(angles)[:, None, :])


def rotate(values, cosine, sine, sign):
    half = ROT // 2
    first = values[..., :half]
    second = values[..., half:ROT]
    return jnp.concatenate(
        [
            first * cosine - sign * second * sine,
            second * cosine + sign * first * sine,
            values[..., ROT:],
        ],
        axis=-1,
    )


def mm(left, right, dims=((1,), (0,))):
    return lax.dot_general(left, right, (dims, ((), ())), preferred_element_type=jnp.float32)


def make_body(parts):
    def body(
        tokens,
        in_proj,
        in_bias,
        out_proj,
        out_bias,
        up_proj,
        up_bias,
        down_proj,
        down_bias,
        first_gain,
        first_shift,
        second_gain,
        second_shift,
        cotangent,
    ):
        length, width = tokens.shape
        me = lax.axis_index("shard")
        heads = width // parts // HEAD_DIM
        span = width // parts
        rows = in_proj.shape[0]
        hidden = up_bias.shape[0]
        scale = HEAD_DIM ** (-0.5)
        vectors = jnp.concatenate(
            [in_bias, out_bias, down_bias, first_gain, first_shift, second_gain, second_shift]
        )
        vectors = lax.all_gather(vectors, "shard", axis=0).astype(jnp.float32)
        cuts = [in_bias.shape[0]] + [span] * 6
        offsets = [sum(cuts[:i]) for i in range(len(cuts))]
        whole = [vectors[:, o : o + c].reshape(-1) for o, c in zip(offsets, cuts)]
        in_b, out_b, down_b, gain1, shift1, gain2, shift2 = whole
        both = lax.all_gather(jnp.stack([tokens, cotangent]), "shard", axis=1, tiled=True)
        x_all, g_all = both[0], both[1]
        w_in = lax.all_to_all(
            in_proj.reshape(rows, 3, parts, span), "shard", 2, 0, tiled=True
        ).reshape(parts * rows, 3 * span)
        w_up = lax.all_to_all(up_proj, "shard", 1, 0, tiled=True)
        b_in = lax.dynamic_slice_in_dim(in_b.reshape(3, parts, span), me, 1, axis=1).reshape(-1)
        x = x_all.astype(jnp.float32)
        mean = jnp.mean(x, axis=1, keepdims=True)
        cen = x - mean
        inv = lax.rsqrt(jnp.mean(cen * cen, axis=1, keepdims=True) + EPS)
        xhat = cen * inv
        attn_in = (xhat * gain1 + shift1).astype(jnp.bfloat16)
        mlp_in = (xhat * gain2 + shift2).astype(jnp.bfloat16)
        total_rows = x.shape[0]
        qkv = (mm(attn_in, w_in) + b_in).reshape(parts, length, 3, heads, HEAD_DIM)
        cosine, sine = rotary_tables(length)
        query = rotate(qkv[:, :, 0], cosine, sine, 1.0).astype(jnp.bfloat16)
        keys = rotate(qkv[:, :, 1], cosine, sine, 1.0).astype(jnp.bfloat16)
        values = qkv[:, :, 2].astype(jnp.bfloat16)
        causal = jnp.arange(length)[:, None] >= jnp.arange(length)[None, :]

        def ein(eq, a, b):
            return jnp.einsum(eq, a, b, preferred_element_type=jnp.float32)

        scores = jnp.where(causal, ein("sqhd,skhd->shqk", query, keys) * scale, MASKED)
        expo = jnp.exp(scores)
        probs_full = expo / jnp.sum(expo, axis=-1, keepdims=True)
        probs = probs_full.astype(jnp.bfloat16)
        attended = ein("shqk,skhd->sqhd", probs, values).astype(jnp.bfloat16)
        attended = attended.reshape(total_rows, span)
        up = mm(mlp_in, w_up) + up_bias.astype(jnp.float32)
        activated, pull = jax.vjp(lambda t: jax.nn.gelu(t, approximate=False), up)
        activated = activated.astype(jnp.bfloat16)
        partial = mm(attended, out_proj) + mm(activated, down_proj)
        branch = lax.psum_scatter(
            partial.astype(jnp.bfloat16), "shard", scatter_dimension=0, tiled=True
        )
        mixed = (tokens.astype(jnp.float32) + branch.astype(jnp.float32) + out_b + down_b).astype(
            jnp.bfloat16
        )
        grad_att = mm(g_all, out_proj, ((1,), (1,))).astype(jnp.bfloat16)
        grad_att = grad_att.reshape(parts, length, heads, HEAD_DIM)
        grad_act = mm(g_all, down_proj, ((1,), (1,)))
        grad_up = pull(grad_act)[0].astype(jnp.bfloat16)
        d_probs = ein("sqhd,skhd->shqk", grad_att, values)
        d_values = ein("shqk,sqhd->skhd", probs, grad_att)
        inner = jnp.sum(d_probs * probs_full, axis=-1, keepdims=True)
        d_scores = (probs_full * (d_probs - inner)).astype(jnp.bfloat16)
        d_query = ein("shqk,skhd->sqhd", d_scores, keys) * scale
        d_keys = ein("shqk,sqhd->skhd", d_scores, query) * scale
        d_query = rotate(d_query, cosine, sine, -1.0)
        d_keys = rotate(d_keys, cosine, sine, -1.0)
        grad_qkv = jnp.stack([d_query, d_keys, d_values], axis=2).astype(jnp.bfloat16)
        grad_qkv = grad_qkv.reshape(total_rows, 3 * span)
        d1 = mm(grad_qkv, w_in, ((1,), (1,)))
        d2 = mm(grad_up, w_up, ((1,), (1,)))
        scaled = (d1 * gain1 + d2 * gain2).astype(jnp.bfloat16)
        e = lax.psum_scatter(scaled, "shard", scatter_dimension=0, tiled=True).astype(jnp.float32)
        own = lambda a: lax.dynamic_slice_in_dim(a, me * length, length, axis=0)
        xh, rv = own(xhat), own(inv)
        tokens_grad = cotangent.astype(jnp.float32) + rv * (
            e - jnp.mean(e, axis=1, keepdims=True) - xh * jnp.mean(e * xh, axis=1, keepdims=True)
        )
        left = ((0,), (0,))
        dw_in = mm(attn_in, grad_qkv, left).astype(jnp.bfloat16)
        dw_up = mm(mlp_in, grad_up, left).astype(jnp.bfloat16)
        dw_out = mm(attended, g_all, left).astype(jnp.bfloat16)
        dw_down = mm(activated, g_all, left).astype(jnp.bfloat16)
        dw_in, dw_up, dw_out, dw_down = lax.psum((dw_in, dw_up, dw_out, dw_down), "rep")
        dw_in = lax.all_to_all(
            dw_in.reshape(parts * rows, 3, 1, span), "shard", 0, 2, tiled=True
        ).reshape(rows, 3 * width)
        dw_up = lax.all_to_all(dw_up, "shard", 0, 1, tiled=True)
        f32 = jnp.float32
        place = lambda v: lax.dynamic_update_slice_in_dim(
            jnp.zeros((3, parts, span), f32), v.reshape(3, 1, span), me, axis=1
        ).reshape(-1)
        vec = [
            place(jnp.sum(grad_qkv, axis=0, dtype=f32)),
            jnp.sum(cotangent.astype(f32), axis=0),
            jnp.sum(d1 * xhat, axis=0),
            jnp.sum(d1, axis=0),
            jnp.sum(d2 * xhat, axis=0),
            jnp.sum(d2, axis=0),
        ]
        vec = jnp.concatenate([v.reshape(parts, -1) for v in vec], axis=1)
        vec = lax.psum_scatter(vec, "shard", scatter_dimension=0, tiled=True)[0]
        vec, up_vec = lax.psum((vec, jnp.sum(grad_up, axis=0, dtype=f32)), "rep")
        o = in_bias.shape[0]
        bias_grad = vec[o : o + span]
        rest = [vec[o + span * i : o + span * (i + 1)] for i in range(1, 5)]
        return (
            mixed,
            tokens_grad,
            dw_in.astype(f32),
            vec[:o],
            dw_out.astype(f32),
            bias_grad,
            dw_up.astype(f32),
            up_vec,
            dw_down.astype(f32),
            bias_grad,
            *rest,
        )

    return body


BF = jnp.bfloat16
F32 = jnp.float32
MESH = pl.DeviceIdType.MESH
VMEM_LIMIT = 67_000_000
NN = ((1,), (0,))
NT = ((1,), (1,))
TN = ((0,), (0,))
IN, UP, DOWN, OUT = range(4)


class Sizes:
    def __init__(self, mesh_shape, length, width, hidden):
        self.copies = mesh_shape["rep"]
        self.n = self.copies // 2
        self.s = mesh_shape["shard"]
        self.l = length
        self.d = width
        self.ff = hidden
        self.span = width // self.n
        self.hid = hidden // self.n
        self.rs = width // self.s
        self.hb = hidden // self.s // self.n
        self.rows = self.n * length

    def fits(self):
        return (
            self.copies == 8
            and self.s == 4
            and self.rs == 256
            and self.span == 256
            and self.hb == 256
            and self.l % 256 == 0
        )


def rotary_lanes(length):
    half = ROT // 2
    inverse = np.exp(-np.log(10000.0) * (2.0 * np.arange(half) / ROT))
    angles = np.arange(length)[:, None] * inverse[None, :]
    cosine, sine = np.cos(angles), np.sin(angles)
    table = np.zeros((3, length, 128), np.float32)
    table[0] = 1.0
    for start in (0, HEAD_DIM):
        table[0, :, start : start + half] = cosine
        table[0, :, start + half : start + ROT] = cosine
        table[1, :, start : start + half] = -sine
        table[2, :, start + half : start + ROT] = sine
    return table


def dot(left, right, dims=NN):
    return lax.dot_general(left, right, (dims, ((), ())), preferred_element_type=F32)


def mo(value, m):
    return pl.multiple_of(value, m)


def fused(z, *refs):
    (tok, cot, inp, upp, outp, downp) = refs[:6]
    vectors_in, rot = refs[6:14], refs[14]
    (mixed_o, tgrad_o, gin_o, gup_o, gdown_o, gout_o, vec_o) = refs[15:22]
    (
        x_all, g_all, a1, a2, wi, wu, wo, wd, qkv, pt, der, act, att, gatt, gup, gqkv,
        msend, mrecv, mpre, mown, esend, erecv, epre, eown,
        dwi, dwu, dwd, dwo, xri, xru, xrd, xro, zri, zru, zrd, zro, fi, fu, fd, fo,
        vec, va, inb, vfull, vz, vu, vr, mean_r, inv_r, vacc, bin_r, bup_r,
        loc, v_s, v_r, x_s, x_r, g_s, g_r, w_s, w_r, wc_s, wc_r,
        o_s, o_r, oc_s, oc_r, m_s, m_r, e_s, e_r, xs_s, xs_r, zs_s, zs_r,
        ag_s, ag_r, agc_s, agc_r, agl, v1_s, v1_r, v2_s, v2_r,
    ) = refs[22:]
    n, s_n, length, width = z.n, z.s, z.l, z.d
    span, hid, rs, hb = z.span, z.hid, z.rs, z.hb
    iw = 3 * span
    scale = HEAD_DIM**-0.5
    r = lax.axis_index("rep")
    zz = lax.axis_index("shard")
    p = lax.div(r, 2)
    c = lax.rem(r, 2)
    other = 1 - c
    partner = (2 * p + other, zz)
    py, px = lax.div(p, 2), lax.rem(p, 2)
    xn, yn, dg = 2 * py + 1 - px, 2 * (1 - py) + px, 2 * (1 - py) + 1 - px
    dev_x, dev_y = (2 * xn + c, zz), (2 * yn + c, zz)
    zp, zo = lax.div(zz, 2), lax.rem(zz, 2)
    is_end = zp == zo
    inner = zp != zo
    mate = 2 * zp + 1 - zo
    mate_dev = (r, mate)
    far_end, far_inner = 3 * (1 - zp), 2 - zp
    left, right = (r, zz - 1), (r, zz + 1)
    has_left, has_right = zz > 0, zz < s_n - 1

    def rc(src, dst, ss, rr, dev):
        return pltpu.make_async_remote_copy(
            src_ref=src, dst_ref=dst, send_sem=ss, recv_sem=rr, device_id=dev, device_id_type=MESH
        )

    def got(ref, rr):
        rc(ref, ref, rr, rr, partner).wait_recv()

    def seq(ref, s):
        return ref.at[pl.ds(mo(s * length, length), length)]

    sends = []

    def start(copy, cond=None):
        if cond is None:
            copy.start()
        else:
            pl.when(cond)(copy.start)
        sends.append((cond, copy))

    own_rows = pl.ds(mo(zz * rs, rs), rs)
    own_hb = pl.ds(mo(zz * hb, hb), hb)
    local_u = [
        pltpu.make_async_copy(
            upp.at[:, pl.ds(mo(i * (hb * n) + p * hb, hb), hb)],
            wu.at[own_rows, pl.ds(i * hb, hb)],
            loc.at[i],
        )
        for i in range(s_n)
    ]
    local_i = [
        pltpu.make_async_copy(
            inp.at[:, pl.ds(mo(i * width + p * span, span), span)],
            wi.at[own_rows, pl.ds(i * span, span)],
            loc.at[s_n + i],
        )
        for i in range(3)
    ]
    at_loc = s_n + 3
    local_d = pltpu.make_async_copy(
        downp.at[pl.ds(mo(p * hb, hb), hb)], wd.at[own_hb], loc.at[at_loc]
    )
    local_x = pltpu.make_async_copy(tok, seq(x_all, p), loc.at[at_loc + 1])
    local_g = pltpu.make_async_copy(cot, seq(g_all, p), loc.at[at_loc + 2])
    local_o = pltpu.make_async_copy(outp, wo, loc.at[at_loc + 3])
    at_home = zz == p
    away = jnp.logical_not(at_home)
    for cp in local_u + [local_x, local_g, local_d] + local_i:
        cp.start()
    pl.when(at_home)(local_o.start)
    off = 0
    for ref in vectors_in:
        size = ref.shape[0]
        vec[:, off : off + size] = ref[...].astype(F32).reshape(1, size)
        off += size

    barrier = pltpu.get_barrier_semaphore()
    for i in range(1, 2 * n):
        pl.semaphore_signal(
            barrier, 1, device_id=(lax.rem(r + i, 2 * n), zz), device_id_type=MESH
        )
    for i in range(1, s_n):
        pl.semaphore_signal(barrier, 1, device_id=(r, lax.rem(zz + i, s_n)), device_id_type=MESH)
    pl.semaphore_wait(barrier, 2 * n - 1 + s_n - 1)

    def line(i):
        q = lax.rem(zz + i, s_n)
        return q, (r, q)

    def plane_send(src, dst, ss, rr, cond=None):
        start(rc(src(0), dst(p, 0), ss(0), rr(p, 0), dev_x), cond)
        start(rc(src(1), dst(p, 1), ss(1), rr(p, 1), dev_y), cond)
        start(rc(src(1), dst(p, 1), ss(2), rr(p, 1), dev_x), cond)
        start(rc(src(0), dst(p, 0), ss(3), rr(p, 0), dev_y), cond)

    def plane_relay(dst, ss, rr):
        got(dst(xn, 0), rr(xn, 0))
        start(rc(dst(xn, 0), dst(xn, 0), ss(4), rr(xn, 0), dev_y))
        got(dst(yn, 1), rr(yn, 1))
        start(rc(dst(yn, 1), dst(yn, 1), ss(5), rr(yn, 1), dev_x))

    def plane_near(dst, rr):
        got(dst(xn, 1), rr(xn, 1))
        got(dst(yn, 0), rr(yn, 0))

    def plane_far(dst, rr):
        got(dst(dg, 0), rr(dg, 0))
        got(dst(dg, 1), rr(dg, 1))

    lh = length // 2

    def part(ref):
        return lambda q, h: ref.at[pl.ds(mo(q * length + h * lh, lh), lh)]

    def sem1(ref):
        return lambda i: ref.at[i]

    def sem2(ref):
        return lambda q, h: ref.at[q, h]

    def rows_of(ref):
        return lambda h: ref.at[pl.ds(h * lh, lh)]

    for i in range(1, s_n):
        q, dev = line(i)
        start(rc(vec, va.at[zz], v_s.at[i], v_r.at[zz], dev))
    plane_send(rows_of(tok), part(x_all), sem1(x_s), sem2(x_r))

    half, hhalf, ohalf = rs // 2, hb // 2, span // 2

    def piece(ref, block):
        return lambda q, core: ref.at[pl.ds(mo(q * block + core * (block // 2), block // 2), block // 2)]

    u_piece, d_piece, i_piece = piece(wu, rs), piece(wd, hb), piece(wi, rs)

    def own_sends(t, get):
        start(rc(get(zz, c), get(zz, c), w_s.at[t, 0], w_r.at[t, zz], left), has_left)
        start(rc(get(zz, c), get(zz, c), w_s.at[t, 1], w_r.at[t, zz], right), has_right)

    def relay(t, get, d):
        def take(q, has, onward, more, slot):
            @pl.when(has)
            def _():
                got(get(q, c), w_r.at[t, q])

            start(
                rc(get(q, c), get(q, c), w_s.at[t, slot], w_r.at[t, q], onward),
                jnp.logical_and(has, more),
            )
            start(rc(get(q, c), get(q, c), wc_s.at[t, slot], wc_r.at[t, q], partner), has)

        take(zz - d, zz - d >= 0, right, has_right, 2 * d)
        take(zz + d, zz + d <= s_n - 1, left, has_left, 2 * d + 1)

    def relay_done(t, get):
        for i in range(1, s_n):
            q, _ = line(i)
            got(get(q, other), wc_r.at[t, q])

    for cp in local_u:
        cp.wait()
    own_sends(UP, u_piece)

    for i in range(1, s_n):
        q, dev = line(i)
        got(va.at[q], v_r.at[q])
    va[zz] = vec[...]
    n_in = 3 * width // s_n
    n_up = hb * n
    at_up = n_in
    at_rest = n_in + n_up

    def vector(i):
        off = at_rest + i * rs
        return jnp.concatenate([va[q, :, off : off + rs] for q in range(s_n)], axis=1)

    out_b, down_b, gain1, shift1, gain2, shift2 = [vector(i) for i in range(6)]
    for q in range(s_n):
        inb[:, q * n_in : (q + 1) * n_in] = va[q, :, :n_in]

    def norm(s):
        step = 32

        def body(i, carry):
            row = pl.ds(mo(s * length + i * step, step), step)
            xv = x_all[row, :].astype(F32)
            mu = jnp.mean(xv, axis=1, keepdims=True)
            cen = xv - mu
            inv = lax.rsqrt(jnp.mean(cen * cen, axis=1, keepdims=True) + EPS)
            xh = cen * inv
            a1[row, :] = (xh * gain1 + shift1).astype(BF)
            a2[row, :] = (xh * gain2 + shift2).astype(BF)
            mean_r[row, :] = mu
            inv_r[row, :] = inv
            return carry

        lax.fori_loop(0, length // step, body, 0)

    local_x.wait()
    norm(p)
    relay(UP, u_piece, 1)
    plane_relay(part(x_all), sem1(x_s), sem2(x_r))
    plane_send(rows_of(cot), part(g_all), sem1(g_s), sem2(g_r))
    relay(UP, u_piece, 2)
    local_d.wait()
    own_sends(DOWN, d_piece)
    plane_near(part(x_all), sem2(x_r))
    norm(xn)
    norm(yn)
    plane_far(part(x_all), sem2(x_r))
    norm(dg)
    relay(UP, u_piece, 3)
    relay_done(UP, u_piece)

    def up_block(s):
        row = pl.ds(mo(s * length, length), length)
        left_a = a2[row, :]
        for j in range(s_n):
            col = pl.ds(j * hb, hb)
            bias = va[j, :, pl.ds(mo(at_up + p * hb, hb), hb)]
            u = dot(left_a, wu[:, j * hb : (j + 1) * hb]) + bias
            phi = 0.5 * (1.0 + lax.erf(u * 0.7071067811865476))
            act[row, col] = (u * phi).astype(BF)
            der[row, col] = phi + u * (0.3989422804014327 * jnp.exp(-0.5 * u * u))

    lax.fori_loop(0, n, lambda s, _: (up_block(s), 0)[1], 0)

    relay(DOWN, d_piece, 1)
    plane_relay(part(g_all), sem1(g_s), sem2(g_r))
    relay(DOWN, d_piece, 2)
    for cp in local_i:
        cp.wait()
    pl.when(at_home)(local_o.wait)
    near_first = ((mate, mate_dev), (far_inner, (r, far_inner)), (far_end, (r, far_end)))
    for i, (q, dev) in enumerate(near_first):
        start(rc(i_piece(zz, c), i_piece(zz, c), w_s.at[IN, i], w_r.at[IN, zz], dev))
    o_piece = lambda core: wo.at[pl.ds(mo(core * ohalf, ohalf), ohalf)]
    for i, (q, dev) in enumerate(near_first):
        start(rc(o_piece(c), o_piece(c), o_s.at[i], o_r.at[0], dev), at_home)
    relay(DOWN, d_piece, 3)
    relay_done(DOWN, d_piece)
    local_g.wait()
    plane_near(part(g_all), sem2(g_r))
    plane_far(part(g_all), sem2(g_r))

    def exchange(t, dw, xr, block_half):
        src = dw.at[:, pl.ds(mo(other * block_half, block_half), block_half)]
        start(rc(src, xr, xs_s.at[t], xs_r.at[t], partner))

    def core_sum(t, dw, xr, block_half):
        mine = pl.ds(mo(c * block_half, block_half), block_half)
        got(xr, xs_r.at[t])

        def body(q, carry):
            xr[q] = (dw[q, mine].astype(F32) + xr[q].astype(F32)).astype(BF)
            return carry

        lax.fori_loop(0, dw.shape[0], body, 0)

    def pair_sum(t, dw, xr, zr, block_half):
        core_sum(t, dw, xr, block_half)
        start(rc(xr.at[far_end], zr.at[2], zs_s.at[t, 0], zs_r.at[t, 2], mate_dev), is_end)
        start(rc(xr.at[far_inner], zr.at[3], zs_s.at[t, 1], zs_r.at[t, 3], mate_dev), is_end)
        start(rc(xr.at[mate], zr.at[0], zs_s.at[t, 2], zs_r.at[t, 0], mate_dev))

    def pass_on(t, xr, zr):
        @pl.when(inner)
        def _():
            for slot, q in ((2, far_end), (3, far_inner)):
                got(zr.at[slot], zs_r.at[t, slot])
                xr[q] = (xr[q].astype(F32) + zr[slot].astype(F32)).astype(BF)
                rc(xr.at[q], zr.at[1], zs_s.at[t, slot - 2], zs_r.at[t, 1], (r, q)).start()

        for slot, q in ((2, far_end), (3, far_inner)):
            cp = rc(xr.at[q], zr.at[1], zs_s.at[t, slot - 2], zs_r.at[t, 1], (r, q))
            sends.append((inner, cp))

    def line_sum(t, xr, zr, fin):
        got(zr.at[0], zs_r.at[t, 0])
        got(zr.at[1], zs_r.at[t, 1])
        total = xr[zz].astype(F32) + zr[0].astype(F32) + zr[1].astype(F32)
        fin[...] = total.astype(BF)

    outs_of = {IN: (gin_o, fi), UP: (gup_o, fu), DOWN: (gdown_o, fd)}

    def area(t):
        o = outs_of[t][0]
        rows = o.shape[2] // 2
        return lambda q, h: o.at[q, c, pl.ds(h * rows, rows)]

    def fin_half(t):
        fin = outs_of[t][1]
        rows = fin.shape[0] // 2
        return lambda h: fin.at[pl.ds(h * rows, rows)]

    def ag1(t):
        return lambda i: ag_s.at[t, i]

    def ag2(t):
        return lambda q, h: ag_r.at[t, q, h]

    local_out = []

    def spread(t):
        o, fin = outs_of[t]
        plane_send(fin_half(t), area(t), ag1(t), ag2(t))
        start(rc(fin, o.at[p, c], agc_s.at[t, 0], agc_r.at[t, p], partner))
        cp = pltpu.make_async_copy(fin, o.at[p, c], agl.at[t])
        cp.start()
        local_out.append((None, cp))

    def spread_relay(t):
        plane_relay(area(t), ag1(t), ag2(t))

    def spread_on(t):
        o = outs_of[t][0]
        plane_near(area(t), ag2(t))
        start(rc(o.at[xn, c], o.at[xn, c], agc_s.at[t, 1], agc_r.at[t, xn], partner))
        start(rc(o.at[yn, c], o.at[yn, c], agc_s.at[t, 2], agc_r.at[t, yn], partner))
        plane_far(area(t), ag2(t))
        start(rc(o.at[dg, c], o.at[dg, c], agc_s.at[t, 3], agc_r.at[t, dg], partner))

    def spread_end(t):
        o = outs_of[t][0]
        for i in range(n):
            q = lax.rem(p + i, n)
            got(o.at[q, other], agc_r.at[t, q])

    for j in range(s_n):
        dwd[j] = dot(act[:, j * hb : (j + 1) * hb], g_all[...], TN).astype(BF)
    exchange(DOWN, dwd, xrd, hhalf)

    bup_r[...] = jnp.zeros_like(bup_r)
    bin_r[...] = jnp.zeros_like(bin_r)

    def grad_up_block(s):
        row = pl.ds(mo(s * length, length), length)
        gs = g_all[row, :]
        for j in range(s_n):
            col = pl.ds(j * hb, hb)
            gu = (dot(gs, wd[j * hb : (j + 1) * hb, :], NT) * der[row, col]).astype(BF)
            gup[row, col] = gu
            bup_r[:, col] += jnp.sum(gu.astype(F32), axis=0, keepdims=True)

    def grad_up_blocks(first, last):
        lax.fori_loop(first, last, lambda s, _: (grad_up_block(s), 0)[1], 0)

    grad_up_blocks(0, 2)
    pair_sum(DOWN, dwd, xrd, zrd, hhalf)
    grad_up_blocks(2, n)
    for j in range(s_n):
        dwu[j] = dot(a2[:, j * rs : (j + 1) * rs], gup[...], TN).astype(BF)
    exchange(UP, dwu, xru, half)

    table = [rot[i] for i in range(3)]

    def turn(t, sign):
        fwd = pltpu.roll(t, 128 - ROT // 2, 1)
        back = pltpu.roll(t, ROT // 2, 1)
        return t * table[0] + (fwd * table[1] + back * table[2]) * sign

    def qkv_block(s):
        row = pl.ds(mo(s * length, length), length)
        left_a = a1[row, :]
        for i in range(3):
            bias = inb[:, pl.ds(mo(i * width + p * span, span), span)]
            v = dot(left_a, wi[:, i * span : (i + 1) * span]) + bias
            for h in range(span // 128):
                cut = v[:, h * 128 : (h + 1) * 128]
                if i < 2:
                    cut = turn(cut, 1.0)
                qkv[row, i * span + h * 128 : i * span + (h + 1) * 128] = cut.astype(BF)

    for i, (q, dev) in enumerate(near_first):
        got(i_piece(q, c), w_r.at[IN, q])
        start(rc(i_piece(q, c), i_piece(q, c), wc_s.at[IN, i], wc_r.at[IN, q], partner))
    pair_sum(UP, dwu, xru, zru, half)
    relay_done(IN, i_piece)
    lax.fori_loop(0, n, lambda s, _: (qkv_block(s), 0)[1], 0)

    pass_on(DOWN, xrd, zrd)
    lane = lax.broadcasted_iota(jnp.int32, (1, 128), 1)
    first = lane < HEAD_DIM
    masks = [first.astype(F32).astype(BF), (1.0 - first.astype(F32)).astype(BF)]
    pairs = span // 128

    def att_forward(idx, carry):
        s = lax.div(idx, pairs)
        pr = lax.rem(idx, pairs)
        row = pl.ds(mo(s * length, length), length)
        q2 = qkv[row, pl.ds(mo(pr * 128, 128), 128)]
        k2 = qkv[row, pl.ds(mo(span + pr * 128, 128), 128)]
        v2 = qkv[row, pl.ds(mo(2 * span + pr * 128, 128), 128)]
        key_i = lax.broadcasted_iota(jnp.int32, (length, length), 0)
        query_i = lax.broadcasted_iota(jnp.int32, (length, length), 1)
        found = []
        for h in range(2):
            st = dot(k2, q2 * masks[h], NT) * scale
            ex = jnp.exp(jnp.where(key_i <= query_i, st, MASKED))
            pr_t = ex / jnp.sum(ex, axis=0, keepdims=True)
            pt[idx * 2 + h] = pr_t
            found.append(dot(pr_t.astype(BF), v2, TN))
        att[row, pl.ds(mo(pr * 128, 128), 128)] = jnp.where(first, found[0], found[1]).astype(BF)
        return carry

    lax.fori_loop(0, n * pairs, att_forward, 0)

    @pl.when(away)
    def _():
        got(o_piece(c), o_r.at[0])

    start(rc(o_piece(c), o_piece(c), oc_s.at[0], oc_r.at[0], partner), away)

    @pl.when(away)
    def _():
        got(o_piece(other), oc_r.at[0])

    def shares(send, pre, ss, rr, k):
        @pl.when(k == 0)
        def _():
            for h, dev in ((0, dev_x), (1, dev_y)):
                rc(send.at[0, pl.ds(h * lh, lh)], pre.at[h], ss.at[h], rr.at[h], dev).start()

    def shares_on(send, recv, pre, ss, rr):
        for k, h, dev in ((2, 1, dev_x), (3, 0, dev_y)):
            got(pre.at[h], rr.at[h])
            row = pl.ds(h * lh, lh)
            send[k, row] = (send[k, row].astype(F32) + pre[h].astype(F32)).astype(BF)
            start(rc(send.at[k], recv.at[k - 2], ss.at[k], rr.at[k], dev))

    def shares_left(send, pre, ss, rr):
        for h, dev in ((0, dev_x), (1, dev_y)):
            rc(send.at[0, pl.ds(h * lh, lh)], pre.at[h], ss.at[h], rr.at[h], dev).wait_send()

    def turn_of(k):
        return jnp.where(k == 0, dg, jnp.where(k == 1, p, jnp.where(k == 2, xn, yn)))

    def out_block(k, carry):
        s = turn_of(k)
        row = pl.ds(mo(s * length, length), length)
        for j in range(width // 256):
            col = slice(j * 256, (j + 1) * 256)
            v = dot(att[row, :], wo[:, col]) + dot(act[row, :], wd[:, col])
            msend[k, :, col] = v.astype(BF)

            @pl.when(k == 1)
            def _():
                mown[:, col] = v

        shares(msend, mpre, m_s, m_r, k)
        return carry

    lax.fori_loop(0, n, out_block, 0)

    dwo[0] = dot(att[...], g_all[...], TN).astype(BF)
    exchange(OUT, dwo, xro, ohalf)

    def grad_att_block(s):
        row = pl.ds(mo(s * length, length), length)
        gatt[row, :] = dot(g_all[row, :], wo[...], NT).astype(BF)

    lax.fori_loop(0, n, lambda s, _: (grad_att_block(s), 0)[1], 0)
    core_sum(OUT, dwo, xro, ohalf)
    to_mate = p == mate
    to_far = lax.div(p, 2) != zp
    start(rc(xro.at[0], zro.at[0], zs_s.at[OUT, 0], zs_r.at[OUT, 0], mate_dev), to_mate)
    start(
        rc(xro.at[0], zro.at[2], zs_s.at[OUT, 1], zs_r.at[OUT, 2], mate_dev),
        jnp.logical_and(to_far, is_end),
    )
    shares_on(msend, mrecv, mpre, m_s, m_r)

    def att_backward(idx, carry):
        s = lax.div(idx, pairs)
        pr = lax.rem(idx, pairs)
        row = pl.ds(mo(s * length, length), length)
        q_col = pl.ds(mo(pr * 128, 128), 128)
        k_col = pl.ds(mo(span + pr * 128, 128), 128)
        v_col = pl.ds(mo(2 * span + pr * 128, 128), 128)
        q2, k2, v2 = qkv[row, q_col], qkv[row, k_col], qkv[row, v_col]
        g2 = gatt[row, q_col]
        dq, dk, dv = [], [], []
        for h in range(2):
            pr_t = pt[idx * 2 + h]
            dp = dot(v2, g2 * masks[h], NT)
            total = jnp.sum(dp * pr_t, axis=0, keepdims=True)
            ds = (pr_t * (dp - total)).astype(BF)
            dv.append(dot(pr_t.astype(BF), g2))
            dk.append(dot(ds, q2))
            dq.append(dot(ds, k2, TN))
        dqv = turn(jnp.where(first, dq[0], dq[1]) * scale, -1.0).astype(BF)
        dkv = turn(jnp.where(first, dk[0], dk[1]) * scale, -1.0).astype(BF)
        dvv = jnp.where(first, dv[0], dv[1]).astype(BF)
        for col, val in ((q_col, dqv), (k_col, dkv), (v_col, dvv)):
            gqkv[row, col] = val
            bin_r[:, col] += jnp.sum(val.astype(F32), axis=0, keepdims=True)
        return carry

    lax.fori_loop(0, n * pairs, att_backward, 0)

    for j in range(s_n):
        dwi[j] = dot(a1[:, j * rs : (j + 1) * rs], gqkv[...], TN).astype(BF)
    exchange(IN, dwi, xri, half)

    vacc[...] = jnp.zeros_like(vacc)

    def in_block(k, carry):
        s = turn_of(k)
        row = pl.ds(mo(s * length, length), length)
        gq = gqkv[row, :]
        gu = gup[row, :]
        mu = mean_r[row, :]
        inv = inv_r[row, :]
        for j in range(s_n):
            col = slice(j * rs, (j + 1) * rs)
            d1 = dot(gq, wi[col, :], NT)
            d2 = dot(gu, wu[col, :], NT)
            xh = (x_all[row, col].astype(F32) - mu) * inv
            vacc[0, :, col] += jnp.sum(d1 * xh, axis=0, keepdims=True)
            vacc[1, :, col] += jnp.sum(d1, axis=0, keepdims=True)
            vacc[2, :, col] += jnp.sum(d2 * xh, axis=0, keepdims=True)
            vacc[3, :, col] += jnp.sum(d2, axis=0, keepdims=True)
            e = d1 * gain1[:, col] + d2 * gain2[:, col]
            esend[k, :, col] = e.astype(BF)

            @pl.when(k == 1)
            def _():
                eown[:, col] = e

        shares(esend, epre, e_s, e_r, k)
        return carry

    lax.fori_loop(0, 2, in_block, 0)
    pair_sum(IN, dwi, xri, zri, half)
    lax.fori_loop(2, n, in_block, 0)

    pass_on(UP, xru, zru)
    line_sum(DOWN, xrd, zrd, fd)
    spread(DOWN)

    slots = vfull.shape[0] // s_n
    vfull[...] = jnp.zeros_like(vfull)
    per = n_in // span
    for i in range(3):
        b = i * n + p
        vfull[lax.div(b, per) * slots + lax.rem(b, per)] = bin_r[:, i * span : (i + 1) * span]
    for q in range(s_n):
        vfull[q * slots + per + p] = bup_r[:, q * hb : (q + 1) * hb]
        col = slice(q * rs, (q + 1) * rs)
        g_own = g_all[pl.ds(mo(p * length, length), length), col].astype(F32)
        vfull[q * slots + per + n] = jnp.sum(g_own, axis=0, keepdims=True)
        for i in range(4):
            vfull[q * slots + per + n + 1 + i] = vacc[i, :, col]
    for i in range(1, s_n):
        q, dev = line(i)
        start(rc(vfull.at[pl.ds(q * slots, slots)], vz.at[zz], v1_s.at[i], v1_r.at[zz], dev))

    shares_on(esend, erecv, epre, e_s, e_r)

    far_and_inner = jnp.logical_and(to_far, inner)
    on = rc(xro.at[0], zro.at[1], zs_s.at[OUT, 2], zs_r.at[OUT, 1], (r, p))

    @pl.when(far_and_inner)
    def _():
        got(zro.at[2], zs_r.at[OUT, 2])
        xro[0] = (xro[0].astype(F32) + zro[2].astype(F32)).astype(BF)
        on.start()

    sends.append((far_and_inner, on))

    got(mrecv.at[0], m_r.at[2])
    got(mrecv.at[1], m_r.at[3])

    def mixed_rows(i, carry):
        step = 32
        row = pl.ds(mo(i * step, step), step)
        xv = x_all[pl.ds(mo(p * length + i * step, step), step), :].astype(F32)
        t = mown[row, :] + mrecv[0, row, :].astype(F32) + mrecv[1, row, :].astype(F32)
        mixed_o[row, :] = (xv + t + out_b + down_b).astype(BF)
        return carry

    lax.fori_loop(0, length // 32, mixed_rows, 0)

    spread_relay(DOWN)
    pass_on(IN, xri, zri)
    line_sum(UP, xru, zru, fu)
    spread(UP)
    spread_on(DOWN)

    @pl.when(at_home)
    def _():
        got(zro.at[0], zs_r.at[OUT, 0])
        got(zro.at[1], zs_r.at[OUT, 1])
        total = xro[0].astype(F32) + zro[0].astype(F32) + zro[1].astype(F32)
        fo[...] = total.astype(BF)

    oq = ohalf // 2
    o_area = lambda q, h: gout_o.at[c, pl.ds(h * oq, oq)]
    plane_send(lambda h: fo.at[pl.ds(h * oq, oq)], o_area, ag1(OUT), ag2(OUT), at_home)
    start(rc(fo, gout_o.at[c], agc_s.at[OUT, 0], agc_r.at[OUT, zz], partner), at_home)
    cp = pltpu.make_async_copy(fo, gout_o.at[c], agl.at[OUT])
    pl.when(at_home)(cp.start)
    local_out.append((at_home, cp))

    total = [vfull[zz * slots + k] for k in range(slots)]
    for i in range(1, s_n):
        q, dev = line(i)
        got(vz.at[q], v1_r.at[q])
        total = [t + vz[q, k] for k, t in enumerate(total)]
    for k in range(slots):
        vu[k] = total[k]
        vr[r, k] = total[k]
    for i in range(1, 2 * n):
        start(rc(vu, vr.at[r], v2_s.at[i], v2_r.at[r], (lax.rem(r + i, 2 * n), zz)))

    line_sum(IN, xri, zri, fi)
    spread(IN)
    spread_relay(UP)

    from_x, from_y = xn == zz, yn == zz

    @pl.when(away)
    def _():
        got(o_area(zz, 0), ag_r.at[OUT, zz, 0])

    start(rc(o_area(zz, 0), o_area(zz, 0), ag_s.at[OUT, 4], ag_r.at[OUT, zz, 0], dev_y), from_x)

    @pl.when(away)
    def _():
        got(o_area(zz, 1), ag_r.at[OUT, zz, 1])

    start(rc(o_area(zz, 1), o_area(zz, 1), ag_s.at[OUT, 5], ag_r.at[OUT, zz, 1], dev_x), from_y)
    start(
        rc(gout_o.at[c], gout_o.at[c], agc_s.at[OUT, 1], agc_r.at[OUT, zz], partner), away
    )
    spread_relay(IN)
    spread_on(UP)

    got(erecv.at[0], e_r.at[2])
    got(erecv.at[1], e_r.at[3])

    def tgrad_rows(i, carry):
        step = 32
        row = pl.ds(mo(i * step, step), step)
        far = pl.ds(mo(p * length + i * step, step), step)
        inv = inv_r[far, :]
        xh = (x_all[far, :].astype(F32) - mean_r[far, :]) * inv
        e = eown[row, :] + erecv[0, row, :].astype(F32) + erecv[1, row, :].astype(F32)
        m0 = jnp.mean(e, axis=1, keepdims=True)
        m1 = jnp.mean(e * xh, axis=1, keepdims=True)
        tgrad_o[row, :] = g_all[far, :].astype(F32) + inv * (e - m0 - xh * m1)
        return carry

    lax.fori_loop(0, length // 32, tgrad_rows, 0)

    for i in range(1, 2 * n):
        q = lax.rem(r + i, 2 * n)
        got(vr.at[q], v2_r.at[q])
    for k in range(slots):
        t = vr[0, k]
        for q in range(1, 2 * n):
            t = t + vr[q, k]
        vec_o[k] = t
    spread_on(IN)
    for t in (DOWN, UP, IN):
        spread_end(t)
    got(gout_o.at[other], agc_r.at[OUT, zz])

    for cond, cp in local_out:
        if cond is None:
            cp.wait()
        else:
            pl.when(cond)(cp.wait)
    shares_left(msend, mpre, m_s, m_r)
    shares_left(esend, epre, e_s, e_r)
    for cond, cp in sends:
        if cond is None:
            cp.wait_send()
        else:
            pl.when(cond)(cp.wait_send)


def fused_call(z, tok, cot, inp, upp, outp, downp, vectors):
    n, s_n, length, width, span, hid = z.n, z.s, z.l, z.d, z.span, z.hid
    rs, hb, rows = z.rs, z.hb, z.rows
    iw = 3 * span
    nv = sum(v.shape[0] for v in vectors)
    slots = 3 * width // s_n // span + n + 5
    V = pltpu.VMEM
    dma = lambda *shape: pltpu.SemaphoreType.DMA(shape)
    share = [
        V((n, length, width), BF), V((2, length, width), BF), V((2, length // 2, width), BF),
        V((length, width), F32),
    ]
    halves = [
        V((s_n, rs // 2, iw), BF), V((s_n, rs // 2, hid), BF), V((s_n, hb // 2, width), BF),
    ]
    scratch = [
        *[V((rows, width), BF)] * 4,
        V((width, iw), BF), V((width, hid), BF), V((span, width), BF), V((hid, width), BF),
        V((rows, iw), BF), V((n * span // HEAD_DIM, length, length), F32),
        V((rows, hid), F32), V((rows, hid), BF), V((rows, span), BF),
        V((rows, span), BF), V((rows, hid), BF), V((rows, iw), BF),
        *share, *share,
        V((s_n, rs, iw), BF), V((s_n, rs, hid), BF), V((s_n, hb, width), BF), V((1, span, width), BF),
        *halves, V((1, span // 2, width), BF),
        *halves, V((3, span // 2, width), BF),
        V((rs // 2, iw), BF), V((rs // 2, hid), BF), V((hb // 2, width), BF), V((span // 2, width), BF),
        V((1, nv), F32), V((s_n, 1, nv), F32), V((1, 3 * width), F32), V((s_n * slots, 1, 256), F32),
        V((s_n, slots, 1, 256), F32), V((slots, 1, 256), F32), V((2 * n, slots, 1, 256), F32),
        V((rows, 1), F32), V((rows, 1), F32), V((4, 1, width), F32), V((1, iw), F32), V((1, hid), F32),
        dma(s_n + 7), dma(s_n), dma(s_n), dma(6), dma(n, 2), dma(6), dma(n, 2),
        dma(3, 2 * s_n), dma(3, s_n), dma(3, 2 * s_n), dma(3, s_n),
        dma(3), dma(1), dma(1), dma(1),
        dma(n), dma(n), dma(n), dma(n), dma(4), dma(4), dma(4, 3), dma(4, 4),
        dma(4, 6), dma(4, n, 2), dma(4, n), dma(4, n), dma(4),
        dma(s_n), dma(s_n), dma(2 * n), dma(2 * n),
    ]
    any_ = pl.BlockSpec(memory_space=pl.ANY)
    vm = pl.BlockSpec(memory_space=pltpu.VMEM)
    outs = [
        jax.ShapeDtypeStruct((length, width), BF),
        jax.ShapeDtypeStruct((length, width), F32),
        jax.ShapeDtypeStruct((n, 2, rs // 2, iw), BF),
        jax.ShapeDtypeStruct((n, 2, rs // 2, hid), BF),
        jax.ShapeDtypeStruct((n, 2, hb // 2, width), BF),
        jax.ShapeDtypeStruct((2, span // 2, width), BF),
        jax.ShapeDtypeStruct((slots, 1, 256), F32),
    ]
    return pl.pallas_call(
        functools.partial(fused, z),
        out_shape=outs,
        in_specs=[any_] * 6 + [vm] * 9,
        out_specs=[vm, vm, any_, any_, any_, any_, vm],
        scratch_shapes=scratch,
        compiler_params=pltpu.CompilerParams(
            collective_id=0, has_side_effects=True, vmem_limit_bytes=VMEM_LIMIT
        ),
        name="block_step",
    )(tok, cot, inp, upp, outp, downp, *vectors, jnp.asarray(rotary_lanes(length)))


def finish(z, *refs):
    mixed, tgrad, g_in, g_up, g_down, g_out, vec = refs[:7]
    mixed_o, tgrad_o, in_o, up_o, down_o, out_o = refs[7:13]
    vec_o = refs[13:21]
    m_v, t_v, bi, bu, bd, bo, fi, fu, fd, fo, m_sem, r_sem, w_sem = refs[21:]
    n, s_n, width, span, hb, rs = z.n, z.s, z.d, z.span, z.hb, z.rs
    half = rs // 2
    jobs = []
    for q in range(n):
        for core in range(2):
            row = slice(core * half, (core + 1) * half)
            jobs.append((g_up.at[q, core], bu.at[q, core], fu.at[q, core], [
                (up_o.at[row, k * hb * n + q * hb : k * hb * n + (q + 1) * hb], slice(k * hb, (k + 1) * hb))
                for k in range(s_n)
            ]))
    for q in range(n):
        for core in range(2):
            start = q * hb + core * (hb // 2)
            jobs.append((g_down.at[q, core], bd.at[q, core], fd.at[q, core], [
                (down_o.at[start : start + hb // 2], slice(None)),
            ]))
    for q in range(n):
        for core in range(2):
            row = slice(core * half, (core + 1) * half)
            jobs.append((g_in.at[q, core], bi.at[q, core], fi.at[q, core], [
                (in_o.at[row, k * width + q * span : k * width + (q + 1) * span], slice(k * span, (k + 1) * span))
                for k in range(3)
            ]))
    for core in range(2):
        start = core * (span // 2)
        jobs.append((g_out.at[core], bo.at[core], fo.at[core], [
            (out_o.at[start : start + span // 2], slice(None)),
        ]))
    through = [
        (pltpu.make_async_copy(a, b, m_sem.at[2 * i]), pltpu.make_async_copy(b, o, m_sem.at[2 * i + 1]))
        for i, (a, b, o) in enumerate(((mixed, m_v, mixed_o), (tgrad, t_v, tgrad_o)))
    ]
    reads = [pltpu.make_async_copy(src, dst, r_sem.at[i]) for i, (src, dst, _, _) in enumerate(jobs)]
    for cp in reads:
        cp.start()
    for cp, _ in through:
        cp.start()
    writes = []
    for (_, low, wide, places), read in zip(jobs, reads):
        read.wait()

        def body(i, carry, low=low, wide=wide):
            row = pl.ds(mo(i * 32, 32), 32)
            wide[row, :] = low[row, :].astype(F32)
            return carry

        lax.fori_loop(0, low.shape[0] // 32, body, 0)
        for place, col in places:
            cp = pltpu.make_async_copy(wide.at[:, col], place, w_sem.at[len(writes)])
            cp.start()
            writes.append(cp)
    for a, b in through:
        a.wait()
        b.start()
    k = 0
    for ref in vec_o:
        blocks = ref.shape[0] // 256
        if ref is vec_o[3]:
            k -= blocks
        for i in range(blocks):
            ref[i * 256 : (i + 1) * 256] = vec[k + i].reshape(256)
        k += blocks
    for cp in writes:
        cp.wait()
    for _, b in through:
        b.wait()


def finish_call(z, pieces):
    n, width, span = z.n, z.d, z.span
    V = pltpu.VMEM
    S = jax.ShapeDtypeStruct
    any_ = pl.BlockSpec(memory_space=pl.ANY)
    vm = pl.BlockSpec(memory_space=pltpu.VMEM)
    rs = z.rs
    outs = [
        S((z.l, width), BF), S((z.l, width), F32), S((rs, 3 * width), F32), S((rs, z.ff), F32),
        S((z.hb * n, width), F32), S((span, width), F32),
        S((3 * width // z.s,), F32), S((z.hb * n,), F32), *[S((rs,), F32)] * 6,
    ]
    shapes = [p.shape for p in pieces[2:6]]
    dma = lambda k: pltpu.SemaphoreType.DMA((k,))
    return pl.pallas_call(
        functools.partial(finish, z),
        out_shape=outs,
        in_specs=[any_] * 6 + [vm],
        out_specs=[any_] * 6 + [vm] * 8,
        scratch_shapes=[
            V((z.l, width), BF), V((z.l, width), F32),
            *[V(s, BF) for s in shapes], *[V(s, F32) for s in shapes],
            dma(4), dma(6 * n + 2), dma(2 * n * (z.s + 4) + 2),
        ],
        compiler_params=pltpu.CompilerParams(vmem_limit_bytes=VMEM_LIMIT),
        name="finish",
    )(*pieces)


def make_fused_body(z):
    def body(
        tokens, in_proj, in_bias, out_proj, out_bias, up_proj, up_bias, down_proj, down_bias,
        first_gain, first_shift, second_gain, second_shift, cotangent,
    ):
        vectors = (in_bias, up_bias, out_bias, down_bias, first_gain, first_shift, second_gain, second_shift)
        pieces = fused_call(z, tokens, cotangent, in_proj, up_proj, out_proj, down_proj, vectors)
        mixed, tgrad, g_in, g_up, g_down, g_out, b_in, b_up, b_out, b_down, *rest = finish_call(
            z, pieces
        )
        return (mixed, tgrad, g_in, b_in, g_out, b_out, g_up, b_up, g_down, b_down, *rest)

    return body


def solution(mesh):
    rows = P(("rep", "shard"), None)
    mat = P("shard", None)
    vec = P("shard")
    in_specs = (rows, mat, vec, mat, vec, mat, vec, mat, vec, vec, vec, vec, vec, rows)
    out_specs = (rows, rows, mat, vec, mat, vec, mat, vec, mat, vec, vec, vec, vec, vec)
    shape = dict(mesh.shape)

    def step(*args):
        tokens, up_proj = args[0], args[5]
        devices = shape["rep"] * shape["shard"]
        z = Sizes(shape, tokens.shape[0] // devices, tokens.shape[1], up_proj.shape[1])
        body = make_fused_body(z) if z.fits() else make_body(shape["shard"])
        return jax.shard_map(
            body, mesh=mesh, in_specs=in_specs, out_specs=out_specs, check_vma=False
        )(*args)

    return step
```

```python
import functools

import jax
import jax.numpy as jnp
import numpy as np
from jax import lax
from jax.experimental import pallas as pl
from jax.experimental.pallas import tpu as pltpu
from jax.sharding import PartitionSpec as P

HEAD_DIM = 64
ROT = 16
EPS = 1e-05
MASKED = -1e30


def rotary_tables(length):
    half = ROT // 2
    inverse = jnp.exp(-jnp.log(10000.0) * (2.0 * jnp.arange(half, dtype=jnp.float32) / ROT))
    angles = jnp.arange(length, dtype=jnp.float32)[:, None] * inverse[None, :]
    return (jnp.cos(angles)[:, None, :], jnp.sin(angles)[:, None, :])


def rotate(values, cosine, sine, sign):
    half = ROT // 2
    first = values[..., :half]
    second = values[..., half:ROT]
    return jnp.concatenate(
        [
            first * cosine - sign * second * sine,
            second * cosine + sign * first * sine,
            values[..., ROT:],
        ],
        axis=-1,
    )


def mm(left, right, dims=((1,), (0,))):
    return lax.dot_general(left, right, (dims, ((), ())), preferred_element_type=jnp.float32)


def make_body(parts):
    def body(
        tokens,
        in_proj,
        in_bias,
        out_proj,
        out_bias,
        up_proj,
        up_bias,
        down_proj,
        down_bias,
        first_gain,
        first_shift,
        second_gain,
        second_shift,
        cotangent,
    ):
        length, width = tokens.shape
        me = lax.axis_index("shard")
        heads = width // parts // HEAD_DIM
        span = width // parts
        rows = in_proj.shape[0]
        hidden = up_bias.shape[0]
        scale = HEAD_DIM ** (-0.5)
        vectors = jnp.concatenate(
            [in_bias, out_bias, down_bias, first_gain, first_shift, second_gain, second_shift]
        )
        vectors = lax.all_gather(vectors, "shard", axis=0).astype(jnp.float32)
        cuts = [in_bias.shape[0]] + [span] * 6
        offsets = [sum(cuts[:i]) for i in range(len(cuts))]
        whole = [vectors[:, o : o + c].reshape(-1) for o, c in zip(offsets, cuts)]
        in_b, out_b, down_b, gain1, shift1, gain2, shift2 = whole
        both = lax.all_gather(jnp.stack([tokens, cotangent]), "shard", axis=1, tiled=True)
        x_all, g_all = both[0], both[1]
        w_in = lax.all_to_all(
            in_proj.reshape(rows, 3, parts, span), "shard", 2, 0, tiled=True
        ).reshape(parts * rows, 3 * span)
        w_up = lax.all_to_all(up_proj, "shard", 1, 0, tiled=True)
        b_in = lax.dynamic_slice_in_dim(in_b.reshape(3, parts, span), me, 1, axis=1).reshape(-1)
        x = x_all.astype(jnp.float32)
        mean = jnp.mean(x, axis=1, keepdims=True)
        cen = x - mean
        inv = lax.rsqrt(jnp.mean(cen * cen, axis=1, keepdims=True) + EPS)
        xhat = cen * inv
        attn_in = (xhat * gain1 + shift1).astype(jnp.bfloat16)
        mlp_in = (xhat * gain2 + shift2).astype(jnp.bfloat16)
        total_rows = x.shape[0]
        qkv = (mm(attn_in, w_in) + b_in).reshape(parts, length, 3, heads, HEAD_DIM)
        cosine, sine = rotary_tables(length)
        query = rotate(qkv[:, :, 0], cosine, sine, 1.0).astype(jnp.bfloat16)
        keys = rotate(qkv[:, :, 1], cosine, sine, 1.0).astype(jnp.bfloat16)
        values = qkv[:, :, 2].astype(jnp.bfloat16)
        causal = jnp.arange(length)[:, None] >= jnp.arange(length)[None, :]

        def ein(eq, a, b):
            return jnp.einsum(eq, a, b, preferred_element_type=jnp.float32)

        scores = jnp.where(causal, ein("sqhd,skhd->shqk", query, keys) * scale, MASKED)
        expo = jnp.exp(scores)
        probs_full = expo / jnp.sum(expo, axis=-1, keepdims=True)
        probs = probs_full.astype(jnp.bfloat16)
        attended = ein("shqk,skhd->sqhd", probs, values).astype(jnp.bfloat16)
        attended = attended.reshape(total_rows, span)
        up = mm(mlp_in, w_up) + up_bias.astype(jnp.float32)
        activated, pull = jax.vjp(lambda t: jax.nn.gelu(t, approximate=False), up)
        activated = activated.astype(jnp.bfloat16)
        partial = mm(attended, out_proj) + mm(activated, down_proj)
        branch = lax.psum_scatter(
            partial.astype(jnp.bfloat16), "shard", scatter_dimension=0, tiled=True
        )
        mixed = (tokens.astype(jnp.float32) + branch.astype(jnp.float32) + out_b + down_b).astype(
            jnp.bfloat16
        )
        grad_att = mm(g_all, out_proj, ((1,), (1,))).astype(jnp.bfloat16)
        grad_att = grad_att.reshape(parts, length, heads, HEAD_DIM)
        grad_act = mm(g_all, down_proj, ((1,), (1,)))
        grad_up = pull(grad_act)[0].astype(jnp.bfloat16)
        d_probs = ein("sqhd,skhd->shqk", grad_att, values)
        d_values = ein("shqk,sqhd->skhd", probs, grad_att)
        inner = jnp.sum(d_probs * probs_full, axis=-1, keepdims=True)
        d_scores = (probs_full * (d_probs - inner)).astype(jnp.bfloat16)
        d_query = ein("shqk,skhd->sqhd", d_scores, keys) * scale
        d_keys = ein("shqk,sqhd->skhd", d_scores, query) * scale
        d_query = rotate(d_query, cosine, sine, -1.0)
        d_keys = rotate(d_keys, cosine, sine, -1.0)
        grad_qkv = jnp.stack([d_query, d_keys, d_values], axis=2).astype(jnp.bfloat16)
        grad_qkv = grad_qkv.reshape(total_rows, 3 * span)
        d1 = mm(grad_qkv, w_in, ((1,), (1,)))
        d2 = mm(grad_up, w_up, ((1,), (1,)))
        scaled = (d1 * gain1 + d2 * gain2).astype(jnp.bfloat16)
        e = lax.psum_scatter(scaled, "shard", scatter_dimension=0, tiled=True).astype(jnp.float32)
        own = lambda a: lax.dynamic_slice_in_dim(a, me * length, length, axis=0)
        xh, rv = own(xhat), own(inv)
        tokens_grad = cotangent.astype(jnp.float32) + rv * (
            e - jnp.mean(e, axis=1, keepdims=True) - xh * jnp.mean(e * xh, axis=1, keepdims=True)
        )
        left = ((0,), (0,))
        dw_in = mm(attn_in, grad_qkv, left).astype(jnp.bfloat16)
        dw_up = mm(mlp_in, grad_up, left).astype(jnp.bfloat16)
        dw_out = mm(attended, g_all, left).astype(jnp.bfloat16)
        dw_down = mm(activated, g_all, left).astype(jnp.bfloat16)
        dw_in, dw_up, dw_out, dw_down = lax.psum((dw_in, dw_up, dw_out, dw_down), "rep")
        dw_in = lax.all_to_all(
            dw_in.reshape(parts * rows, 3, 1, span), "shard", 0, 2, tiled=True
        ).reshape(rows, 3 * width)
        dw_up = lax.all_to_all(dw_up, "shard", 0, 1, tiled=True)
        f32 = jnp.float32
        place = lambda v: lax.dynamic_update_slice_in_dim(
            jnp.zeros((3, parts, span), f32), v.reshape(3, 1, span), me, axis=1
        ).reshape(-1)
        vec = [
            place(jnp.sum(grad_qkv, axis=0, dtype=f32)),
            jnp.sum(cotangent.astype(f32), axis=0),
            jnp.sum(d1 * xhat, axis=0),
            jnp.sum(d1, axis=0),
            jnp.sum(d2 * xhat, axis=0),
            jnp.sum(d2, axis=0),
        ]
        vec = jnp.concatenate([v.reshape(parts, -1) for v in vec], axis=1)
        vec = lax.psum_scatter(vec, "shard", scatter_dimension=0, tiled=True)[0]
        vec, up_vec = lax.psum((vec, jnp.sum(grad_up, axis=0, dtype=f32)), "rep")
        o = in_bias.shape[0]
        bias_grad = vec[o : o + span]
        rest = [vec[o + span * i : o + span * (i + 1)] for i in range(1, 5)]
        return (
            mixed,
            tokens_grad,
            dw_in.astype(f32),
            vec[:o],
            dw_out.astype(f32),
            bias_grad,
            dw_up.astype(f32),
            up_vec,
            dw_down.astype(f32),
            bias_grad,
            *rest,
        )

    return body


BF = jnp.bfloat16
F32 = jnp.float32
MESH = pl.DeviceIdType.MESH
VMEM_LIMIT = 67_000_000
NN = ((1,), (0,))
NT = ((1,), (1,))
TN = ((0,), (0,))
IN, UP, DOWN, OUT = range(4)


class Sizes:
    def __init__(self, mesh_shape, length, width, hidden):
        self.copies = mesh_shape["rep"]
        self.n = self.copies // 2
        self.s = mesh_shape["shard"]
        self.l = length
        self.d = width
        self.ff = hidden
        self.span = width // self.n
        self.hid = hidden // self.n
        self.rs = width // self.s
        self.hb = hidden // self.s // self.n
        self.rows = self.n * length

    def fits(self):
        return (
            self.copies == 8
            and self.s == 4
            and self.rs == 256
            and self.span == 256
            and self.hb == 256
            and self.l % 256 == 0
        )


def rotary_lanes(length):
    half = ROT // 2
    inverse = np.exp(-np.log(10000.0) * (2.0 * np.arange(half) / ROT))
    angles = np.arange(length)[:, None] * inverse[None, :]
    cosine, sine = np.cos(angles), np.sin(angles)
    table = np.zeros((3, length, 128), np.float32)
    table[0] = 1.0
    for start in (0, HEAD_DIM):
        table[0, :, start : start + half] = cosine
        table[0, :, start + half : start + ROT] = cosine
        table[1, :, start : start + half] = -sine
        table[2, :, start + half : start + ROT] = sine
    return table


def dot(left, right, dims=NN):
    return lax.dot_general(left, right, (dims, ((), ())), preferred_element_type=F32)


def mo(value, m):
    return pl.multiple_of(value, m)


def fused(z, *refs):
    (tok, cot, inp, upp, outp, downp) = refs[:6]
    vectors_in, rot = refs[6:14], refs[14]
    (mixed_o, tgrad_o, gin_o, gup_o, gdown_o, gout_o, vec_o) = refs[15:22]
    (
        x_all, g_all, a1, a2, wi, wu, wo, wd, qkv, pt, der, act, att, gatt, gup, gqkv,
        msend, mrecv, mpre, mown, esend, erecv, epre, eown,
        dwi, dwu, dwd, dwo, xri, xru, xrd, xro, zri, zru, zrd, zro, fi, fu, fd, fo,
        vec, va, inb, vfull, vz, vu, vr, mean_r, inv_r, vacc, bin_r, bup_r,
        loc, v_s, v_r, x_s, x_r, g_s, g_r, w_s, w_r, wc_s, wc_r,
        o_s, o_r, oc_s, oc_r, m_s, m_r, e_s, e_r, xs_s, xs_r, zs_s, zs_r,
        ag_s, ag_r, agc_s, agc_r, agl, v1_s, v1_r, v2_s, v2_r,
    ) = refs[22:]
    n, s_n, length, width = z.n, z.s, z.l, z.d
    span, hid, rs, hb = z.span, z.hid, z.rs, z.hb
    iw = 3 * span
    scale = HEAD_DIM**-0.5
    r = lax.axis_index("rep")
    zz = lax.axis_index("shard")
    p = lax.div(r, 2)
    c = lax.rem(r, 2)
    other = 1 - c
    partner = (2 * p + other, zz)
    py, px = lax.div(p, 2), lax.rem(p, 2)
    xn, yn, dg = 2 * py + 1 - px, 2 * (1 - py) + px, 2 * (1 - py) + 1 - px
    dev_x, dev_y = (2 * xn + c, zz), (2 * yn + c, zz)
    zp, zo = lax.div(zz, 2), lax.rem(zz, 2)
    is_end = zp == zo
    inner = zp != zo
    mate = 2 * zp + 1 - zo
    mate_dev = (r, mate)
    far_end, far_inner = 3 * (1 - zp), 2 - zp
    left, right = (r, zz - 1), (r, zz + 1)
    has_left, has_right = zz > 0, zz < s_n - 1

    def rc(src, dst, ss, rr, dev):
        return pltpu.make_async_remote_copy(
            src_ref=src, dst_ref=dst, send_sem=ss, recv_sem=rr, device_id=dev, device_id_type=MESH
        )

    def got(ref, rr):
        rc(ref, ref, rr, rr, partner).wait_recv()

    def seq(ref, s):
        return ref.at[pl.ds(mo(s * length, length), length)]

    sends = []

    def start(copy, cond=None):
        if cond is None:
            copy.start()
        else:
            pl.when(cond)(copy.start)
        sends.append((cond, copy))

    own_rows = pl.ds(mo(zz * rs, rs), rs)
    own_hb = pl.ds(mo(zz * hb, hb), hb)
    local_u = [
        pltpu.make_async_copy(
            upp.at[:, pl.ds(mo(i * (hb * n) + p * hb, hb), hb)],
            wu.at[own_rows, pl.ds(i * hb, hb)],
            loc.at[i],
        )
        for i in range(s_n)
    ]
    local_i = [
        pltpu.make_async_copy(
            inp.at[:, pl.ds(mo(i * width + (p + n * k) * 128, 128), 128)],
            wi.at[own_rows, pl.ds(i * span + k * 128, 128)],
            loc.at[s_n + 2 * i + k],
        )
        for i in range(3)
        for k in range(2)
    ]
    at_loc = s_n + 6
    local_d = pltpu.make_async_copy(
        downp.at[pl.ds(mo(p * hb, hb), hb)], wd.at[own_hb], loc.at[at_loc]
    )
    local_x = pltpu.make_async_copy(tok, seq(x_all, p), loc.at[at_loc + 1])
    local_g = pltpu.make_async_copy(cot, seq(g_all, p), loc.at[at_loc + 2])
    local_o = pltpu.make_async_copy(
        outp.at[pl.ds(mo(px * 128, 128), 128)], wo.at[pl.ds(mo(zp * 128, 128), 128)], loc.at[at_loc + 3]
    )
    at_home = zo == py
    away = jnp.logical_not(at_home)
    for cp in local_i + [local_x] + local_u + [local_g, local_d]:
        cp.start()
    pl.when(at_home)(local_o.start)
    off = 0
    for ref in vectors_in:
        size = ref.shape[0]
        vec[:, off : off + size] = ref[...].astype(F32).reshape(1, size)
        off += size

    barrier = pltpu.get_barrier_semaphore()
    for i in range(1, 2 * n):
        pl.semaphore_signal(
            barrier, 1, device_id=(lax.rem(r + i, 2 * n), zz), device_id_type=MESH
        )
    for i in range(1, s_n):
        pl.semaphore_signal(barrier, 1, device_id=(r, lax.rem(zz + i, s_n)), device_id_type=MESH)
    pl.semaphore_wait(barrier, 2 * n - 1 + s_n - 1)

    def line(i):
        q = lax.rem(zz + i, s_n)
        return q, (r, q)

    def plane_send(src, dst, ss, rr, cond=None):
        start(rc(src(0), dst(p, 0), ss(0), rr(p, 0), dev_x), cond)
        start(rc(src(1), dst(p, 1), ss(1), rr(p, 1), dev_y), cond)
        start(rc(src(1), dst(p, 1), ss(2), rr(p, 1), dev_x), cond)
        start(rc(src(0), dst(p, 0), ss(3), rr(p, 0), dev_y), cond)

    def plane_relay(dst, ss, rr):
        got(dst(xn, 0), rr(xn, 0))
        start(rc(dst(xn, 0), dst(xn, 0), ss(4), rr(xn, 0), dev_y))
        got(dst(yn, 1), rr(yn, 1))
        start(rc(dst(yn, 1), dst(yn, 1), ss(5), rr(yn, 1), dev_x))

    def plane_near(dst, rr):
        got(dst(xn, 1), rr(xn, 1))
        got(dst(yn, 0), rr(yn, 0))

    def plane_far(dst, rr):
        got(dst(dg, 0), rr(dg, 0))
        got(dst(dg, 1), rr(dg, 1))

    lh = length // 2

    def part(ref):
        return lambda q, h: ref.at[pl.ds(mo(q * length + h * lh, lh), lh)]

    def sem1(ref):
        return lambda i: ref.at[i]

    def sem2(ref):
        return lambda q, h: ref.at[q, h]

    def rows_of(ref):
        return lambda h: ref.at[pl.ds(h * lh, lh)]

    for i in range(1, s_n):
        q, dev = line(i)
        start(rc(vec, va.at[zz], v_s.at[i], v_r.at[zz], dev))
    plane_send(rows_of(tok), part(x_all), sem1(x_s), sem2(x_r))

    half, hhalf, ohalf = rs // 2, hb // 2, span // 4
    cuts = {IN: 2, UP: 1, DOWN: 1}

    def piece(t, ref, block):
        rows = block // 2 // cuts[t]
        return lambda q, core, h: ref.at[pl.ds(mo(q * block + core * (block // 2) + h * rows, rows), rows)]

    u_piece, d_piece, i_piece = piece(UP, wu, rs), piece(DOWN, wd, hb), piece(IN, wi, rs)

    def own_sends(t, get):
        for h in range(cuts[t]):
            mine = get(zz, c, h)
            start(rc(mine, mine, w_s.at[t, h, 0], w_r.at[t, h, zz], left), has_left)
            start(rc(mine, mine, w_s.at[t, h, 1], w_r.at[t, h, zz], right), has_right)

    def relay(t, get, d, who):
        def take(h, q, has, onward, more, slot):
            ref = get(q, c, h)

            @pl.when(has)
            def _():
                got(ref, w_r.at[t, h, q])

            start(
                rc(ref, ref, w_s.at[t, h, slot], w_r.at[t, h, q], onward),
                jnp.logical_and(has, more),
            )
            start(rc(ref, ref, wc_s.at[t, h, slot], wc_r.at[t, h, q], partner), has)

        for h in range(cuts[t]):
            from_left = jnp.logical_and(who, zz - d >= 0)
            from_right = jnp.logical_and(who, zz + d <= s_n - 1)
            take(h, zz - d, from_left, right, has_right, 2 * d)
            take(h, zz + d, from_right, left, has_left, 2 * d + 1)

    def relay_done(t, get):
        for h in range(cuts[t]):
            for i in range(1, s_n):
                q, _ = line(i)
                got(get(q, other, h), wc_r.at[t, h, q])

    for cp in local_i:
        cp.wait()
    own_sends(IN, i_piece)

    for i in range(1, s_n):
        q, dev = line(i)
        got(va.at[q], v_r.at[q])
    va[zz] = vec[...]
    n_in = 3 * width // s_n
    n_up = hb * n
    at_up = n_in
    at_rest = n_in + n_up

    def vector(i):
        off = at_rest + i * rs
        return jnp.concatenate([va[q, :, off : off + rs] for q in range(s_n)], axis=1)

    out_b, down_b, gain1, shift1, gain2, shift2 = [vector(i) for i in range(6)]
    for q in range(s_n):
        inb[:, q * n_in : (q + 1) * n_in] = va[q, :, :n_in]

    def norm(s):
        step = 32

        def body(i, carry):
            row = pl.ds(mo(s * length + i * step, step), step)
            xv = x_all[row, :].astype(F32)
            mu = jnp.mean(xv, axis=1, keepdims=True)
            cen = xv - mu
            inv = lax.rsqrt(jnp.mean(cen * cen, axis=1, keepdims=True) + EPS)
            xh = cen * inv
            a1[row, :] = (xh * gain1 + shift1).astype(BF)
            a2[row, :] = (xh * gain2 + shift2).astype(BF)
            mean_r[row, :] = mu
            inv_r[row, :] = inv
            return carry

        lax.fori_loop(0, length // step, body, 0)

    table = [rot[i] for i in range(3)]

    def turn(t, sign):
        fwd = pltpu.roll(t, 128 - ROT // 2, 1)
        back = pltpu.roll(t, ROT // 2, 1)
        return t * table[0] + (fwd * table[1] + back * table[2]) * sign

    def turn_of(k):
        return jnp.where(k == 0, p, jnp.where(k == 1, xn, jnp.where(k == 2, yn, dg)))

    def qkv_block(k, carry):
        row = pl.ds(mo(turn_of(k) * length, length), length)
        left_a = a1[row, :]
        for i in range(3):
            v = dot(left_a, wi[:, i * span : (i + 1) * span])
            for h in range(2):
                bias = inb[:, pl.ds(mo(i * width + (p + n * h) * 128, 128), 128)]
                cut = v[:, h * 128 : (h + 1) * 128] + bias
                if i < 2:
                    cut = turn(cut, 1.0)
                qkv[row, i * span + h * 128 : i * span + (h + 1) * 128] = cut.astype(BF)
        return carry

    relay(IN, i_piece, 1, inner)
    local_x.wait()
    norm(p)
    relay(IN, i_piece, 2, inner)
    for cp in local_u:
        cp.wait()
    own_sends(UP, u_piece)
    plane_relay(part(x_all), sem1(x_s), sem2(x_r))
    plane_send(rows_of(cot), part(g_all), sem1(g_s), sem2(g_r))
    plane_near(part(x_all), sem2(x_r))
    norm(xn)
    norm(yn)
    relay(UP, u_piece, 1, inner)
    for d in range(1, s_n):
        relay(IN, i_piece, d, is_end)
    relay_done(IN, i_piece)
    lax.fori_loop(0, 3, qkv_block, 0)
    relay(UP, u_piece, 2, inner)
    local_d.wait()
    own_sends(DOWN, d_piece)
    def o_piece(block, core):
        return wo.at[pl.ds(mo(block * 128 + core * ohalf, ohalf), ohalf)]

    pl.when(at_home)(local_o.wait)
    near_first = (mate_dev, (r, far_inner), (r, far_end))
    for i, dev in enumerate(near_first):
        start(rc(o_piece(zp, c), o_piece(zp, c), o_s.at[i], o_r.at[zp], dev), at_home)
    plane_far(part(x_all), sem2(x_r))
    norm(dg)
    lax.fori_loop(3, n, qkv_block, 0)
    plane_relay(part(g_all), sem1(g_s), sem2(g_r))

    lane = lax.broadcasted_iota(jnp.int32, (1, 128), 1)
    first = lane < HEAD_DIM
    masks = [first.astype(F32).astype(BF), (1.0 - first.astype(F32)).astype(BF)]
    pairs = span // 128

    def att_forward(idx, carry):
        s = lax.div(idx, pairs)
        pr = lax.rem(idx, pairs)
        row = pl.ds(mo(s * length, length), length)
        q2 = qkv[row, pl.ds(mo(pr * 128, 128), 128)]
        k2 = qkv[row, pl.ds(mo(span + pr * 128, 128), 128)]
        v2 = qkv[row, pl.ds(mo(2 * span + pr * 128, 128), 128)]
        key_i = lax.broadcasted_iota(jnp.int32, (length, length), 0)
        query_i = lax.broadcasted_iota(jnp.int32, (length, length), 1)
        found = []
        for h in range(2):
            st = dot(k2, q2 * masks[h], NT) * scale
            ex = jnp.exp(jnp.where(key_i <= query_i, st, MASKED))
            pr_t = ex / jnp.sum(ex, axis=0, keepdims=True)
            pt[idx * 2 + h] = pr_t
            found.append(dot(pr_t.astype(BF), v2, TN))
        att[row, pl.ds(mo(pr * 128, 128), 128)] = jnp.where(first, found[0], found[1]).astype(BF)
        return carry

    lax.fori_loop(0, n * pairs // 2, att_forward, 0)
    relay(DOWN, d_piece, 1, inner)
    lax.fori_loop(n * pairs // 2, n * pairs, att_forward, 0)
    for d in range(1, s_n):
        relay(UP, u_piece, d, is_end)
    relay_done(UP, u_piece)

    def up_block(s, carry):
        row = pl.ds(mo(s * length, length), length)
        left_a = a2[row, :]
        for j in range(s_n):
            col = pl.ds(j * hb, hb)
            bias = va[j, :, pl.ds(mo(at_up + p * hb, hb), hb)]
            u = dot(left_a, wu[:, j * hb : (j + 1) * hb]) + bias
            phi = 0.5 * (1.0 + lax.erf(u * 0.7071067811865476))
            act[row, col] = (u * phi).astype(BF)
            der[row, col] = phi + u * (0.3989422804014327 * jnp.exp(-0.5 * u * u))
        return carry

    lax.fori_loop(0, n, up_block, 0)
    relay(DOWN, d_piece, 2, inner)

    def exchange(t, dw, xr, block_half):
        src = dw.at[:, pl.ds(mo(other * block_half, block_half), block_half)]
        start(rc(src, xr, xs_s.at[t], xs_r.at[t], partner))

    def core_sum(t, dw, xr, block_half):
        mine = pl.ds(mo(c * block_half, block_half), block_half)
        got(xr, xs_r.at[t])

        def body(q, carry):
            xr[q] = (dw[q, mine].astype(F32) + xr[q].astype(F32)).astype(BF)
            return carry

        lax.fori_loop(0, dw.shape[0], body, 0)

    def pair_sum(t, dw, xr, zr, block_half):
        core_sum(t, dw, xr, block_half)
        start(rc(xr.at[far_end], zr.at[2], zs_s.at[t, 0], zs_r.at[t, 2], mate_dev), is_end)
        start(rc(xr.at[far_inner], zr.at[3], zs_s.at[t, 1], zs_r.at[t, 3], mate_dev), is_end)
        start(rc(xr.at[mate], zr.at[0], zs_s.at[t, 2], zs_r.at[t, 0], mate_dev))

    def pass_on(t, xr, zr):
        @pl.when(inner)
        def _():
            for slot, q in ((2, far_end), (3, far_inner)):
                got(zr.at[slot], zs_r.at[t, slot])
                xr[q] = (xr[q].astype(F32) + zr[slot].astype(F32)).astype(BF)
                rc(xr.at[q], zr.at[1], zs_s.at[t, slot - 2], zs_r.at[t, 1], (r, q)).start()

        for slot, q in ((2, far_end), (3, far_inner)):
            cp = rc(xr.at[q], zr.at[1], zs_s.at[t, slot - 2], zs_r.at[t, 1], (r, q))
            sends.append((inner, cp))

    def line_sum(t, xr, zr, fin):
        got(zr.at[0], zs_r.at[t, 0])
        got(zr.at[1], zs_r.at[t, 1])
        total = xr[zz].astype(F32) + zr[0].astype(F32) + zr[1].astype(F32)
        fin[...] = total.astype(BF)

    outs_of = {IN: (gin_o, fi), UP: (gup_o, fu), DOWN: (gdown_o, fd)}

    def area(t):
        o = outs_of[t][0]
        rows = o.shape[2] // 2
        return lambda q, h: o.at[q, c, pl.ds(h * rows, rows)]

    def fin_half(t):
        fin = outs_of[t][1]
        rows = fin.shape[0] // 2
        return lambda h: fin.at[pl.ds(h * rows, rows)]

    def ag1(t):
        return lambda i: ag_s.at[t, i]

    def ag2(t):
        return lambda q, h: ag_r.at[t, q, h]

    local_out = []

    def spread(t):
        o, fin = outs_of[t]
        plane_send(fin_half(t), area(t), ag1(t), ag2(t))
        start(rc(fin, o.at[p, c], agc_s.at[t, 0], agc_r.at[t, p], partner))
        cp = pltpu.make_async_copy(fin, o.at[p, c], agl.at[t])
        cp.start()
        local_out.append((None, cp))

    def spread_relay(t):
        plane_relay(area(t), ag1(t), ag2(t))

    def spread_near(t):
        o = outs_of[t][0]
        plane_near(area(t), ag2(t))
        start(rc(o.at[xn, c], o.at[xn, c], agc_s.at[t, 1], agc_r.at[t, xn], partner))
        start(rc(o.at[yn, c], o.at[yn, c], agc_s.at[t, 2], agc_r.at[t, yn], partner))

    def spread_far(t):
        o = outs_of[t][0]
        plane_far(area(t), ag2(t))
        start(rc(o.at[dg, c], o.at[dg, c], agc_s.at[t, 3], agc_r.at[t, dg], partner))

    def spread_end(t):
        o = outs_of[t][0]
        for i in range(n):
            q = lax.rem(p + i, n)
            got(o.at[q, other], agc_r.at[t, q])

    local_g.wait()
    plane_near(part(g_all), sem2(g_r))
    plane_far(part(g_all), sem2(g_r))

    for j in range(s_n):
        dwd[j] = dot(act[:, j * hb : (j + 1) * hb], g_all[...], TN).astype(BF)
    exchange(DOWN, dwd, xrd, hhalf)
    dwo_all = dot(att[...], g_all[...], TN).astype(BF)
    for i in range(2):
        dwo[i] = dwo_all[i * 128 : (i + 1) * 128]
    exchange(OUT, dwo, xro, ohalf)
    pair_sum(DOWN, dwd, xrd, zrd, hhalf)
    core_sum(OUT, dwo, xro, ohalf)
    near_b, far_b = zp, 1 - zp
    start(rc(xro.at[near_b], zro.at[0], zs_s.at[OUT, 0], zs_r.at[OUT, 0], mate_dev), away)
    start(rc(xro.at[far_b], zro.at[2], zs_s.at[OUT, 1], zs_r.at[OUT, 2], mate_dev), is_end)

    def o_take(block, cond):
        @pl.when(cond)
        def _():
            got(o_piece(block, c), o_r.at[block])

        start(
            rc(o_piece(block, c), o_piece(block, c), oc_s.at[block], oc_r.at[block], partner), cond
        )

    def o_done(block, cond):
        @pl.when(cond)
        def _():
            got(o_piece(block, other), oc_r.at[block])

    always = zz >= 0
    o_take(near_b, away)
    o_take(far_b, always)
    o_done(near_b, away)
    o_done(far_b, always)

    bup_r[...] = jnp.zeros_like(bup_r)
    bin_r[...] = jnp.zeros_like(bin_r)

    def grad_att_block(s, carry):
        row = pl.ds(mo(s * length, length), length)
        gatt[row, :] = dot(g_all[row, :], wo[...], NT).astype(BF)
        return carry

    lax.fori_loop(0, n, grad_att_block, 0)

    def att_backward(idx, carry):
        s = lax.div(idx, pairs)
        pr = lax.rem(idx, pairs)
        row = pl.ds(mo(s * length, length), length)
        q_col = pl.ds(mo(pr * 128, 128), 128)
        k_col = pl.ds(mo(span + pr * 128, 128), 128)
        v_col = pl.ds(mo(2 * span + pr * 128, 128), 128)
        q2, k2, v2 = qkv[row, q_col], qkv[row, k_col], qkv[row, v_col]
        g2 = gatt[row, q_col]
        dq, dk, dv = [], [], []
        for h in range(2):
            pr_t = pt[idx * 2 + h]
            dp = dot(v2, g2 * masks[h], NT)
            total = jnp.sum(dp * pr_t, axis=0, keepdims=True)
            ds = (pr_t * (dp - total)).astype(BF)
            dv.append(dot(pr_t.astype(BF), g2))
            dk.append(dot(ds, q2))
            dq.append(dot(ds, k2, TN))
        dqv = turn(jnp.where(first, dq[0], dq[1]) * scale, -1.0).astype(BF)
        dkv = turn(jnp.where(first, dk[0], dk[1]) * scale, -1.0).astype(BF)
        dvv = jnp.where(first, dv[0], dv[1]).astype(BF)
        for col, val in ((q_col, dqv), (k_col, dkv), (v_col, dvv)):
            gqkv[row, col] = val
            bin_r[:, col] += jnp.sum(val.astype(F32), axis=0, keepdims=True)
        return carry

    lax.fori_loop(0, n * pairs, att_backward, 0)

    for j in range(s_n):
        dwi[j] = dot(a1[:, j * rs : (j + 1) * rs], gqkv[...], TN).astype(BF)
    exchange(IN, dwi, xri, half)
    for d in range(1, s_n):
        relay(DOWN, d_piece, d, is_end)
    relay_done(DOWN, d_piece)

    def shares(send, pre, ss, rr, k):
        @pl.when(k == 0)
        def _():
            for h, dev in ((0, dev_x), (1, dev_y)):
                rc(send.at[0, pl.ds(h * lh, lh)], pre.at[h], ss.at[h], rr.at[h], dev).start()

    def shares_on(send, recv, pre, ss, rr):
        for k, h, dev in ((1, 1, dev_x), (2, 0, dev_y)):
            got(pre.at[h], rr.at[h])
            row = pl.ds(h * lh, lh)
            send[k, row] = (send[k, row].astype(F32) + pre[h].astype(F32)).astype(BF)
            start(rc(send.at[k], recv.at[k - 1], ss.at[k + 1], rr.at[k + 1], dev))

    def shares_left(send, pre, ss, rr):
        for h, dev in ((0, dev_x), (1, dev_y)):
            rc(send.at[0, pl.ds(h * lh, lh)], pre.at[h], ss.at[h], rr.at[h], dev).wait_send()

    def share_of(k):
        return jnp.where(k == 0, dg, jnp.where(k == 1, xn, jnp.where(k == 2, yn, p)))

    def out_block(k, carry):
        row = pl.ds(mo(share_of(k) * length, length), length)
        for j in range(width // 256):
            col = slice(j * 256, (j + 1) * 256)
            v = dot(att[row, :], wo[:, col]) + dot(act[row, :], wd[:, col])
            msend[k, :, col] = v.astype(BF)
            mown[:, col] = v
        shares(msend, mpre, m_s, m_r, k)
        return carry

    lax.fori_loop(0, 2, out_block, 0)
    pair_sum(IN, dwi, xri, zri, half)
    lax.fori_loop(2, n, out_block, 0)
    pass_on(DOWN, xrd, zrd)

    def grad_up_block(s, carry):
        row = pl.ds(mo(s * length, length), length)
        gs = g_all[row, :]
        for j in range(s_n):
            col = pl.ds(j * hb, hb)
            gu = (dot(gs, wd[j * hb : (j + 1) * hb, :], NT) * der[row, col]).astype(BF)
            gup[row, col] = gu
            bup_r[:, col] += jnp.sum(gu.astype(F32), axis=0, keepdims=True)
        return carry

    lax.fori_loop(0, 2, grad_up_block, 0)
    shares_on(msend, mrecv, mpre, m_s, m_r)
    lax.fori_loop(2, n, grad_up_block, 0)
    for j in range(s_n):
        dwu[j] = dot(a2[:, j * rs : (j + 1) * rs], gup[...], TN).astype(BF)
    exchange(UP, dwu, xru, half)

    vacc[...] = jnp.zeros_like(vacc)

    def in_block(k, carry):
        row = pl.ds(mo(share_of(k) * length, length), length)
        gq = gqkv[row, :]
        gu = gup[row, :]
        mu = mean_r[row, :]
        inv = inv_r[row, :]
        for j in range(s_n):
            col = slice(j * rs, (j + 1) * rs)
            d1 = dot(gq, wi[col, :], NT)
            d2 = dot(gu, wu[col, :], NT)
            xh = (x_all[row, col].astype(F32) - mu) * inv
            vacc[0, :, col] += jnp.sum(d1 * xh, axis=0, keepdims=True)
            vacc[1, :, col] += jnp.sum(d1, axis=0, keepdims=True)
            vacc[2, :, col] += jnp.sum(d2 * xh, axis=0, keepdims=True)
            vacc[3, :, col] += jnp.sum(d2, axis=0, keepdims=True)
            e = d1 * gain1[:, col] + d2 * gain2[:, col]
            esend[k, :, col] = e.astype(BF)
            eown[:, col] = e
        shares(esend, epre, e_s, e_r, k)
        return carry

    lax.fori_loop(0, 1, in_block, 0)
    pair_sum(UP, dwu, xru, zru, half)
    lax.fori_loop(1, n, in_block, 0)

    on = rc(xro.at[far_b], zro.at[1], zs_s.at[OUT, 2], zs_r.at[OUT, 1], (r, 2 * (1 - zp) + py))

    @pl.when(inner)
    def _():
        got(zro.at[2], zs_r.at[OUT, 2])
        xro[far_b] = (xro[far_b].astype(F32) + zro[2].astype(F32)).astype(BF)
        on.start()

    sends.append((inner, on))
    line_sum(DOWN, xrd, zrd, fd)
    spread(DOWN)
    pass_on(IN, xri, zri)

    shares_on(esend, erecv, epre, e_s, e_r)

    slots = vfull.shape[0] // s_n
    vfull[...] = jnp.zeros_like(vfull)
    per = n_in // 128
    for i in range(3):
        for h in range(2):
            b = i * 2 * n + p + n * h
            col = slice(i * span + h * 128, i * span + (h + 1) * 128)
            vfull[lax.div(b, per) * slots + lax.rem(b, per)] = bin_r[:, col]
    at_g = per + 2 * n
    for q in range(s_n):
        for h in range(2):
            up_col = slice(q * hb + h * 128, q * hb + (h + 1) * 128)
            vfull[q * slots + per + 2 * p + h] = bup_r[:, up_col]
            col = slice(q * rs + h * 128, q * rs + (h + 1) * 128)
            g_own = g_all[pl.ds(mo(p * length, length), length), col].astype(F32)
            vfull[q * slots + at_g + h] = jnp.sum(g_own, axis=0, keepdims=True)
            for i in range(4):
                vfull[q * slots + at_g + 2 + 2 * i + h] = vacc[i, :, col]
    for i in range(1, s_n):
        q, dev = line(i)
        start(rc(vfull.at[pl.ds(q * slots, slots)], vz.at[zz], v1_s.at[i], v1_r.at[zz], dev))

    @pl.when(at_home)
    def _():
        got(zro.at[0], zs_r.at[OUT, 0])
        got(zro.at[1], zs_r.at[OUT, 1])
        total = xro[near_b].astype(F32) + zro[0].astype(F32) + zro[1].astype(F32)
        fo[...] = total.astype(BF)

    oq = ohalf // 2

    def o_whole(q):
        return gout_o.at[lax.rem(q, 2), c]

    def o_area(q, h):
        return gout_o.at[lax.rem(q, 2), c, pl.ds(h * oq, oq)]

    plane_send(lambda h: fo.at[pl.ds(h * oq, oq)], o_area, ag1(OUT), ag2(OUT), at_home)
    start(rc(fo, o_whole(p), agc_s.at[OUT, 0], agc_r.at[OUT, p], partner), at_home)
    cp = pltpu.make_async_copy(fo, o_whole(p), agl.at[OUT])
    pl.when(at_home)(cp.start)
    local_out.append((at_home, cp))

    got(mrecv.at[0], m_r.at[2])
    got(mrecv.at[1], m_r.at[3])

    def mixed_rows(i, carry):
        step = 32
        row = pl.ds(mo(i * step, step), step)
        xv = x_all[pl.ds(mo(p * length + i * step, step), step), :].astype(F32)
        t = mown[row, :] + mrecv[0, row, :].astype(F32) + mrecv[1, row, :].astype(F32)
        mixed_o[row, :] = (xv + t + out_b + down_b).astype(BF)
        return carry

    lax.fori_loop(0, length // 32, mixed_rows, 0)

    spread_relay(DOWN)
    line_sum(IN, xri, zri, fi)
    spread(IN)
    pass_on(UP, xru, zru)

    total = [vfull[zz * slots + k] for k in range(slots)]
    for i in range(1, s_n):
        q, dev = line(i)
        got(vz.at[q], v1_r.at[q])
        total = [t + vz[q, k] for k, t in enumerate(total)]
    for k in range(slots):
        vu[k] = total[k]
        vr[r, k] = total[k]
    for i in range(1, 2 * n):
        start(rc(vu, vr.at[r], v2_s.at[i], v2_r.at[r], (lax.rem(r + i, 2 * n), zz)))

    def o_got(q, h, cond):
        @pl.when(cond)
        def _():
            got(o_area(q, h), ag_r.at[OUT, q, h])

    o_got(xn, 0, at_home)
    start(rc(o_area(xn, 0), o_area(xn, 0), ag_s.at[OUT, 4], ag_r.at[OUT, xn, 0], dev_y), at_home)
    o_got(yn, 1, away)
    start(rc(o_area(yn, 1), o_area(yn, 1), ag_s.at[OUT, 5], ag_r.at[OUT, yn, 1], dev_x), away)
    spread_near(DOWN)
    spread_far(DOWN)
    spread_relay(IN)

    line_sum(UP, xru, zru, fu)
    spread(UP)

    got(erecv.at[0], e_r.at[2])
    got(erecv.at[1], e_r.at[3])

    def tgrad_rows(i, carry):
        step = 32
        row = pl.ds(mo(i * step, step), step)
        far = pl.ds(mo(p * length + i * step, step), step)
        inv = inv_r[far, :]
        xh = (x_all[far, :].astype(F32) - mean_r[far, :]) * inv
        e = eown[row, :] + erecv[0, row, :].astype(F32) + erecv[1, row, :].astype(F32)
        m0 = jnp.mean(e, axis=1, keepdims=True)
        m1 = jnp.mean(e * xh, axis=1, keepdims=True)
        tgrad_o[row, :] = g_all[far, :].astype(F32) + inv * (e - m0 - xh * m1)
        return carry

    lax.fori_loop(0, length // 32, tgrad_rows, 0)

    o_got(xn, 1, at_home)
    start(rc(o_whole(xn), o_whole(xn), agc_s.at[OUT, 1], agc_r.at[OUT, xn], partner), at_home)
    o_got(yn, 0, away)
    start(rc(o_whole(yn), o_whole(yn), agc_s.at[OUT, 2], agc_r.at[OUT, yn], partner), away)
    o_got(dg, 0, away)
    o_got(dg, 1, away)
    start(rc(o_whole(dg), o_whole(dg), agc_s.at[OUT, 3], agc_r.at[OUT, dg], partner), away)

    for i in range(1, 2 * n):
        q = lax.rem(r + i, 2 * n)
        got(vr.at[q], v2_r.at[q])
    for k in range(slots):
        t = vr[0, k]
        for q in range(1, 2 * n):
            t = t + vr[q, k]
        vec_o[k] = t
    spread_near(IN)
    spread_far(IN)
    spread_relay(UP)
    spread_near(UP)
    spread_far(UP)
    for t in (DOWN, IN, UP):
        spread_end(t)
    for q, cond in ((p, at_home), (xn, at_home), (yn, away), (dg, away)):

        @pl.when(cond)
        def _():
            got(gout_o.at[lax.rem(q, 2), other], agc_r.at[OUT, q])

    for cond, cp in local_out:
        if cond is None:
            cp.wait()
        else:
            pl.when(cond)(cp.wait)
    shares_left(msend, mpre, m_s, m_r)
    shares_left(esend, epre, e_s, e_r)
    for cond, cp in sends:
        if cond is None:
            cp.wait_send()
        else:
            pl.when(cond)(cp.wait_send)


def fused_call(z, tok, cot, inp, upp, outp, downp, vectors):
    n, s_n, length, width, span, hid = z.n, z.s, z.l, z.d, z.span, z.hid
    rs, hb, rows = z.rs, z.hb, z.rows
    iw = 3 * span
    nv = sum(v.shape[0] for v in vectors)
    slots = (3 * width // s_n + hb * n + 5 * rs) // 128
    V = pltpu.VMEM
    dma = lambda *shape: pltpu.SemaphoreType.DMA(shape)
    share = [
        V((n, length, width), BF), V((2, length, width), BF), V((2, length // 2, width), BF),
        V((length, width), F32),
    ]
    halves = [
        V((s_n, rs // 2, iw), BF), V((s_n, rs // 2, hid), BF), V((s_n, hb // 2, width), BF),
    ]
    scratch = [
        *[V((rows, width), BF)] * 4,
        V((width, iw), BF), V((width, hid), BF), V((span, width), BF), V((hid, width), BF),
        V((rows, iw), BF), V((n * span // HEAD_DIM, length, length), F32),
        V((rows, hid), F32), V((rows, hid), BF), V((rows, span), BF),
        V((rows, span), BF), V((rows, hid), BF), V((rows, iw), BF),
        *share, *share,
        V((s_n, rs, iw), BF), V((s_n, rs, hid), BF), V((s_n, hb, width), BF), V((2, span // 2, width), BF),
        *halves, V((2, span // 4, width), BF),
        *halves, V((3, span // 4, width), BF),
        V((rs // 2, iw), BF), V((rs // 2, hid), BF), V((hb // 2, width), BF), V((span // 4, width), BF),
        V((1, nv), F32), V((s_n, 1, nv), F32), V((1, 3 * width), F32), V((s_n * slots, 1, 128), F32),
        V((s_n, slots, 1, 128), F32), V((slots, 1, 128), F32), V((2 * n, slots, 1, 128), F32),
        V((rows, 1), F32), V((rows, 1), F32), V((4, 1, width), F32), V((1, iw), F32), V((1, hid), F32),
        dma(s_n + 10), dma(s_n), dma(s_n), dma(6), dma(n, 2), dma(6), dma(n, 2),
        dma(3, 2, 2 * s_n), dma(3, 2, s_n), dma(3, 2, 2 * s_n), dma(3, 2, s_n),
        dma(3), dma(2), dma(2), dma(2),
        dma(n), dma(n), dma(n), dma(n), dma(4), dma(4), dma(4, 3), dma(4, 4),
        dma(4, 6), dma(4, n, 2), dma(4, n), dma(4, n), dma(4),
        dma(s_n), dma(s_n), dma(2 * n), dma(2 * n),
    ]
    any_ = pl.BlockSpec(memory_space=pl.ANY)
    vm = pl.BlockSpec(memory_space=pltpu.VMEM)
    outs = [
        jax.ShapeDtypeStruct((length, width), BF),
        jax.ShapeDtypeStruct((length, width), F32),
        jax.ShapeDtypeStruct((n, 2, rs // 2, iw), BF),
        jax.ShapeDtypeStruct((n, 2, rs // 2, hid), BF),
        jax.ShapeDtypeStruct((n, 2, hb // 2, width), BF),
        jax.ShapeDtypeStruct((2, 2, span // 4, width), BF),
        jax.ShapeDtypeStruct((slots, 1, 128), F32),
    ]
    return pl.pallas_call(
        functools.partial(fused, z),
        out_shape=outs,
        in_specs=[any_] * 6 + [vm] * 9,
        out_specs=[vm, vm, any_, any_, any_, any_, vm],
        scratch_shapes=scratch,
        compiler_params=pltpu.CompilerParams(
            collective_id=0, has_side_effects=True, vmem_limit_bytes=VMEM_LIMIT
        ),
        name="block_step",
    )(tok, cot, inp, upp, outp, downp, *vectors, jnp.asarray(rotary_lanes(length)))


def finish(z, *refs):
    mixed, tgrad, g_in, g_up, g_down, g_out, vec = refs[:7]
    mixed_o, tgrad_o, in_o, up_o, down_o, out_o = refs[7:13]
    vec_o = refs[13:21]
    m_v, t_v, bi, bu, bd, bo, fi, fu, fd, fo, m_sem, r_sem, w_sem = refs[21:]
    n, s_n, width, span, hb, rs = z.n, z.s, z.d, z.span, z.hb, z.rs
    half = rs // 2
    jobs = []
    for q in range(n):
        for core in range(2):
            row = slice(core * half, (core + 1) * half)
            jobs.append((g_up.at[q, core], bu.at[q, core], fu.at[q, core], [
                (up_o.at[row, k * hb * n + q * hb : k * hb * n + (q + 1) * hb], slice(k * hb, (k + 1) * hb))
                for k in range(s_n)
            ]))
    for q in range(n):
        for core in range(2):
            start = q * hb + core * (hb // 2)
            jobs.append((g_down.at[q, core], bd.at[q, core], fd.at[q, core], [
                (down_o.at[start : start + hb // 2], slice(None)),
            ]))
    for q in range(n):
        for core in range(2):
            row = slice(core * half, (core + 1) * half)
            jobs.append((g_in.at[q, core], bi.at[q, core], fi.at[q, core], [
                (
                    in_o.at[row, k * width + (q + n * h) * 128 : k * width + (q + n * h + 1) * 128],
                    slice(k * span + h * 128, k * span + (h + 1) * 128),
                )
                for k in range(3)
                for h in range(2)
            ]))
    for j in range(2):
        for core in range(2):
            start = (2 * j + core) * (span // 4)
            jobs.append((g_out.at[j, core], bo.at[j, core], fo.at[j, core], [
                (out_o.at[start : start + span // 4], slice(None)),
            ]))
    through = [
        (pltpu.make_async_copy(a, b, m_sem.at[2 * i]), pltpu.make_async_copy(b, o, m_sem.at[2 * i + 1]))
        for i, (a, b, o) in enumerate(((mixed, m_v, mixed_o), (tgrad, t_v, tgrad_o)))
    ]
    reads = [pltpu.make_async_copy(src, dst, r_sem.at[i]) for i, (src, dst, _, _) in enumerate(jobs)]
    for cp in reads:
        cp.start()
    for cp, _ in through:
        cp.start()
    writes = []
    for (_, low, wide, places), read in zip(jobs, reads):
        read.wait()

        def body(i, carry, low=low, wide=wide):
            row = pl.ds(mo(i * 32, 32), 32)
            wide[row, :] = low[row, :].astype(F32)
            return carry

        lax.fori_loop(0, low.shape[0] // 32, body, 0)
        for place, col in places:
            cp = pltpu.make_async_copy(wide.at[:, col], place, w_sem.at[len(writes)])
            cp.start()
            writes.append(cp)
    for a, b in through:
        a.wait()
        b.start()
    k = 0
    for ref in vec_o:
        blocks = ref.shape[0] // 128
        if ref is vec_o[3]:
            k -= blocks
        for i in range(blocks):
            ref[i * 128 : (i + 1) * 128] = vec[k + i].reshape(128)
        k += blocks
    for cp in writes:
        cp.wait()
    for _, b in through:
        b.wait()


def finish_call(z, pieces):
    n, width, span = z.n, z.d, z.span
    V = pltpu.VMEM
    S = jax.ShapeDtypeStruct
    any_ = pl.BlockSpec(memory_space=pl.ANY)
    vm = pl.BlockSpec(memory_space=pltpu.VMEM)
    rs = z.rs
    outs = [
        S((z.l, width), BF), S((z.l, width), F32), S((rs, 3 * width), F32), S((rs, z.ff), F32),
        S((z.hb * n, width), F32), S((span, width), F32),
        S((3 * width // z.s,), F32), S((z.hb * n,), F32), *[S((rs,), F32)] * 6,
    ]
    shapes = [p.shape for p in pieces[2:6]]
    dma = lambda k: pltpu.SemaphoreType.DMA((k,))
    return pl.pallas_call(
        functools.partial(finish, z),
        out_shape=outs,
        in_specs=[any_] * 6 + [vm],
        out_specs=[any_] * 6 + [vm] * 8,
        scratch_shapes=[
            V((z.l, width), BF), V((z.l, width), F32),
            *[V(s, BF) for s in shapes], *[V(s, F32) for s in shapes],
            dma(4), dma(6 * n + 4), dma(2 * n * (z.s + 7) + 4),
        ],
        compiler_params=pltpu.CompilerParams(vmem_limit_bytes=VMEM_LIMIT),
        name="finish",
    )(*pieces)


def make_fused_body(z):
    def body(
        tokens, in_proj, in_bias, out_proj, out_bias, up_proj, up_bias, down_proj, down_bias,
        first_gain, first_shift, second_gain, second_shift, cotangent,
    ):
        vectors = (in_bias, up_bias, out_bias, down_bias, first_gain, first_shift, second_gain, second_shift)
        pieces = fused_call(z, tokens, cotangent, in_proj, up_proj, out_proj, down_proj, vectors)
        mixed, tgrad, g_in, g_up, g_down, g_out, b_in, b_up, b_out, b_down, *rest = finish_call(
            z, pieces
        )
        return (mixed, tgrad, g_in, b_in, g_out, b_out, g_up, b_up, g_down, b_down, *rest)

    return body


def solution(mesh):
    rows = P(("rep", "shard"), None)
    mat = P("shard", None)
    vec = P("shard")
    in_specs = (rows, mat, vec, mat, vec, mat, vec, mat, vec, vec, vec, vec, vec, rows)
    out_specs = (rows, rows, mat, vec, mat, vec, mat, vec, mat, vec, vec, vec, vec, vec)
    shape = dict(mesh.shape)

    def step(*args):
        tokens, up_proj = args[0], args[5]
        devices = shape["rep"] * shape["shard"]
        z = Sizes(shape, tokens.shape[0] // devices, tokens.shape[1], up_proj.shape[1])
        body = make_fused_body(z) if z.fits() else make_body(shape["shard"])
        return jax.shard_map(
            body, mesh=mesh, in_specs=in_specs, out_specs=out_specs, check_vma=False
        )(*args)

    return step
```

```python
import functools

import jax
import jax.numpy as jnp
import numpy as np
from jax import lax
from jax.experimental import pallas as pl
from jax.experimental.pallas import tpu as pltpu
from jax.sharding import PartitionSpec as P

HEAD_DIM = 64
ROT = 16
EPS = 1e-05
MASKED = -1e30


def rotary_tables(length):
    half = ROT // 2
    inverse = jnp.exp(-jnp.log(10000.0) * (2.0 * jnp.arange(half, dtype=jnp.float32) / ROT))
    angles = jnp.arange(length, dtype=jnp.float32)[:, None] * inverse[None, :]
    return (jnp.cos(angles)[:, None, :], jnp.sin(angles)[:, None, :])


def rotate(values, cosine, sine, sign):
    half = ROT // 2
    first = values[..., :half]
    second = values[..., half:ROT]
    return jnp.concatenate(
        [
            first * cosine - sign * second * sine,
            second * cosine + sign * first * sine,
            values[..., ROT:],
        ],
        axis=-1,
    )


def mm(left, right, dims=((1,), (0,))):
    return lax.dot_general(left, right, (dims, ((), ())), preferred_element_type=jnp.float32)


def make_body(parts):
    def body(
        tokens,
        in_proj,
        in_bias,
        out_proj,
        out_bias,
        up_proj,
        up_bias,
        down_proj,
        down_bias,
        first_gain,
        first_shift,
        second_gain,
        second_shift,
        cotangent,
    ):
        length, width = tokens.shape
        me = lax.axis_index("shard")
        heads = width // parts // HEAD_DIM
        span = width // parts
        rows = in_proj.shape[0]
        hidden = up_bias.shape[0]
        scale = HEAD_DIM ** (-0.5)
        vectors = jnp.concatenate(
            [in_bias, out_bias, down_bias, first_gain, first_shift, second_gain, second_shift]
        )
        vectors = lax.all_gather(vectors, "shard", axis=0).astype(jnp.float32)
        cuts = [in_bias.shape[0]] + [span] * 6
        offsets = [sum(cuts[:i]) for i in range(len(cuts))]
        whole = [vectors[:, o : o + c].reshape(-1) for o, c in zip(offsets, cuts)]
        in_b, out_b, down_b, gain1, shift1, gain2, shift2 = whole
        both = lax.all_gather(jnp.stack([tokens, cotangent]), "shard", axis=1, tiled=True)
        x_all, g_all = both[0], both[1]
        w_in = lax.all_to_all(
            in_proj.reshape(rows, 3, parts, span), "shard", 2, 0, tiled=True
        ).reshape(parts * rows, 3 * span)
        w_up = lax.all_to_all(up_proj, "shard", 1, 0, tiled=True)
        b_in = lax.dynamic_slice_in_dim(in_b.reshape(3, parts, span), me, 1, axis=1).reshape(-1)
        x = x_all.astype(jnp.float32)
        mean = jnp.mean(x, axis=1, keepdims=True)
        cen = x - mean
        inv = lax.rsqrt(jnp.mean(cen * cen, axis=1, keepdims=True) + EPS)
        xhat = cen * inv
        attn_in = (xhat * gain1 + shift1).astype(jnp.bfloat16)
        mlp_in = (xhat * gain2 + shift2).astype(jnp.bfloat16)
        total_rows = x.shape[0]
        qkv = (mm(attn_in, w_in) + b_in).reshape(parts, length, 3, heads, HEAD_DIM)
        cosine, sine = rotary_tables(length)
        query = rotate(qkv[:, :, 0], cosine, sine, 1.0).astype(jnp.bfloat16)
        keys = rotate(qkv[:, :, 1], cosine, sine, 1.0).astype(jnp.bfloat16)
        values = qkv[:, :, 2].astype(jnp.bfloat16)
        causal = jnp.arange(length)[:, None] >= jnp.arange(length)[None, :]

        def ein(eq, a, b):
            return jnp.einsum(eq, a, b, preferred_element_type=jnp.float32)

        scores = jnp.where(causal, ein("sqhd,skhd->shqk", query, keys) * scale, MASKED)
        expo = jnp.exp(scores)
        probs_full = expo / jnp.sum(expo, axis=-1, keepdims=True)
        probs = probs_full.astype(jnp.bfloat16)
        attended = ein("shqk,skhd->sqhd", probs, values).astype(jnp.bfloat16)
        attended = attended.reshape(total_rows, span)
        up = mm(mlp_in, w_up) + up_bias.astype(jnp.float32)
        activated, pull = jax.vjp(lambda t: jax.nn.gelu(t, approximate=False), up)
        activated = activated.astype(jnp.bfloat16)
        partial = mm(attended, out_proj) + mm(activated, down_proj)
        branch = lax.psum_scatter(
            partial.astype(jnp.bfloat16), "shard", scatter_dimension=0, tiled=True
        )
        mixed = (tokens.astype(jnp.float32) + branch.astype(jnp.float32) + out_b + down_b).astype(
            jnp.bfloat16
        )
        grad_att = mm(g_all, out_proj, ((1,), (1,))).astype(jnp.bfloat16)
        grad_att = grad_att.reshape(parts, length, heads, HEAD_DIM)
        grad_act = mm(g_all, down_proj, ((1,), (1,)))
        grad_up = pull(grad_act)[0].astype(jnp.bfloat16)
        d_probs = ein("sqhd,skhd->shqk", grad_att, values)
        d_values = ein("shqk,sqhd->skhd", probs, grad_att)
        inner = jnp.sum(d_probs * probs_full, axis=-1, keepdims=True)
        d_scores = (probs_full * (d_probs - inner)).astype(jnp.bfloat16)
        d_query = ein("shqk,skhd->sqhd", d_scores, keys) * scale
        d_keys = ein("shqk,sqhd->skhd", d_scores, query) * scale
        d_query = rotate(d_query, cosine, sine, -1.0)
        d_keys = rotate(d_keys, cosine, sine, -1.0)
        grad_qkv = jnp.stack([d_query, d_keys, d_values], axis=2).astype(jnp.bfloat16)
        grad_qkv = grad_qkv.reshape(total_rows, 3 * span)
        d1 = mm(grad_qkv, w_in, ((1,), (1,)))
        d2 = mm(grad_up, w_up, ((1,), (1,)))
        scaled = (d1 * gain1 + d2 * gain2).astype(jnp.bfloat16)
        e = lax.psum_scatter(scaled, "shard", scatter_dimension=0, tiled=True).astype(jnp.float32)
        own = lambda a: lax.dynamic_slice_in_dim(a, me * length, length, axis=0)
        xh, rv = own(xhat), own(inv)
        tokens_grad = cotangent.astype(jnp.float32) + rv * (
            e - jnp.mean(e, axis=1, keepdims=True) - xh * jnp.mean(e * xh, axis=1, keepdims=True)
        )
        left = ((0,), (0,))
        dw_in = mm(attn_in, grad_qkv, left).astype(jnp.bfloat16)
        dw_up = mm(mlp_in, grad_up, left).astype(jnp.bfloat16)
        dw_out = mm(attended, g_all, left).astype(jnp.bfloat16)
        dw_down = mm(activated, g_all, left).astype(jnp.bfloat16)
        dw_in, dw_up, dw_out, dw_down = lax.psum((dw_in, dw_up, dw_out, dw_down), "rep")
        dw_in = lax.all_to_all(
            dw_in.reshape(parts * rows, 3, 1, span), "shard", 0, 2, tiled=True
        ).reshape(rows, 3 * width)
        dw_up = lax.all_to_all(dw_up, "shard", 0, 1, tiled=True)
        f32 = jnp.float32
        place = lambda v: lax.dynamic_update_slice_in_dim(
            jnp.zeros((3, parts, span), f32), v.reshape(3, 1, span), me, axis=1
        ).reshape(-1)
        vec = [
            place(jnp.sum(grad_qkv, axis=0, dtype=f32)),
            jnp.sum(cotangent.astype(f32), axis=0),
            jnp.sum(d1 * xhat, axis=0),
            jnp.sum(d1, axis=0),
            jnp.sum(d2 * xhat, axis=0),
            jnp.sum(d2, axis=0),
        ]
        vec = jnp.concatenate([v.reshape(parts, -1) for v in vec], axis=1)
        vec = lax.psum_scatter(vec, "shard", scatter_dimension=0, tiled=True)[0]
        vec, up_vec = lax.psum((vec, jnp.sum(grad_up, axis=0, dtype=f32)), "rep")
        o = in_bias.shape[0]
        bias_grad = vec[o : o + span]
        rest = [vec[o + span * i : o + span * (i + 1)] for i in range(1, 5)]
        return (
            mixed,
            tokens_grad,
            dw_in.astype(f32),
            vec[:o],
            dw_out.astype(f32),
            bias_grad,
            dw_up.astype(f32),
            up_vec,
            dw_down.astype(f32),
            bias_grad,
            *rest,
        )

    return body


BF = jnp.bfloat16
F32 = jnp.float32
MESH = pl.DeviceIdType.MESH
VMEM_LIMIT = 67_000_000
NN = ((1,), (0,))
NT = ((1,), (1,))
TN = ((0,), (0,))
IN, UP, DOWN, OUT = range(4)


class Sizes:
    def __init__(self, mesh_shape, length, width, hidden):
        self.copies = mesh_shape["rep"]
        self.n = self.copies // 2
        self.s = mesh_shape["shard"]
        self.l = length
        self.d = width
        self.ff = hidden
        self.span = width // self.n
        self.hid = hidden // self.n
        self.rs = width // self.s
        self.hb = hidden // self.s // self.n
        self.rows = self.n * length

    def fits(self):
        return (
            self.copies == 8
            and self.s == 4
            and self.rs == 256
            and self.span == 256
            and self.hb == 256
            and self.l % 256 == 0
        )


def rotary_lanes(length):
    half = ROT // 2
    inverse = np.exp(-np.log(10000.0) * (2.0 * np.arange(half) / ROT))
    angles = np.arange(length)[:, None] * inverse[None, :]
    cosine, sine = np.cos(angles), np.sin(angles)
    table = np.zeros((3, length, 128), np.float32)
    table[0] = 1.0
    for start in (0, HEAD_DIM):
        table[0, :, start : start + half] = cosine
        table[0, :, start + half : start + ROT] = cosine
        table[1, :, start : start + half] = -sine
        table[2, :, start + half : start + ROT] = sine
    return table


def dot(left, right, dims=NN):
    return lax.dot_general(left, right, (dims, ((), ())), preferred_element_type=F32)


def mo(value, m):
    return pl.multiple_of(value, m)


def fused(z, *refs):
    (tok, cot, inp, upp, outp, downp) = refs[:6]
    vectors_in, rot = refs[6:14], refs[14]
    (mixed_o, tgrad_o, gin_o, gup_o, gdown_o, gout_o, vec_o) = refs[15:22]
    (
        x_all, g_all, a1, a2, wi, wu, wo, wd, qkv, pt, der, act, att, gatt, gup, gqkv,
        msend, mrecv, mpre, mown, esend, erecv, epre, eown,
        dwi, dwu, dwd, dwo, xri, xru, xrd, xro, zri, zru, zrd, zro, fi, fu, fd, fo,
        vec, va, inb, vfull, vz, vu, vr, stat, vacc, bin_r, bup_r,
        loc, v_s, v_r, x_s, x_r, g_s, g_r, w_s, w_r, wc_s, wc_r,
        o_s, o_r, oc_s, oc_r, m_s, m_r, e_s, e_r, xs_s, xs_r, zs_s, zs_r,
        ag_s, ag_r, agc_s, agc_r, agl, v1_s, v1_r, v2_s, v2_r,
    ) = refs[22:]
    n, s_n, length, width = z.n, z.s, z.l, z.d
    span, hid, rs, hb = z.span, z.hid, z.rs, z.hb
    iw = 3 * span
    scale = HEAD_DIM**-0.5
    r = lax.axis_index("rep")
    zz = lax.axis_index("shard")
    p = lax.div(r, 2)
    c = lax.rem(r, 2)
    other = 1 - c
    partner = (2 * p + other, zz)
    py, px = lax.div(p, 2), lax.rem(p, 2)
    xn, yn, dg = 2 * py + 1 - px, 2 * (1 - py) + px, 2 * (1 - py) + 1 - px
    dev_x, dev_y = (2 * xn + c, zz), (2 * yn + c, zz)
    zp, zo = lax.div(zz, 2), lax.rem(zz, 2)
    is_end = zp == zo
    inner = zp != zo
    mate = 2 * zp + 1 - zo
    mate_dev = (r, mate)
    far_end, far_inner = 3 * (1 - zp), 2 - zp
    left, right = (r, zz - 1), (r, zz + 1)
    has_left, has_right = zz > 0, zz < s_n - 1

    def rc(src, dst, ss, rr, dev):
        return pltpu.make_async_remote_copy(
            src_ref=src, dst_ref=dst, send_sem=ss, recv_sem=rr, device_id=dev, device_id_type=MESH
        )

    def got(ref, rr):
        rc(ref, ref, rr, rr, partner).wait_recv()

    def seq(ref, s):
        return ref.at[pl.ds(mo(s * length, length), length)]

    sends = []

    def start(copy, cond=None):
        if cond is None:
            copy.start()
        else:
            pl.when(cond)(copy.start)
        sends.append((cond, copy))

    own_rows = pl.ds(mo(zz * rs, rs), rs)
    own_hb = pl.ds(mo(zz * hb, hb), hb)
    local_u = [
        pltpu.make_async_copy(
            upp.at[:, pl.ds(mo(i * (hb * n) + p * hb, hb), hb)],
            wu.at[own_rows, pl.ds(i * hb, hb)],
            loc.at[i],
        )
        for i in range(s_n)
    ]
    local_i = [
        pltpu.make_async_copy(
            inp.at[:, pl.ds(mo(i * width + (p + n * k) * 128, 128), 128)],
            wi.at[own_rows, pl.ds(i * span + k * 128, 128)],
            loc.at[s_n + 2 * i + k],
        )
        for i in range(3)
        for k in range(2)
    ]
    at_loc = s_n + 6
    local_d = pltpu.make_async_copy(
        downp.at[pl.ds(mo(p * hb, hb), hb)], wd.at[own_hb], loc.at[at_loc]
    )
    local_x = pltpu.make_async_copy(tok, seq(x_all, p), loc.at[at_loc + 1])
    local_g = pltpu.make_async_copy(cot, seq(g_all, p), loc.at[at_loc + 2])
    local_o = pltpu.make_async_copy(
        outp.at[pl.ds(mo(px * 128, 128), 128)], wo.at[pl.ds(mo(zp * 128, 128), 128)], loc.at[at_loc + 3]
    )
    at_home = zo == py
    away = jnp.logical_not(at_home)
    for cp in local_i + [local_x] + local_u + [local_g, local_d]:
        cp.start()
    pl.when(at_home)(local_o.start)
    off = 0
    for ref in vectors_in:
        size = ref.shape[0]
        vec[:, off : off + size] = ref[...].astype(F32).reshape(1, size)
        off += size

    barrier = pltpu.get_barrier_semaphore()
    for i in range(1, 2 * n):
        pl.semaphore_signal(
            barrier, 1, device_id=(lax.rem(r + i, 2 * n), zz), device_id_type=MESH
        )
    for i in range(1, s_n):
        pl.semaphore_signal(barrier, 1, device_id=(r, lax.rem(zz + i, s_n)), device_id_type=MESH)
    pl.semaphore_wait(barrier, 2 * n - 1 + s_n - 1)

    def line(i):
        q = lax.rem(zz + i, s_n)
        return q, (r, q)

    def plane_send(src, dst, ss, rr, cond=None):
        start(rc(src(0), dst(p, 0), ss(0), rr(p, 0), dev_x), cond)
        start(rc(src(1), dst(p, 1), ss(1), rr(p, 1), dev_y), cond)
        start(rc(src(1), dst(p, 1), ss(2), rr(p, 1), dev_x), cond)
        start(rc(src(0), dst(p, 0), ss(3), rr(p, 0), dev_y), cond)

    def plane_relay(dst, ss, rr):
        got(dst(xn, 0), rr(xn, 0))
        start(rc(dst(xn, 0), dst(xn, 0), ss(4), rr(xn, 0), dev_y))
        got(dst(yn, 1), rr(yn, 1))
        start(rc(dst(yn, 1), dst(yn, 1), ss(5), rr(yn, 1), dev_x))

    def plane_near(dst, rr):
        got(dst(xn, 1), rr(xn, 1))
        got(dst(yn, 0), rr(yn, 0))

    def plane_far(dst, rr):
        got(dst(dg, 0), rr(dg, 0))
        got(dst(dg, 1), rr(dg, 1))

    lh = length // 2

    def part(ref):
        return lambda q, h: ref.at[pl.ds(mo(q * length + h * lh, lh), lh)]

    def sem1(ref):
        return lambda i: ref.at[i]

    def sem2(ref):
        return lambda q, h: ref.at[q, h]

    def rows_of(ref):
        return lambda h: ref.at[pl.ds(h * lh, lh)]

    for i in range(1, s_n):
        q, dev = line(i)
        start(rc(vec, va.at[zz], v_s.at[i], v_r.at[zz], dev))
    plane_send(rows_of(tok), part(x_all), sem1(x_s), sem2(x_r))

    half, hhalf, ohalf = rs // 2, hb // 2, span // 4
    cuts = {IN: 2, UP: 1, DOWN: 1}

    def piece(t, ref, block):
        rows = block // 2 // cuts[t]
        return lambda q, core, h: ref.at[pl.ds(mo(q * block + core * (block // 2) + h * rows, rows), rows)]

    u_piece, d_piece, i_piece = piece(UP, wu, rs), piece(DOWN, wd, hb), piece(IN, wi, rs)

    def own_sends(t, get):
        for h in range(cuts[t]):
            mine = get(zz, c, h)
            start(rc(mine, mine, w_s.at[t, h, 0], w_r.at[t, h, zz], left), has_left)
            start(rc(mine, mine, w_s.at[t, h, 1], w_r.at[t, h, zz], right), has_right)

    def relay(t, get, d, who):
        def take(h, q, has, onward, more, slot):
            ref = get(q, c, h)

            @pl.when(has)
            def _():
                got(ref, w_r.at[t, h, q])

            start(
                rc(ref, ref, w_s.at[t, h, slot], w_r.at[t, h, q], onward),
                jnp.logical_and(has, more),
            )
            start(rc(ref, ref, wc_s.at[t, h, slot], wc_r.at[t, h, q], partner), has)

        for h in range(cuts[t]):
            from_left = jnp.logical_and(who, zz - d >= 0)
            from_right = jnp.logical_and(who, zz + d <= s_n - 1)
            take(h, zz - d, from_left, right, has_right, 2 * d)
            take(h, zz + d, from_right, left, has_left, 2 * d + 1)

    def relay_done(t, get):
        for h in range(cuts[t]):
            for i in range(1, s_n):
                q, _ = line(i)
                got(get(q, other, h), wc_r.at[t, h, q])

    for cp in local_i:
        cp.wait()
    own_sends(IN, i_piece)

    for i in range(1, s_n):
        q, dev = line(i)
        got(va.at[q], v_r.at[q])
    va[zz] = vec[...]
    n_in = 3 * width // s_n
    n_up = hb * n
    at_up = n_in
    at_rest = n_in + n_up

    def vector(i):
        off = at_rest + i * rs
        return jnp.concatenate([va[q, :, off : off + rs] for q in range(s_n)], axis=1)

    out_b, down_b, gain1, shift1, gain2, shift2 = [vector(i) for i in range(6)]
    for q in range(s_n):
        inb[:, q * n_in : (q + 1) * n_in] = va[q, :, :n_in]

    def norm(s):
        step = 32

        def body(i, carry):
            row = pl.ds(mo(s * length + i * step, step), step)
            xv = x_all[row, :].astype(F32)
            mu = jnp.mean(xv, axis=1, keepdims=True)
            cen = xv - mu
            inv = lax.rsqrt(jnp.mean(cen * cen, axis=1, keepdims=True) + EPS)
            xh = cen * inv
            a1[row, :] = (xh * gain1 + shift1).astype(BF)
            a2[row, :] = (xh * gain2 + shift2).astype(BF)
            stat[row, 0:1] = mu
            stat[row, 1:2] = inv
            return carry

        lax.fori_loop(0, length // step, body, 0)

    table = [rot[i] for i in range(3)]

    def turn(t, sign):
        fwd = pltpu.roll(t, 128 - ROT // 2, 1)
        back = pltpu.roll(t, ROT // 2, 1)
        return t * table[0] + (fwd * table[1] + back * table[2]) * sign

    def turn_of(k):
        return jnp.where(k == 0, p, jnp.where(k == 1, xn, jnp.where(k == 2, yn, dg)))

    def qkv_block(k, carry):
        row = pl.ds(mo(turn_of(k) * length, length), length)
        left_a = a1[row, :]
        for i in range(3):
            v = dot(left_a, wi[:, i * span : (i + 1) * span])
            for h in range(2):
                bias = inb[:, pl.ds(mo(i * width + (p + n * h) * 128, 128), 128)]
                cut = v[:, h * 128 : (h + 1) * 128] + bias
                if i < 2:
                    cut = turn(cut, 1.0)
                qkv[row, i * span + h * 128 : i * span + (h + 1) * 128] = cut.astype(BF)
        return carry

    relay(IN, i_piece, 1, inner)
    local_x.wait()
    norm(p)
    relay(IN, i_piece, 2, inner)
    for cp in local_u:
        cp.wait()
    own_sends(UP, u_piece)
    plane_relay(part(x_all), sem1(x_s), sem2(x_r))
    plane_send(rows_of(cot), part(g_all), sem1(g_s), sem2(g_r))
    plane_near(part(x_all), sem2(x_r))
    norm(xn)
    norm(yn)
    relay(UP, u_piece, 1, inner)
    for d in range(1, s_n):
        relay(IN, i_piece, d, is_end)
    relay_done(IN, i_piece)
    lax.fori_loop(0, 3, qkv_block, 0)
    relay(UP, u_piece, 2, inner)
    local_d.wait()
    own_sends(DOWN, d_piece)
    def o_piece(block, core):
        return wo.at[pl.ds(mo(block * 128 + core * ohalf, ohalf), ohalf)]

    pl.when(at_home)(local_o.wait)
    near_first = (mate_dev, (r, far_inner), (r, far_end))
    for i, dev in enumerate(near_first):
        start(rc(o_piece(zp, c), o_piece(zp, c), o_s.at[i], o_r.at[zp], dev), at_home)
    plane_far(part(x_all), sem2(x_r))
    norm(dg)
    lax.fori_loop(3, n, qkv_block, 0)
    plane_relay(part(g_all), sem1(g_s), sem2(g_r))

    lane = lax.broadcasted_iota(jnp.int32, (1, 128), 1)
    first = lane < HEAD_DIM
    masks = [first.astype(F32).astype(BF), (1.0 - first.astype(F32)).astype(BF)]
    pairs = span // 128

    def att_forward(idx, carry):
        s = lax.div(idx, pairs)
        pr = lax.rem(idx, pairs)
        row = pl.ds(mo(s * length, length), length)
        q2 = qkv[row, pl.ds(mo(pr * 128, 128), 128)]
        k2 = qkv[row, pl.ds(mo(span + pr * 128, 128), 128)]
        v2 = qkv[row, pl.ds(mo(2 * span + pr * 128, 128), 128)]
        key_i = lax.broadcasted_iota(jnp.int32, (length, length), 0)
        query_i = lax.broadcasted_iota(jnp.int32, (length, length), 1)
        found = []
        for h in range(2):
            st = dot(k2, q2 * masks[h], NT) * scale
            ex = jnp.exp(jnp.where(key_i <= query_i, st, MASKED))
            pr_t = ex / jnp.sum(ex, axis=0, keepdims=True)
            pt[idx * 2 + h] = pr_t
            found.append(dot(pr_t.astype(BF), v2, TN))
        att[row, pl.ds(mo(pr * 128, 128), 128)] = jnp.where(first, found[0], found[1]).astype(BF)
        return carry

    lax.fori_loop(0, n * pairs // 2, att_forward, 0)
    relay(DOWN, d_piece, 1, inner)
    lax.fori_loop(n * pairs // 2, n * pairs, att_forward, 0)
    for d in range(1, s_n):
        relay(UP, u_piece, d, is_end)
    relay_done(UP, u_piece)

    def up_block(s, carry):
        row = pl.ds(mo(s * length, length), length)
        left_a = a2[row, :]
        for j in range(s_n):
            col = pl.ds(j * hb, hb)
            bias = va[j, :, pl.ds(mo(at_up + p * hb, hb), hb)]
            u = dot(left_a, wu[:, j * hb : (j + 1) * hb]) + bias
            phi = 0.5 * (1.0 + lax.erf(u * 0.7071067811865476))
            act[row, col] = (u * phi).astype(BF)
            der[row, col] = phi + u * (0.3989422804014327 * jnp.exp(-0.5 * u * u))
        return carry

    lax.fori_loop(0, n, up_block, 0)
    relay(DOWN, d_piece, 2, inner)

    def exchange(t, dw, xr, block_half):
        src = dw.at[:, pl.ds(mo(other * block_half, block_half), block_half)]
        start(rc(src, xr, xs_s.at[t], xs_r.at[t], partner))

    def core_sum(t, dw, xr, block_half):
        mine = pl.ds(mo(c * block_half, block_half), block_half)
        got(xr, xs_r.at[t])

        def body(q, carry):
            xr[q] = (dw[q, mine].astype(F32) + xr[q].astype(F32)).astype(BF)
            return carry

        lax.fori_loop(0, dw.shape[0], body, 0)

    def pair_sum(t, dw, xr, zr, block_half):
        core_sum(t, dw, xr, block_half)
        start(rc(xr.at[far_end], zr.at[2], zs_s.at[t, 0], zs_r.at[t, 2], mate_dev), is_end)
        start(rc(xr.at[far_inner], zr.at[3], zs_s.at[t, 1], zs_r.at[t, 3], mate_dev), is_end)
        start(rc(xr.at[mate], zr.at[0], zs_s.at[t, 2], zs_r.at[t, 0], mate_dev))

    def pass_on(t, xr, zr):
        @pl.when(inner)
        def _():
            for slot, q in ((2, far_end), (3, far_inner)):
                got(zr.at[slot], zs_r.at[t, slot])
                xr[q] = (xr[q].astype(F32) + zr[slot].astype(F32)).astype(BF)
                rc(xr.at[q], zr.at[1], zs_s.at[t, slot - 2], zs_r.at[t, 1], (r, q)).start()

        for slot, q in ((2, far_end), (3, far_inner)):
            cp = rc(xr.at[q], zr.at[1], zs_s.at[t, slot - 2], zs_r.at[t, 1], (r, q))
            sends.append((inner, cp))

    def line_sum(t, xr, zr, fin):
        got(zr.at[0], zs_r.at[t, 0])
        got(zr.at[1], zs_r.at[t, 1])
        total = xr[zz].astype(F32) + zr[0].astype(F32) + zr[1].astype(F32)
        fin[...] = total.astype(BF)

    outs_of = {IN: (gin_o, fi), UP: (gup_o, fu), DOWN: (gdown_o, fd)}

    def area(t):
        o = outs_of[t][0]
        rows = o.shape[2] // 2
        return lambda q, h: o.at[q, c, pl.ds(h * rows, rows)]

    def fin_half(t):
        fin = outs_of[t][1]
        rows = fin.shape[0] // 2
        return lambda h: fin.at[pl.ds(h * rows, rows)]

    def ag1(t):
        return lambda i: ag_s.at[t, i]

    def ag2(t):
        return lambda q, h: ag_r.at[t, q, h]

    local_out = []

    def spread(t):
        o, fin = outs_of[t]
        plane_send(fin_half(t), area(t), ag1(t), ag2(t))
        start(rc(fin, o.at[p, c], agc_s.at[t, 0], agc_r.at[t, p], partner))
        cp = pltpu.make_async_copy(fin, o.at[p, c], agl.at[t])
        cp.start()
        local_out.append((None, cp))

    def spread_relay(t):
        plane_relay(area(t), ag1(t), ag2(t))

    def spread_near(t):
        o = outs_of[t][0]
        plane_near(area(t), ag2(t))
        start(rc(o.at[xn, c], o.at[xn, c], agc_s.at[t, 1], agc_r.at[t, xn], partner))
        start(rc(o.at[yn, c], o.at[yn, c], agc_s.at[t, 2], agc_r.at[t, yn], partner))

    def spread_far(t):
        o = outs_of[t][0]
        plane_far(area(t), ag2(t))
        start(rc(o.at[dg, c], o.at[dg, c], agc_s.at[t, 3], agc_r.at[t, dg], partner))

    def spread_end(t):
        o = outs_of[t][0]
        for i in range(n):
            q = lax.rem(p + i, n)
            got(o.at[q, other], agc_r.at[t, q])

    local_g.wait()
    plane_near(part(g_all), sem2(g_r))
    plane_far(part(g_all), sem2(g_r))

    dwo_all = dot(att[...], g_all[...], TN).astype(BF)
    for i in range(2):
        dwo[i] = dwo_all[i * 128 : (i + 1) * 128]
    exchange(OUT, dwo, xro, ohalf)
    for j in range(s_n):
        dwd[j] = dot(act[:, j * hb : (j + 1) * hb], g_all[...], TN).astype(BF)
    exchange(DOWN, dwd, xrd, hhalf)
    core_sum(OUT, dwo, xro, ohalf)
    near_b, far_b = zp, 1 - zp
    start(rc(xro.at[far_b], zro.at[2], zs_s.at[OUT, 1], zs_r.at[OUT, 2], mate_dev), is_end)
    start(rc(xro.at[near_b], zro.at[0], zs_s.at[OUT, 0], zs_r.at[OUT, 0], mate_dev), away)
    pair_sum(DOWN, dwd, xrd, zrd, hhalf)

    def o_take(block, cond):
        @pl.when(cond)
        def _():
            got(o_piece(block, c), o_r.at[block])

        start(
            rc(o_piece(block, c), o_piece(block, c), oc_s.at[block], oc_r.at[block], partner), cond
        )

    def o_done(block, cond):
        @pl.when(cond)
        def _():
            got(o_piece(block, other), oc_r.at[block])

    always = zz >= 0
    o_take(near_b, away)
    o_take(far_b, always)
    o_done(near_b, away)
    o_done(far_b, always)

    bup_r[...] = jnp.zeros_like(bup_r)
    bin_r[...] = jnp.zeros_like(bin_r)

    def grad_att_block(s, carry):
        row = pl.ds(mo(s * length, length), length)
        gatt[row, :] = dot(g_all[row, :], wo[...], NT).astype(BF)
        return carry

    lax.fori_loop(0, n, grad_att_block, 0)

    def att_backward(idx, carry):
        s = lax.div(idx, pairs)
        pr = lax.rem(idx, pairs)
        row = pl.ds(mo(s * length, length), length)
        q_col = pl.ds(mo(pr * 128, 128), 128)
        k_col = pl.ds(mo(span + pr * 128, 128), 128)
        v_col = pl.ds(mo(2 * span + pr * 128, 128), 128)
        q2, k2, v2 = qkv[row, q_col], qkv[row, k_col], qkv[row, v_col]
        g2 = gatt[row, q_col]
        dq, dk, dv = [], [], []
        for h in range(2):
            pr_t = pt[idx * 2 + h]
            dp = dot(v2, g2 * masks[h], NT)
            total = jnp.sum(dp * pr_t, axis=0, keepdims=True)
            ds = (pr_t * (dp - total)).astype(BF)
            dv.append(dot(pr_t.astype(BF), g2))
            dk.append(dot(ds, q2))
            dq.append(dot(ds, k2, TN))
        dqv = turn(jnp.where(first, dq[0], dq[1]) * scale, -1.0).astype(BF)
        dkv = turn(jnp.where(first, dk[0], dk[1]) * scale, -1.0).astype(BF)
        dvv = jnp.where(first, dv[0], dv[1]).astype(BF)
        for col, val in ((q_col, dqv), (k_col, dkv), (v_col, dvv)):
            gqkv[row, col] = val
            bin_r[:, col] += jnp.sum(val.astype(F32), axis=0, keepdims=True)
        return carry

    lax.fori_loop(0, n * pairs - 4, att_backward, 0)
    on = rc(xro.at[far_b], zro.at[1], zs_s.at[OUT, 2], zs_r.at[OUT, 1], (r, 2 * (1 - zp) + py))

    @pl.when(inner)
    def _():
        got(zro.at[2], zs_r.at[OUT, 2])
        xro[far_b] = (xro[far_b].astype(F32) + zro[2].astype(F32)).astype(BF)
        on.start()

    sends.append((inner, on))
    lax.fori_loop(n * pairs - 4, n * pairs - 2, att_backward, 0)

    for d in range(1, s_n):
        relay(DOWN, d_piece, d, is_end)
    relay_done(DOWN, d_piece)

    def ways(send, recv, pre, ss, rr):
        row = lambda h: pl.ds(h * lh, lh)
        return (
            (0, rc(send.at[0, row(0)], pre.at[0], ss.at[0], rr.at[0], dev_x)),
            (0, rc(send.at[0, row(1)], pre.at[1], ss.at[1], rr.at[1], dev_y)),
            (1, rc(send.at[1, row(0)], recv.at[0, row(0)], ss.at[2], rr.at[2], dev_x)),
            (2, rc(send.at[2, row(1)], recv.at[1, row(1)], ss.at[3], rr.at[3], dev_y)),
        )

    def shares(k, *refs):
        for j in range(3):

            @pl.when(k == j)
            def _():
                for i, cp in ways(*refs):
                    if i == j:
                        cp.start()

    def shares_on(send, recv, pre, ss, rr):
        for k, h, dev in ((1, 1, dev_x), (2, 0, dev_y)):
            got(pre.at[h], rr.at[h])
            row = pl.ds(h * lh, lh)
            send[k, row] = (send[k, row].astype(F32) + pre[h].astype(F32)).astype(BF)
            start(rc(send.at[k, row], recv.at[k - 1, row], ss.at[k + 3], rr.at[k + 3], dev))

    def shares_got(recv, rr):
        for k, h in ((0, 0), (1, 1)):
            row, rest = pl.ds(h * lh, lh), pl.ds((1 - h) * lh, lh)
            got(recv.at[k, row], rr.at[k + 2])
            got(recv.at[k, rest], rr.at[k + 4])

    def shares_left(*refs):
        for _, cp in ways(*refs):
            cp.wait_send()

    def share_of(k):
        return jnp.where(k == 0, dg, jnp.where(k == 1, xn, jnp.where(k == 2, yn, p)))

    m_refs = (msend, mrecv, mpre, m_s, m_r)
    e_refs = (esend, erecv, epre, e_s, e_r)

    def out_block(k, carry):
        row = pl.ds(mo(share_of(k) * length, length), length)
        for j in range(width // 256):
            col = slice(j * 256, (j + 1) * 256)
            v = dot(att[row, :], wo[:, col]) + dot(act[row, :], wd[:, col])
            msend[k, :, col] = v.astype(BF)
            mown[:, col] = v
        shares(k, *m_refs)
        return carry

    lax.fori_loop(0, n, out_block, 0)
    @pl.when(at_home)
    def _():
        got(zro.at[0], zs_r.at[OUT, 0])
        got(zro.at[1], zs_r.at[OUT, 1])
        total = xro[near_b].astype(F32) + zro[0].astype(F32) + zro[1].astype(F32)
        fo[...] = total.astype(BF)

    oq = ohalf // 2

    def o_whole(q):
        return gout_o.at[lax.rem(q, 2), c]

    def o_area(q, h):
        return gout_o.at[lax.rem(q, 2), c, pl.ds(h * oq, oq)]

    plane_send(lambda h: fo.at[pl.ds(h * oq, oq)], o_area, ag1(OUT), ag2(OUT), at_home)
    start(rc(fo, o_whole(p), agc_s.at[OUT, 0], agc_r.at[OUT, p], partner), at_home)
    cp = pltpu.make_async_copy(fo, o_whole(p), agl.at[OUT])
    pl.when(at_home)(cp.start)
    local_out.append((at_home, cp))

    pass_on(DOWN, xrd, zrd)
    lax.fori_loop(n * pairs - 2, n * pairs, att_backward, 0)
    shares_on(*m_refs)

    for j in range(s_n):
        dwi[j] = dot(a1[:, j * rs : (j + 1) * rs], gqkv[...], TN).astype(BF)
    exchange(IN, dwi, xri, half)

    def grad_up_block(s, carry):
        row = pl.ds(mo(s * length, length), length)
        gs = g_all[row, :]
        for j in range(s_n):
            col = pl.ds(j * hb, hb)
            gu = (dot(gs, wd[j * hb : (j + 1) * hb, :], NT) * der[row, col]).astype(BF)
            gup[row, col] = gu
            bup_r[:, col] += jnp.sum(gu.astype(F32), axis=0, keepdims=True)
        return carry

    lax.fori_loop(0, 2, grad_up_block, 0)
    pair_sum(IN, dwi, xri, zri, half)
    lax.fori_loop(2, n, grad_up_block, 0)
    for j in range(s_n):
        dwu[j] = dot(a2[:, j * rs : (j + 1) * rs], gup[...], TN).astype(BF)
    exchange(UP, dwu, xru, half)

    vacc[...] = jnp.zeros_like(vacc)

    def in_block(k, carry):
        row = pl.ds(mo(share_of(k) * length, length), length)
        gq = gqkv[row, :]
        gu = gup[row, :]
        mu = stat[row, 0:1]
        inv = stat[row, 1:2]
        for j in range(s_n):
            col = slice(j * rs, (j + 1) * rs)
            d1 = dot(gq, wi[col, :], NT)
            d2 = dot(gu, wu[col, :], NT)
            xh = (x_all[row, col].astype(F32) - mu) * inv
            vacc[0, :, col] += jnp.sum(d1 * xh, axis=0, keepdims=True)
            vacc[1, :, col] += jnp.sum(d1, axis=0, keepdims=True)
            vacc[2, :, col] += jnp.sum(d2 * xh, axis=0, keepdims=True)
            vacc[3, :, col] += jnp.sum(d2, axis=0, keepdims=True)
            e = d1 * gain1[:, col] + d2 * gain2[:, col]
            esend[k, :, col] = e.astype(BF)
            eown[:, col] = e
        shares(k, *e_refs)
        return carry

    lax.fori_loop(0, 1, in_block, 0)
    pair_sum(UP, dwu, xru, zru, half)
    lax.fori_loop(1, 3, in_block, 0)
    pass_on(IN, xri, zri)
    lax.fori_loop(3, n, in_block, 0)

    line_sum(DOWN, xrd, zrd, fd)
    spread(DOWN)

    shares_on(*e_refs)

    slots = vfull.shape[0] // s_n
    vfull[...] = jnp.zeros_like(vfull)
    per = n_in // 128
    for i in range(3):
        for h in range(2):
            b = i * 2 * n + p + n * h
            col = slice(i * span + h * 128, i * span + (h + 1) * 128)
            vfull[lax.div(b, per) * slots + lax.rem(b, per)] = bin_r[:, col]
    at_g = per + 2 * n
    for q in range(s_n):
        for h in range(2):
            up_col = slice(q * hb + h * 128, q * hb + (h + 1) * 128)
            vfull[q * slots + per + 2 * p + h] = bup_r[:, up_col]
            col = slice(q * rs + h * 128, q * rs + (h + 1) * 128)
            g_own = g_all[pl.ds(mo(p * length, length), length), col].astype(F32)
            vfull[q * slots + at_g + h] = jnp.sum(g_own, axis=0, keepdims=True)
            for i in range(4):
                vfull[q * slots + at_g + 2 + 2 * i + h] = vacc[i, :, col]
    for i in range(1, s_n):
        q, dev = line(i)
        start(rc(vfull.at[pl.ds(q * slots, slots)], vz.at[zz], v1_s.at[i], v1_r.at[zz], dev))

    pass_on(UP, xru, zru)

    shares_got(mrecv, m_r)

    def mixed_rows(i, carry):
        step = 32
        row = pl.ds(mo(i * step, step), step)
        xv = x_all[pl.ds(mo(p * length + i * step, step), step), :].astype(F32)
        t = mown[row, :] + mrecv[0, row, :].astype(F32) + mrecv[1, row, :].astype(F32)
        mixed_o[row, :] = (xv + t + out_b + down_b).astype(BF)
        return carry

    lax.fori_loop(0, length // 32, mixed_rows, 0)

    spread_relay(DOWN)
    line_sum(IN, xri, zri, fi)
    spread(IN)
    def o_got(q, h, cond):
        @pl.when(cond)
        def _():
            got(o_area(q, h), ag_r.at[OUT, q, h])

    o_got(xn, 0, at_home)
    start(rc(o_area(xn, 0), o_area(xn, 0), ag_s.at[OUT, 4], ag_r.at[OUT, xn, 0], dev_y), at_home)
    o_got(yn, 1, away)
    start(rc(o_area(yn, 1), o_area(yn, 1), ag_s.at[OUT, 5], ag_r.at[OUT, yn, 1], dev_x), away)
    line_sum(UP, xru, zru, fu)
    spread(UP)

    spread_relay(IN)

    spread_near(DOWN)
    spread_far(DOWN)
    total = [vfull[zz * slots + k] for k in range(slots)]
    for i in range(1, s_n):
        q, dev = line(i)
        got(vz.at[q], v1_r.at[q])
        total = [t + vz[q, k] for k, t in enumerate(total)]
    for k in range(slots):
        vu[k] = total[k]
        vr[r, k] = total[k]
    for i in range(1, 2 * n):
        start(rc(vu, vr.at[r], v2_s.at[i], v2_r.at[r], (lax.rem(r + i, 2 * n), zz)))

    shares_got(erecv, e_r)

    def tgrad_rows(i, carry):
        step = 32
        row = pl.ds(mo(i * step, step), step)
        far = pl.ds(mo(p * length + i * step, step), step)
        inv = stat[far, 1:2]
        xh = (x_all[far, :].astype(F32) - stat[far, 0:1]) * inv
        e = eown[row, :] + erecv[0, row, :].astype(F32) + erecv[1, row, :].astype(F32)
        m0 = jnp.mean(e, axis=1, keepdims=True)
        m1 = jnp.mean(e * xh, axis=1, keepdims=True)
        tgrad_o[row, :] = g_all[far, :].astype(F32) + inv * (e - m0 - xh * m1)
        return carry

    lax.fori_loop(0, length // 32, tgrad_rows, 0)

    spread_relay(UP)
    o_got(xn, 1, at_home)
    start(rc(o_whole(xn), o_whole(xn), agc_s.at[OUT, 1], agc_r.at[OUT, xn], partner), at_home)
    o_got(yn, 0, away)
    start(rc(o_whole(yn), o_whole(yn), agc_s.at[OUT, 2], agc_r.at[OUT, yn], partner), away)
    o_got(dg, 0, away)
    o_got(dg, 1, away)
    start(rc(o_whole(dg), o_whole(dg), agc_s.at[OUT, 3], agc_r.at[OUT, dg], partner), away)

    spread_near(IN)
    spread_far(IN)
    for i in range(1, 2 * n):
        q = lax.rem(r + i, 2 * n)
        got(vr.at[q], v2_r.at[q])
    for k in range(slots):
        t = vr[0, k]
        for q in range(1, 2 * n):
            t = t + vr[q, k]
        vec_o[k] = t
    spread_near(UP)
    spread_far(UP)
    for t in (DOWN, IN, UP):
        spread_end(t)
    for q, cond in ((p, at_home), (xn, at_home), (yn, away), (dg, away)):

        @pl.when(cond)
        def _():
            got(gout_o.at[lax.rem(q, 2), other], agc_r.at[OUT, q])

    for cond, cp in local_out:
        if cond is None:
            cp.wait()
        else:
            pl.when(cond)(cp.wait)
    shares_left(*m_refs)
    shares_left(*e_refs)
    for cond, cp in sends:
        if cond is None:
            cp.wait_send()
        else:
            pl.when(cond)(cp.wait_send)


def fused_call(z, tok, cot, inp, upp, outp, downp, vectors):
    n, s_n, length, width, span, hid = z.n, z.s, z.l, z.d, z.span, z.hid
    rs, hb, rows = z.rs, z.hb, z.rows
    iw = 3 * span
    nv = sum(v.shape[0] for v in vectors)
    slots = (3 * width // s_n + hb * n + 5 * rs) // 128
    V = pltpu.VMEM
    dma = lambda *shape: pltpu.SemaphoreType.DMA(shape)
    share = [
        V((n, length, width), BF), V((2, length, width), BF), V((2, length // 2, width), BF),
        V((length, width), F32),
    ]
    halves = [
        V((s_n, rs // 2, iw), BF), V((s_n, rs // 2, hid), BF), V((s_n, hb // 2, width), BF),
    ]
    scratch = [
        *[V((rows, width), BF)] * 4,
        V((width, iw), BF), V((width, hid), BF), V((span, width), BF), V((hid, width), BF),
        V((rows, iw), BF), V((n * span // HEAD_DIM, length, length), F32),
        V((rows, hid), F32), V((rows, hid), BF), V((rows, span), BF),
        V((rows, span), BF), V((rows, hid), BF), V((rows, iw), BF),
        *share, *share,
        V((s_n, rs, iw), BF), V((s_n, rs, hid), BF), V((s_n, hb, width), BF), V((2, span // 2, width), BF),
        *halves, V((2, span // 4, width), BF),
        *halves, V((3, span // 4, width), BF),
        V((rs // 2, iw), BF), V((rs // 2, hid), BF), V((hb // 2, width), BF), V((span // 4, width), BF),
        V((1, nv), F32), V((s_n, 1, nv), F32), V((1, 3 * width), F32), V((s_n * slots, 1, 128), F32),
        V((s_n, slots, 1, 128), F32), V((slots, 1, 128), F32), V((2 * n, slots, 1, 128), F32),
        V((rows, 2), F32), V((4, 1, width), F32), V((1, iw), F32), V((1, hid), F32),
        dma(s_n + 10), dma(s_n), dma(s_n), dma(6), dma(n, 2), dma(6), dma(n, 2),
        dma(3, 2, 2 * s_n), dma(3, 2, s_n), dma(3, 2, 2 * s_n), dma(3, 2, s_n),
        dma(3), dma(2), dma(2), dma(2),
        dma(6), dma(6), dma(6), dma(6), dma(4), dma(4), dma(4, 3), dma(4, 4),
        dma(4, 6), dma(4, n, 2), dma(4, n), dma(4, n), dma(4),
        dma(s_n), dma(s_n), dma(2 * n), dma(2 * n),
    ]
    any_ = pl.BlockSpec(memory_space=pl.ANY)
    vm = pl.BlockSpec(memory_space=pltpu.VMEM)
    outs = [
        jax.ShapeDtypeStruct((length, width), BF),
        jax.ShapeDtypeStruct((length, width), F32),
        jax.ShapeDtypeStruct((n, 2, rs // 2, iw), BF),
        jax.ShapeDtypeStruct((n, 2, rs // 2, hid), BF),
        jax.ShapeDtypeStruct((n, 2, hb // 2, width), BF),
        jax.ShapeDtypeStruct((2, 2, span // 4, width), BF),
        jax.ShapeDtypeStruct((slots, 1, 128), F32),
    ]
    return pl.pallas_call(
        functools.partial(fused, z),
        out_shape=outs,
        in_specs=[any_] * 6 + [vm] * 9,
        out_specs=[vm, vm, any_, any_, any_, any_, vm],
        scratch_shapes=scratch,
        compiler_params=pltpu.CompilerParams(
            collective_id=0, has_side_effects=True, vmem_limit_bytes=VMEM_LIMIT
        ),
        name="block_step",
    )(tok, cot, inp, upp, outp, downp, *vectors, jnp.asarray(rotary_lanes(length)))


def finish(z, *refs):
    mixed, tgrad, g_in, g_up, g_down, g_out, vec = refs[:7]
    mixed_o, tgrad_o, in_o, up_o, down_o, out_o = refs[7:13]
    vec_o = refs[13:21]
    m_v, t_v, bi, bu, bd, bo, fi, fu, fd, fo, m_sem, r_sem, w_sem = refs[21:]
    n, s_n, width, span, hb, rs = z.n, z.s, z.d, z.span, z.hb, z.rs
    half = rs // 2
    jobs = []
    for q in range(n):
        for core in range(2):
            row = slice(core * half, (core + 1) * half)
            jobs.append((g_up.at[q, core], bu.at[q, core], fu.at[q, core], [
                (up_o.at[row, k * hb * n + q * hb : k * hb * n + (q + 1) * hb], slice(k * hb, (k + 1) * hb))
                for k in range(s_n)
            ]))
    for q in range(n):
        for core in range(2):
            start = q * hb + core * (hb // 2)
            jobs.append((g_down.at[q, core], bd.at[q, core], fd.at[q, core], [
                (down_o.at[start : start + hb // 2], slice(None)),
            ]))
    for q in range(n):
        for core in range(2):
            row = slice(core * half, (core + 1) * half)
            jobs.append((g_in.at[q, core], bi.at[q, core], fi.at[q, core], [
                (
                    in_o.at[row, k * width + (q + n * h) * 128 : k * width + (q + n * h + 1) * 128],
                    slice(k * span + h * 128, k * span + (h + 1) * 128),
                )
                for k in range(3)
                for h in range(2)
            ]))
    for j in range(2):
        for core in range(2):
            start = (2 * j + core) * (span // 4)
            jobs.append((g_out.at[j, core], bo.at[j, core], fo.at[j, core], [
                (out_o.at[start : start + span // 4], slice(None)),
            ]))
    through = [
        (pltpu.make_async_copy(a, b, m_sem.at[2 * i]), pltpu.make_async_copy(b, o, m_sem.at[2 * i + 1]))
        for i, (a, b, o) in enumerate(((mixed, m_v, mixed_o), (tgrad, t_v, tgrad_o)))
    ]
    reads = [pltpu.make_async_copy(src, dst, r_sem.at[i]) for i, (src, dst, _, _) in enumerate(jobs)]
    for cp in reads:
        cp.start()
    for cp, _ in through:
        cp.start()
    writes = []
    for (_, low, wide, places), read in zip(jobs, reads):
        read.wait()

        def body(i, carry, low=low, wide=wide):
            row = pl.ds(mo(i * 32, 32), 32)
            wide[row, :] = low[row, :].astype(F32)
            return carry

        lax.fori_loop(0, low.shape[0] // 32, body, 0)
        for place, col in places:
            cp = pltpu.make_async_copy(wide.at[:, col], place, w_sem.at[len(writes)])
            cp.start()
            writes.append(cp)
    for a, b in through:
        a.wait()
        b.start()
    k = 0
    for ref in vec_o:
        blocks = ref.shape[0] // 128
        if ref is vec_o[3]:
            k -= blocks
        for i in range(blocks):
            ref[i * 128 : (i + 1) * 128] = vec[k + i].reshape(128)
        k += blocks
    for cp in writes:
        cp.wait()
    for _, b in through:
        b.wait()


def finish_call(z, pieces):
    n, width, span = z.n, z.d, z.span
    V = pltpu.VMEM
    S = jax.ShapeDtypeStruct
    any_ = pl.BlockSpec(memory_space=pl.ANY)
    vm = pl.BlockSpec(memory_space=pltpu.VMEM)
    rs = z.rs
    outs = [
        S((z.l, width), BF), S((z.l, width), F32), S((rs, 3 * width), F32), S((rs, z.ff), F32),
        S((z.hb * n, width), F32), S((span, width), F32),
        S((3 * width // z.s,), F32), S((z.hb * n,), F32), *[S((rs,), F32)] * 6,
    ]
    shapes = [p.shape for p in pieces[2:6]]
    dma = lambda k: pltpu.SemaphoreType.DMA((k,))
    return pl.pallas_call(
        functools.partial(finish, z),
        out_shape=outs,
        in_specs=[any_] * 6 + [vm],
        out_specs=[any_] * 6 + [vm] * 8,
        scratch_shapes=[
            V((z.l, width), BF), V((z.l, width), F32),
            *[V(s, BF) for s in shapes], *[V(s, F32) for s in shapes],
            dma(4), dma(6 * n + 4), dma(2 * n * (z.s + 7) + 4),
        ],
        compiler_params=pltpu.CompilerParams(vmem_limit_bytes=VMEM_LIMIT),
        name="finish",
    )(*pieces)


def make_fused_body(z):
    def body(
        tokens, in_proj, in_bias, out_proj, out_bias, up_proj, up_bias, down_proj, down_bias,
        first_gain, first_shift, second_gain, second_shift, cotangent,
    ):
        vectors = (in_bias, up_bias, out_bias, down_bias, first_gain, first_shift, second_gain, second_shift)
        pieces = fused_call(z, tokens, cotangent, in_proj, up_proj, out_proj, down_proj, vectors)
        mixed, tgrad, g_in, g_up, g_down, g_out, b_in, b_up, b_out, b_down, *rest = finish_call(
            z, pieces
        )
        return (mixed, tgrad, g_in, b_in, g_out, b_out, g_up, b_up, g_down, b_down, *rest)

    return body


def solution(mesh):
    rows = P(("rep", "shard"), None)
    mat = P("shard", None)
    vec = P("shard")
    in_specs = (rows, mat, vec, mat, vec, mat, vec, mat, vec, vec, vec, vec, vec, rows)
    out_specs = (rows, rows, mat, vec, mat, vec, mat, vec, mat, vec, vec, vec, vec, vec)
    shape = dict(mesh.shape)

    def step(*args):
        tokens, up_proj = args[0], args[5]
        devices = shape["rep"] * shape["shard"]
        z = Sizes(shape, tokens.shape[0] // devices, tokens.shape[1], up_proj.shape[1])
        body = make_fused_body(z) if z.fits() else make_body(shape["shard"])
        return jax.shard_map(
            body, mesh=mesh, in_specs=in_specs, out_specs=out_specs, check_vma=False
        )(*args)

    return step
```

```python
import functools

import jax
import jax.numpy as jnp
import numpy as np
from jax import lax
from jax.experimental import pallas as pl
from jax.experimental.pallas import tpu as pltpu
from jax.sharding import PartitionSpec as P

HEAD_DIM = 64
ROT = 16
EPS = 1e-05
MASKED = -1e30


def rotary_tables(length):
    half = ROT // 2
    inverse = jnp.exp(-jnp.log(10000.0) * (2.0 * jnp.arange(half, dtype=jnp.float32) / ROT))
    angles = jnp.arange(length, dtype=jnp.float32)[:, None] * inverse[None, :]
    return (jnp.cos(angles)[:, None, :], jnp.sin(angles)[:, None, :])


def rotate(values, cosine, sine, sign):
    half = ROT // 2
    first = values[..., :half]
    second = values[..., half:ROT]
    return jnp.concatenate(
        [
            first * cosine - sign * second * sine,
            second * cosine + sign * first * sine,
            values[..., ROT:],
        ],
        axis=-1,
    )


def mm(left, right, dims=((1,), (0,))):
    return lax.dot_general(left, right, (dims, ((), ())), preferred_element_type=jnp.float32)


def make_body(parts):
    def body(
        tokens,
        in_proj,
        in_bias,
        out_proj,
        out_bias,
        up_proj,
        up_bias,
        down_proj,
        down_bias,
        first_gain,
        first_shift,
        second_gain,
        second_shift,
        cotangent,
    ):
        length, width = tokens.shape
        me = lax.axis_index("shard")
        heads = width // parts // HEAD_DIM
        span = width // parts
        rows = in_proj.shape[0]
        hidden = up_bias.shape[0]
        scale = HEAD_DIM ** (-0.5)
        vectors = jnp.concatenate(
            [in_bias, out_bias, down_bias, first_gain, first_shift, second_gain, second_shift]
        )
        vectors = lax.all_gather(vectors, "shard", axis=0).astype(jnp.float32)
        cuts = [in_bias.shape[0]] + [span] * 6
        offsets = [sum(cuts[:i]) for i in range(len(cuts))]
        whole = [vectors[:, o : o + c].reshape(-1) for o, c in zip(offsets, cuts)]
        in_b, out_b, down_b, gain1, shift1, gain2, shift2 = whole
        both = lax.all_gather(jnp.stack([tokens, cotangent]), "shard", axis=1, tiled=True)
        x_all, g_all = both[0], both[1]
        w_in = lax.all_to_all(
            in_proj.reshape(rows, 3, parts, span), "shard", 2, 0, tiled=True
        ).reshape(parts * rows, 3 * span)
        w_up = lax.all_to_all(up_proj, "shard", 1, 0, tiled=True)
        b_in = lax.dynamic_slice_in_dim(in_b.reshape(3, parts, span), me, 1, axis=1).reshape(-1)
        x = x_all.astype(jnp.float32)
        mean = jnp.mean(x, axis=1, keepdims=True)
        cen = x - mean
        inv = lax.rsqrt(jnp.mean(cen * cen, axis=1, keepdims=True) + EPS)
        xhat = cen * inv
        attn_in = (xhat * gain1 + shift1).astype(jnp.bfloat16)
        mlp_in = (xhat * gain2 + shift2).astype(jnp.bfloat16)
        total_rows = x.shape[0]
        qkv = (mm(attn_in, w_in) + b_in).reshape(parts, length, 3, heads, HEAD_DIM)
        cosine, sine = rotary_tables(length)
        query = rotate(qkv[:, :, 0], cosine, sine, 1.0).astype(jnp.bfloat16)
        keys = rotate(qkv[:, :, 1], cosine, sine, 1.0).astype(jnp.bfloat16)
        values = qkv[:, :, 2].astype(jnp.bfloat16)
        causal = jnp.arange(length)[:, None] >= jnp.arange(length)[None, :]

        def ein(eq, a, b):
            return jnp.einsum(eq, a, b, preferred_element_type=jnp.float32)

        scores = jnp.where(causal, ein("sqhd,skhd->shqk", query, keys) * scale, MASKED)
        expo = jnp.exp(scores)
        probs_full = expo / jnp.sum(expo, axis=-1, keepdims=True)
        probs = probs_full.astype(jnp.bfloat16)
        attended = ein("shqk,skhd->sqhd", probs, values).astype(jnp.bfloat16)
        attended = attended.reshape(total_rows, span)
        up = mm(mlp_in, w_up) + up_bias.astype(jnp.float32)
        activated, pull = jax.vjp(lambda t: jax.nn.gelu(t, approximate=False), up)
        activated = activated.astype(jnp.bfloat16)
        partial = mm(attended, out_proj) + mm(activated, down_proj)
        branch = lax.psum_scatter(
            partial.astype(jnp.bfloat16), "shard", scatter_dimension=0, tiled=True
        )
        mixed = (tokens.astype(jnp.float32) + branch.astype(jnp.float32) + out_b + down_b).astype(
            jnp.bfloat16
        )
        grad_att = mm(g_all, out_proj, ((1,), (1,))).astype(jnp.bfloat16)
        grad_att = grad_att.reshape(parts, length, heads, HEAD_DIM)
        grad_act = mm(g_all, down_proj, ((1,), (1,)))
        grad_up = pull(grad_act)[0].astype(jnp.bfloat16)
        d_probs = ein("sqhd,skhd->shqk", grad_att, values)
        d_values = ein("shqk,sqhd->skhd", probs, grad_att)
        inner = jnp.sum(d_probs * probs_full, axis=-1, keepdims=True)
        d_scores = (probs_full * (d_probs - inner)).astype(jnp.bfloat16)
        d_query = ein("shqk,skhd->sqhd", d_scores, keys) * scale
        d_keys = ein("shqk,sqhd->skhd", d_scores, query) * scale
        d_query = rotate(d_query, cosine, sine, -1.0)
        d_keys = rotate(d_keys, cosine, sine, -1.0)
        grad_qkv = jnp.stack([d_query, d_keys, d_values], axis=2).astype(jnp.bfloat16)
        grad_qkv = grad_qkv.reshape(total_rows, 3 * span)
        d1 = mm(grad_qkv, w_in, ((1,), (1,)))
        d2 = mm(grad_up, w_up, ((1,), (1,)))
        scaled = (d1 * gain1 + d2 * gain2).astype(jnp.bfloat16)
        e = lax.psum_scatter(scaled, "shard", scatter_dimension=0, tiled=True).astype(jnp.float32)
        own = lambda a: lax.dynamic_slice_in_dim(a, me * length, length, axis=0)
        xh, rv = own(xhat), own(inv)
        tokens_grad = cotangent.astype(jnp.float32) + rv * (
            e - jnp.mean(e, axis=1, keepdims=True) - xh * jnp.mean(e * xh, axis=1, keepdims=True)
        )
        left = ((0,), (0,))
        dw_in = mm(attn_in, grad_qkv, left).astype(jnp.bfloat16)
        dw_up = mm(mlp_in, grad_up, left).astype(jnp.bfloat16)
        dw_out = mm(attended, g_all, left).astype(jnp.bfloat16)
        dw_down = mm(activated, g_all, left).astype(jnp.bfloat16)
        dw_in, dw_up, dw_out, dw_down = lax.psum((dw_in, dw_up, dw_out, dw_down), "rep")
        dw_in = lax.all_to_all(
            dw_in.reshape(parts * rows, 3, 1, span), "shard", 0, 2, tiled=True
        ).reshape(rows, 3 * width)
        dw_up = lax.all_to_all(dw_up, "shard", 0, 1, tiled=True)
        f32 = jnp.float32
        place = lambda v: lax.dynamic_update_slice_in_dim(
            jnp.zeros((3, parts, span), f32), v.reshape(3, 1, span), me, axis=1
        ).reshape(-1)
        vec = [
            place(jnp.sum(grad_qkv, axis=0, dtype=f32)),
            jnp.sum(cotangent.astype(f32), axis=0),
            jnp.sum(d1 * xhat, axis=0),
            jnp.sum(d1, axis=0),
            jnp.sum(d2 * xhat, axis=0),
            jnp.sum(d2, axis=0),
        ]
        vec = jnp.concatenate([v.reshape(parts, -1) for v in vec], axis=1)
        vec = lax.psum_scatter(vec, "shard", scatter_dimension=0, tiled=True)[0]
        vec, up_vec = lax.psum((vec, jnp.sum(grad_up, axis=0, dtype=f32)), "rep")
        o = in_bias.shape[0]
        bias_grad = vec[o : o + span]
        rest = [vec[o + span * i : o + span * (i + 1)] for i in range(1, 5)]
        return (
            mixed,
            tokens_grad,
            dw_in.astype(f32),
            vec[:o],
            dw_out.astype(f32),
            bias_grad,
            dw_up.astype(f32),
            up_vec,
            dw_down.astype(f32),
            bias_grad,
            *rest,
        )

    return body


BF = jnp.bfloat16
F32 = jnp.float32
MESH = pl.DeviceIdType.MESH
VMEM_LIMIT = 67_000_000
NN = ((1,), (0,))
NT = ((1,), (1,))
TN = ((0,), (0,))
IN, UP, DOWN, OUT = range(4)
VECTORS, TOKENS, COTANGENTS, ROWS, OUTPUT, INPUT, SUMS, TOTALS = range(8)


class Sizes:
    def __init__(self, mesh_shape, length, width, hidden):
        self.copies = mesh_shape["rep"]
        self.n = self.copies // 2
        self.s = mesh_shape["shard"]
        self.l = length
        self.d = width
        self.ff = hidden
        self.span = width // self.n
        self.hid = hidden // self.n
        self.rs = width // self.s
        self.hb = hidden // self.s // self.n
        self.rows = self.n * length

    def fits(self):
        return (
            self.copies == 8
            and self.s == 4
            and self.rs == 256
            and self.span == 256
            and self.hb == 256
            and self.l % 256 == 0
        )


def rotary_lanes(length):
    half = ROT // 2
    inverse = np.exp(-np.log(10000.0) * (2.0 * np.arange(half) / ROT))
    angles = np.arange(length)[:, None] * inverse[None, :]
    cosine, sine = np.cos(angles), np.sin(angles)
    table = np.zeros((3, length, 128), np.float32)
    table[0] = 1.0
    for start in (0, HEAD_DIM):
        table[0, :, start : start + half] = cosine
        table[0, :, start + half : start + ROT] = cosine
        table[1, :, start : start + half] = -sine
        table[2, :, start + half : start + ROT] = sine
    return table


def dot(left, right, dims=NN):
    return lax.dot_general(left, right, (dims, ((), ())), preferred_element_type=F32)


def mo(value, m):
    return pl.multiple_of(value, m)


def fused(z, *refs):
    (tok, cot, inp, upp, outp, downp) = refs[:6]
    vectors_in, rot_in = refs[6:14], refs[14]
    (mixed_o, tgrad_o, gin_o, gup_o, gdown_o, gout_o, vec_o) = refs[15:22]
    (
        x_all, g_all, a1, a2, wi, wu, wo, wd, qkv, pt, der, act, att, gatt, gup, gqkv,
        msend, mrecv, mpre, mown, esend, erecv, epre, eown,
        dwi, dwu, dwd, dwo, xri, xru, xrd, xro, zri, zru, zrd, zro, fi, fu, fd, fo,
        vec, va, inb, vfull, vz, vu, vr, stat, vacc, bin_r, bup_r,
        loc, io, one_s, one_r, x_r, g_r, w_s, w_r, wc_s, wc_r, o_r, oc_s, oc_r,
        m_r, e_r, xs_s, xs_r, zs_s, zs_r, zo_s, zo_r, ag_s, ag_r, agc_s, agc_r, agl,
        rot, mixed_v, tgrad_v, vec_v, *vectors_v,
    ) = refs[22:]
    n, s_n, length, width = z.n, z.s, z.l, z.d
    span, hid, rs, hb = z.span, z.hid, z.rs, z.hb
    iw = 3 * span
    scale = HEAD_DIM**-0.5
    r = lax.axis_index("rep")
    zz = lax.axis_index("shard")
    p = lax.div(r, 2)
    c = lax.rem(r, 2)
    other = 1 - c
    partner = (2 * p + other, zz)
    py, px = lax.div(p, 2), lax.rem(p, 2)
    xn, yn, dg = 2 * py + 1 - px, 2 * (1 - py) + px, 2 * (1 - py) + 1 - px
    dev_x, dev_y = (2 * xn + c, zz), (2 * yn + c, zz)
    zp, zo = lax.div(zz, 2), lax.rem(zz, 2)
    is_end = zp == zo
    inner = zp != zo
    mate = 2 * zp + 1 - zo
    mate_dev = (r, mate)
    far_end, far_inner = 3 * (1 - zp), 2 - zp
    to_left, to_right = (r, zz - 1), (r, zz + 1)
    has_left, has_right = zz > 0, zz < s_n - 1

    def rc(src, dst, ss, rr, dev):
        return pltpu.make_async_remote_copy(
            src_ref=src, dst_ref=dst, send_sem=ss, recv_sem=rr, device_id=dev, device_id_type=MESH
        )

    def got(ref, rr):
        rc(ref, ref, rr, rr, partner).wait_recv()

    def seq(ref, s):
        return ref.at[pl.ds(mo(s * length, length), length)]

    def start(copy, cond=None):
        if cond is None:
            copy.start()
        else:
            pl.when(cond)(copy.start)

    def left(ref, ss, cond=None):
        cp = rc(ref, ref, ss, ss, partner)
        if cond is None:
            cp.wait_send()
        else:
            pl.when(cond)(cp.wait_send)

    own_rows = pl.ds(mo(zz * rs, rs), rs)
    own_hb = pl.ds(mo(zz * hb, hb), hb)
    local_u = [
        pltpu.make_async_copy(
            upp.at[:, pl.ds(mo(i * (hb * n) + p * hb, hb), hb)],
            wu.at[own_rows, pl.ds(i * hb, hb)],
            loc.at[1],
        )
        for i in range(s_n)
    ]
    local_i = [
        pltpu.make_async_copy(
            inp.at[:, pl.ds(mo(i * width + (p + n * k) * 128, 128), 128)],
            wi.at[own_rows, pl.ds(i * span + k * 128, 128)],
            loc.at[0],
        )
        for i in range(3)
        for k in range(2)
    ]
    local_d = pltpu.make_async_copy(
        downp.at[pl.ds(mo(p * hb, hb), hb)], wd.at[own_hb], loc.at[2]
    )
    local_x = pltpu.make_async_copy(tok, seq(x_all, p), loc.at[3])
    local_g = pltpu.make_async_copy(cot, seq(g_all, p), loc.at[4])
    local_o = pltpu.make_async_copy(
        outp.at[pl.ds(mo(px * 128, 128), 128)], wo.at[pl.ds(mo(zp * 128, 128), 128)], loc.at[5]
    )
    at_home = zo == py
    away = jnp.logical_not(at_home)
    local_v = [
        pltpu.make_async_copy(src, dst, io.at[i])
        for i, (src, dst) in enumerate(zip(vectors_in, vectors_v))
    ]
    local_r = pltpu.make_async_copy(rot_in, rot, io.at[8])
    for cp in local_v + local_i + [local_x] + local_u + [local_g, local_d, local_r]:
        cp.start()
    pl.when(at_home)(local_o.start)
    off = 0
    for ref, cp in zip(vectors_v, local_v):
        cp.wait()
        size = ref.shape[0]
        vec[:, off : off + size] = ref[...].astype(F32).reshape(1, size)
        off += size

    barrier = pltpu.get_barrier_semaphore()
    for i in range(1, 2 * n):
        pl.semaphore_signal(
            barrier, 1, device_id=(lax.rem(r + i, 2 * n), zz), device_id_type=MESH
        )
    for i in range(1, s_n):
        pl.semaphore_signal(barrier, 1, device_id=(r, lax.rem(zz + i, s_n)), device_id_type=MESH)
    pl.semaphore_wait(barrier, 2 * n - 1 + s_n - 1)

    def line(i):
        q = lax.rem(zz + i, s_n)
        return q, (r, q)

    def plane_send(src, dst, ss, rr, cond=None):
        start(rc(src(0), dst(p, 0), ss, rr(0), dev_x), cond)
        start(rc(src(1), dst(p, 1), ss, rr(1), dev_y), cond)
        start(rc(src(1), dst(p, 1), ss, rr(2), dev_x), cond)
        start(rc(src(0), dst(p, 0), ss, rr(2), dev_y), cond)

    def plane_relay(dst, ss, rr):
        got(dst(xn, 0), rr(0))
        start(rc(dst(xn, 0), dst(xn, 0), ss, rr(3), dev_y))
        got(dst(yn, 1), rr(1))
        start(rc(dst(yn, 1), dst(yn, 1), ss, rr(3), dev_x))

    def plane_near(block, rr):
        got(block, rr(2))

    def plane_far(block, rr):
        got(block, rr(3))

    lh = length // 2

    def part(ref):
        return lambda q, h: ref.at[pl.ds(mo(q * length + h * lh, lh), lh)]

    def sems(ref):
        return lambda i: ref.at[i]

    def rows_of(ref):
        return lambda h: ref.at[pl.ds(h * lh, lh)]

    for i in range(1, s_n):
        q, dev = line(i)
        start(rc(vec, va.at[zz], one_s.at[VECTORS], one_r.at[0], dev))
    plane_send(rows_of(tok), part(x_all), one_s.at[TOKENS], sems(x_r))

    half, hhalf, ohalf = rs // 2, hb // 2, span // 4
    cuts = {IN: 2, UP: 1, DOWN: 1}
    stream = {IN: 0, UP: 2, DOWN: 3}
    weight = {IN: wi, UP: wu, DOWN: wd}

    def piece(t, ref, block):
        rows = block // 2 // cuts[t]
        return lambda q, core, h: ref.at[pl.ds(mo(q * block + core * (block // 2) + h * rows, rows), rows)]

    u_piece, d_piece, i_piece = piece(UP, wu, rs), piece(DOWN, wd, hb), piece(IN, wi, rs)

    def own_sends(t, get):
        for h in range(cuts[t]):
            mine = get(zz, c, h)
            k = stream[t] + h
            start(rc(mine, mine, w_s.at[k], w_r.at[k, zz], to_left), has_left)
            start(rc(mine, mine, w_s.at[k], w_r.at[k, zz], to_right), has_right)

    def relay(t, get, d, who):
        def take(h, q, has, onward, more):
            ref = get(q, c, h)
            k = stream[t] + h

            @pl.when(has)
            def _():
                got(ref, w_r.at[k, q])

            start(rc(ref, ref, w_s.at[k], w_r.at[k, q], onward), jnp.logical_and(has, more))
            start(rc(ref, ref, wc_s.at[k], wc_r.at[k], partner), has)

        for h in range(cuts[t]):
            from_left = jnp.logical_and(who, zz - d >= 0)
            from_right = jnp.logical_and(who, zz + d <= s_n - 1)
            take(h, zz - d, from_left, to_right, has_right)
            take(h, zz + d, from_right, to_left, has_left)

    def pieces(t, count):
        rows = weight[t].shape[0] // s_n // 2 // cuts[t]
        return weight[t].at[pl.ds(0, count * rows)]

    def relay_done(t):
        for h in range(cuts[t]):
            got(pieces(t, s_n - 1), wc_r.at[stream[t] + h])

    pltpu.make_async_copy(wi.at[own_rows], wi.at[own_rows], loc.at[0]).wait()
    own_sends(IN, i_piece)

    got(va.at[pl.ds(0, s_n - 1)], one_r.at[0])
    va[zz] = vec[...]
    n_in = 3 * width // s_n
    n_up = hb * n
    at_up = n_in
    at_rest = n_in + n_up

    def vector(i):
        off = at_rest + i * rs
        return jnp.concatenate([va[q, :, off : off + rs] for q in range(s_n)], axis=1)

    out_b, down_b, gain1, shift1, gain2, shift2 = [vector(i) for i in range(6)]
    for q in range(s_n):
        inb[:, q * n_in : (q + 1) * n_in] = va[q, :, :n_in]

    def norm(s):
        step = 32

        def body(i, carry):
            row = pl.ds(mo(s * length + i * step, step), step)
            xv = x_all[row, :].astype(F32)
            mu = jnp.mean(xv, axis=1, keepdims=True)
            cen = xv - mu
            inv = lax.rsqrt(jnp.mean(cen * cen, axis=1, keepdims=True) + EPS)
            xh = cen * inv
            a1[row, :] = (xh * gain1 + shift1).astype(BF)
            a2[row, :] = (xh * gain2 + shift2).astype(BF)
            stat[row, 0:1] = mu
            stat[row, 1:2] = inv
            return carry

        lax.fori_loop(0, length // step, body, 0)

    local_r.wait()
    table = [rot[i] for i in range(3)]

    def turn(t, sign):
        fwd = pltpu.roll(t, 128 - ROT // 2, 1)
        back = pltpu.roll(t, ROT // 2, 1)
        return t * table[0] + (fwd * table[1] + back * table[2]) * sign

    def turn_of(k):
        return jnp.where(k == 0, p, jnp.where(k == 1, xn, jnp.where(k == 2, yn, dg)))

    def qkv_block(k, carry):
        row = pl.ds(mo(turn_of(k) * length, length), length)
        left_a = a1[row, :]
        for i in range(3):
            v = dot(left_a, wi[:, i * span : (i + 1) * span])
            for h in range(2):
                bias = inb[:, pl.ds(mo(i * width + (p + n * h) * 128, 128), 128)]
                cut = v[:, h * 128 : (h + 1) * 128] + bias
                if i < 2:
                    cut = turn(cut, 1.0)
                qkv[row, i * span + h * 128 : i * span + (h + 1) * 128] = cut.astype(BF)
        return carry

    relay(IN, i_piece, 1, inner)
    local_x.wait()
    norm(p)
    relay(IN, i_piece, 2, inner)
    pltpu.make_async_copy(wu.at[own_rows], wu.at[own_rows], loc.at[1]).wait()
    own_sends(UP, u_piece)
    plane_relay(part(x_all), one_s.at[TOKENS], sems(x_r))
    plane_send(rows_of(cot), part(g_all), one_s.at[COTANGENTS], sems(g_r))
    plane_near(seq(x_all, xn), sems(x_r))
    norm(xn)
    norm(yn)
    relay(UP, u_piece, 1, inner)
    for d in range(1, s_n):
        relay(IN, i_piece, d, is_end)
    relay_done(IN)
    lax.fori_loop(0, 3, qkv_block, 0)
    relay(UP, u_piece, 2, inner)
    local_d.wait()
    own_sends(DOWN, d_piece)
    def o_piece(block, core):
        return wo.at[pl.ds(mo(block * 128 + core * ohalf, ohalf), ohalf)]

    pl.when(at_home)(local_o.wait)
    near_first = (mate_dev, (r, far_inner), (r, far_end))
    for dev in near_first:
        start(rc(o_piece(zp, c), o_piece(zp, c), one_s.at[ROWS], o_r.at[zp], dev), at_home)
    plane_far(seq(x_all, dg), sems(x_r))
    norm(dg)
    lax.fori_loop(3, n, qkv_block, 0)
    plane_relay(part(g_all), one_s.at[COTANGENTS], sems(g_r))

    lane = lax.broadcasted_iota(jnp.int32, (1, 128), 1)
    first = lane < HEAD_DIM
    masks = [first.astype(F32).astype(BF), (1.0 - first.astype(F32)).astype(BF)]
    pairs = span // 128

    def att_forward(idx, carry):
        s = lax.div(idx, pairs)
        pr = lax.rem(idx, pairs)
        row = pl.ds(mo(s * length, length), length)
        q2 = qkv[row, pl.ds(mo(pr * 128, 128), 128)]
        k2 = qkv[row, pl.ds(mo(span + pr * 128, 128), 128)]
        v2 = qkv[row, pl.ds(mo(2 * span + pr * 128, 128), 128)]
        key_i = lax.broadcasted_iota(jnp.int32, (length, length), 0)
        query_i = lax.broadcasted_iota(jnp.int32, (length, length), 1)
        found = []
        for h in range(2):
            st = dot(k2, q2 * masks[h], NT) * scale
            ex = jnp.exp(jnp.where(key_i <= query_i, st, MASKED))
            pr_t = ex / jnp.sum(ex, axis=0, keepdims=True)
            pt[idx * 2 + h] = pr_t
            found.append(dot(pr_t.astype(BF), v2, TN))
        att[row, pl.ds(mo(pr * 128, 128), 128)] = jnp.where(first, found[0], found[1]).astype(BF)
        return carry

    lax.fori_loop(0, n * pairs // 2, att_forward, 0)
    relay(DOWN, d_piece, 1, inner)
    lax.fori_loop(n * pairs // 2, n * pairs, att_forward, 0)
    for d in range(1, s_n):
        relay(UP, u_piece, d, is_end)
    relay_done(UP)

    def up_block(s, carry):
        row = pl.ds(mo(s * length, length), length)
        left_a = a2[row, :]
        for j in range(s_n):
            col = pl.ds(j * hb, hb)
            bias = va[j, :, pl.ds(mo(at_up + p * hb, hb), hb)]
            u = dot(left_a, wu[:, j * hb : (j + 1) * hb]) + bias
            phi = 0.5 * (1.0 + lax.erf(u * 0.7071067811865476))
            act[row, col] = (u * phi).astype(BF)
            der[row, col] = phi + u * (0.3989422804014327 * jnp.exp(-0.5 * u * u))
        return carry

    lax.fori_loop(0, n, up_block, 0)
    relay(DOWN, d_piece, 2, inner)

    def exchange(t, dw, xr, block_half):
        src = dw.at[:, pl.ds(mo(other * block_half, block_half), block_half)]
        start(rc(src, xr, xs_s.at[t], xs_r.at[t], partner))

    def core_sum(t, dw, xr, block_half):
        mine = pl.ds(mo(c * block_half, block_half), block_half)
        got(xr, xs_r.at[t])

        def body(q, carry):
            xr[q] = (dw[q, mine].astype(F32) + xr[q].astype(F32)).astype(BF)
            return carry

        lax.fori_loop(0, dw.shape[0], body, 0)

    def pair_sum(t, dw, xr, zr, block_half):
        core_sum(t, dw, xr, block_half)
        start(rc(xr.at[far_end], zr.at[2], zs_s.at[t], zs_r.at[t, 1], mate_dev), is_end)
        start(rc(xr.at[far_inner], zr.at[3], zs_s.at[t], zs_r.at[t, 2], mate_dev), is_end)
        start(rc(xr.at[mate], zr.at[0], zs_s.at[t], zs_r.at[t, 0], mate_dev))

    def pass_on(t, xr, zr):
        @pl.when(inner)
        def _():
            for slot, q in ((2, far_end), (3, far_inner)):
                got(zr.at[slot], zs_r.at[t, slot - 1])
                xr[q] = (xr[q].astype(F32) + zr[slot].astype(F32)).astype(BF)
                rc(xr.at[q], zr.at[1], zs_s.at[t], zs_r.at[t, 0], (r, q)).start()

    def line_sum(t, xr, zr, fin):
        got(zr.at[pl.ds(0, 2)], zs_r.at[t, 0])
        total = xr[zz].astype(F32) + zr[0].astype(F32) + zr[1].astype(F32)
        fin[...] = total.astype(BF)

    outs_of = {IN: (gin_o, fi), UP: (gup_o, fu), DOWN: (gdown_o, fd)}

    def area(t):
        o = outs_of[t][0]
        rows = o.shape[2] // 2
        return lambda q, h: o.at[q, c, pl.ds(h * rows, rows)]

    def fin_half(t):
        fin = outs_of[t][1]
        rows = fin.shape[0] // 2
        return lambda h: fin.at[pl.ds(h * rows, rows)]

    local_out = []

    def spread(t):
        o, fin = outs_of[t]
        plane_send(fin_half(t), area(t), ag_s.at[t], sems(ag_r.at[t]))
        start(rc(fin, o.at[p, c], agc_s.at[t], agc_r.at[t], partner))
        cp = pltpu.make_async_copy(fin, o.at[p, c], agl.at[t])
        cp.start()
        local_out.append((None, cp))

    def spread_relay(t):
        plane_relay(area(t), ag_s.at[t], sems(ag_r.at[t]))

    def across(t, q):
        o = outs_of[t][0]
        start(rc(o.at[q, c], o.at[q, c], agc_s.at[t], agc_r.at[t], partner))

    def spread_near(t):
        plane_near(outs_of[t][0].at[xn, c], sems(ag_r.at[t]))
        across(t, xn)
        across(t, yn)

    def spread_far(t):
        plane_far(outs_of[t][0].at[dg, c], sems(ag_r.at[t]))
        across(t, dg)

    def spread_end(t):
        got(outs_of[t][0].at[:, other], agc_r.at[t])

    local_g.wait()
    plane_near(seq(g_all, xn), sems(g_r))
    plane_far(seq(g_all, dg), sems(g_r))

    dwo_all = dot(att[...], g_all[...], TN).astype(BF)
    for i in range(2):
        dwo[i] = dwo_all[i * 128 : (i + 1) * 128]
    exchange(OUT, dwo, xro, ohalf)
    for j in range(s_n):
        dwd[j] = dot(act[:, j * hb : (j + 1) * hb], g_all[...], TN).astype(BF)
    exchange(DOWN, dwd, xrd, hhalf)
    core_sum(OUT, dwo, xro, ohalf)
    near_b, far_b = zp, 1 - zp
    start(rc(xro.at[far_b], zro.at[2], zo_s.at[0], zo_r.at[1], mate_dev), is_end)
    start(rc(xro.at[near_b], zro.at[0], zo_s.at[1], zo_r.at[0], mate_dev), away)
    pair_sum(DOWN, dwd, xrd, zrd, hhalf)

    def o_take(k, block, cond):
        ref = o_piece(block, c)

        @pl.when(cond)
        def _():
            got(ref, o_r.at[block])

        start(rc(ref, ref, oc_s.at[k], oc_r.at[k], partner), cond)

    def o_done(k, block, cond):
        @pl.when(cond)
        def _():
            got(o_piece(block, other), oc_r.at[k])

    always = zz >= 0
    o_take(0, near_b, away)
    o_take(1, far_b, always)
    o_done(0, near_b, away)
    o_done(1, far_b, always)

    bup_r[...] = jnp.zeros_like(bup_r)
    bin_r[...] = jnp.zeros_like(bin_r)

    def grad_att_block(s, carry):
        row = pl.ds(mo(s * length, length), length)
        gatt[row, :] = dot(g_all[row, :], wo[...], NT).astype(BF)
        return carry

    lax.fori_loop(0, n, grad_att_block, 0)

    def att_backward(idx, carry):
        s = lax.div(idx, pairs)
        pr = lax.rem(idx, pairs)
        row = pl.ds(mo(s * length, length), length)
        q_col = pl.ds(mo(pr * 128, 128), 128)
        k_col = pl.ds(mo(span + pr * 128, 128), 128)
        v_col = pl.ds(mo(2 * span + pr * 128, 128), 128)
        q2, k2, v2 = qkv[row, q_col], qkv[row, k_col], qkv[row, v_col]
        g2 = gatt[row, q_col]
        dq, dk, dv = [], [], []
        for h in range(2):
            pr_t = pt[idx * 2 + h]
            dp = dot(v2, g2 * masks[h], NT)
            total = jnp.sum(dp * pr_t, axis=0, keepdims=True)
            ds = (pr_t * (dp - total)).astype(BF)
            dv.append(dot(pr_t.astype(BF), g2))
            dk.append(dot(ds, q2))
            dq.append(dot(ds, k2, TN))
        dqv = turn(jnp.where(first, dq[0], dq[1]) * scale, -1.0).astype(BF)
        dkv = turn(jnp.where(first, dk[0], dk[1]) * scale, -1.0).astype(BF)
        dvv = jnp.where(first, dv[0], dv[1]).astype(BF)
        for col, val in ((q_col, dqv), (k_col, dkv), (v_col, dvv)):
            gqkv[row, col] = val
            bin_r[:, col] += jnp.sum(val.astype(F32), axis=0, keepdims=True)
        return carry

    lax.fori_loop(0, n * pairs - 4, att_backward, 0)
    on = rc(xro.at[far_b], zro.at[1], zo_s.at[0], zo_r.at[0], (r, 2 * (1 - zp) + py))

    @pl.when(inner)
    def _():
        got(zro.at[2], zo_r.at[1])
        xro[far_b] = (xro[far_b].astype(F32) + zro[2].astype(F32)).astype(BF)
        on.start()

    lax.fori_loop(n * pairs - 4, n * pairs - 2, att_backward, 0)

    for d in range(1, s_n):
        relay(DOWN, d_piece, d, is_end)
    relay_done(DOWN)

    def shares(k, send, recv, pre, ss, rr):
        row = lambda h: pl.ds(h * lh, lh)

        @pl.when(k == 0)
        def _():
            rc(send.at[0, row(0)], pre.at[0], ss, rr.at[0], dev_x).start()
            rc(send.at[0, row(1)], pre.at[1], ss, rr.at[1], dev_y).start()

        @pl.when(k == 1)
        def _():
            rc(send.at[1, row(0)], recv.at[0, row(0)], ss, rr.at[2], dev_x).start()

        @pl.when(k == 2)
        def _():
            rc(send.at[2, row(1)], recv.at[1, row(1)], ss, rr.at[2], dev_y).start()

    def shares_on(send, recv, pre, ss, rr):
        for k, h, dev in ((1, 1, dev_x), (2, 0, dev_y)):
            got(pre.at[h], rr.at[h])
            row = pl.ds(h * lh, lh)
            send[k, row] = (send[k, row].astype(F32) + pre[h].astype(F32)).astype(BF)
            start(rc(send.at[k, row], recv.at[k - 1, row], ss, rr.at[2], dev))

    def share_of(k):
        return jnp.where(k == 0, dg, jnp.where(k == 1, xn, jnp.where(k == 2, yn, p)))

    m_refs = (msend, mrecv, mpre, one_s.at[OUTPUT], m_r)
    e_refs = (esend, erecv, epre, one_s.at[INPUT], e_r)

    def out_block(k, carry):
        row = pl.ds(mo(share_of(k) * length, length), length)
        for j in range(width // 256):
            col = slice(j * 256, (j + 1) * 256)
            v = dot(att[row, :], wo[:, col]) + dot(act[row, :], wd[:, col])
            msend[k, :, col] = v.astype(BF)
            mown[:, col] = v
        shares(k, *m_refs)
        return carry

    lax.fori_loop(0, n, out_block, 0)
    @pl.when(at_home)
    def _():
        got(zro.at[pl.ds(0, 2)], zo_r.at[0])
        total = xro[near_b].astype(F32) + zro[0].astype(F32) + zro[1].astype(F32)
        fo[...] = total.astype(BF)

    oq = ohalf // 2

    def o_whole(q):
        return gout_o.at[lax.rem(q, 2), c]

    def o_area(q, h):
        return gout_o.at[lax.rem(q, 2), c, pl.ds(h * oq, oq)]

    plane_send(lambda h: fo.at[pl.ds(h * oq, oq)], o_area, ag_s.at[OUT], sems(ag_r.at[OUT]), at_home)
    start(rc(fo, o_whole(p), agc_s.at[OUT], agc_r.at[OUT], partner), at_home)
    cp = pltpu.make_async_copy(fo, o_whole(p), agl.at[OUT])
    pl.when(at_home)(cp.start)
    local_out.append((at_home, cp))

    pass_on(DOWN, xrd, zrd)
    lax.fori_loop(n * pairs - 2, n * pairs, att_backward, 0)
    shares_on(*m_refs)

    for j in range(s_n):
        dwi[j] = dot(a1[:, j * rs : (j + 1) * rs], gqkv[...], TN).astype(BF)
    exchange(IN, dwi, xri, half)

    def grad_up_block(s, carry):
        row = pl.ds(mo(s * length, length), length)
        gs = g_all[row, :]
        for j in range(s_n):
            col = pl.ds(j * hb, hb)
            gu = (dot(gs, wd[j * hb : (j + 1) * hb, :], NT) * der[row, col]).astype(BF)
            gup[row, col] = gu
            bup_r[:, col] += jnp.sum(gu.astype(F32), axis=0, keepdims=True)
        return carry

    lax.fori_loop(0, 2, grad_up_block, 0)
    pair_sum(IN, dwi, xri, zri, half)
    lax.fori_loop(2, n, grad_up_block, 0)
    for j in range(s_n):
        dwu[j] = dot(a2[:, j * rs : (j + 1) * rs], gup[...], TN).astype(BF)
    exchange(UP, dwu, xru, half)

    vacc[...] = jnp.zeros_like(vacc)

    def in_block(k, carry):
        row = pl.ds(mo(share_of(k) * length, length), length)
        gq = gqkv[row, :]
        gu = gup[row, :]
        mu = stat[row, 0:1]
        inv = stat[row, 1:2]
        for j in range(s_n):
            col = slice(j * rs, (j + 1) * rs)
            d1 = dot(gq, wi[col, :], NT)
            d2 = dot(gu, wu[col, :], NT)
            xh = (x_all[row, col].astype(F32) - mu) * inv
            vacc[0, :, col] += jnp.sum(d1 * xh, axis=0, keepdims=True)
            vacc[1, :, col] += jnp.sum(d1, axis=0, keepdims=True)
            vacc[2, :, col] += jnp.sum(d2 * xh, axis=0, keepdims=True)
            vacc[3, :, col] += jnp.sum(d2, axis=0, keepdims=True)
            e = d1 * gain1[:, col] + d2 * gain2[:, col]
            esend[k, :, col] = e.astype(BF)
            eown[:, col] = e
        shares(k, *e_refs)
        return carry

    lax.fori_loop(0, 1, in_block, 0)
    pair_sum(UP, dwu, xru, zru, half)
    lax.fori_loop(1, 3, in_block, 0)
    pass_on(IN, xri, zri)
    lax.fori_loop(3, n, in_block, 0)

    line_sum(DOWN, xrd, zrd, fd)
    spread(DOWN)

    shares_on(*e_refs)

    slots = vfull.shape[0] // s_n
    vfull[...] = jnp.zeros_like(vfull)
    per = n_in // 128
    for i in range(3):
        for h in range(2):
            b = i * 2 * n + p + n * h
            col = slice(i * span + h * 128, i * span + (h + 1) * 128)
            vfull[lax.div(b, per) * slots + lax.rem(b, per)] = bin_r[:, col]
    at_g = per + 2 * n
    for q in range(s_n):
        for h in range(2):
            up_col = slice(q * hb + h * 128, q * hb + (h + 1) * 128)
            vfull[q * slots + per + 2 * p + h] = bup_r[:, up_col]
            col = slice(q * rs + h * 128, q * rs + (h + 1) * 128)
            g_own = g_all[pl.ds(mo(p * length, length), length), col].astype(F32)
            vfull[q * slots + at_g + h] = jnp.sum(g_own, axis=0, keepdims=True)
            for i in range(4):
                vfull[q * slots + at_g + 2 + 2 * i + h] = vacc[i, :, col]
    for i in range(1, s_n):
        q, dev = line(i)
        start(rc(vfull.at[pl.ds(q * slots, slots)], vz.at[zz], one_s.at[SUMS], one_r.at[1], dev))

    pass_on(UP, xru, zru)

    got(mrecv, m_r.at[2])

    def mixed_rows(i, carry):
        step = 32
        row = pl.ds(mo(i * step, step), step)
        xv = x_all[pl.ds(mo(p * length + i * step, step), step), :].astype(F32)
        t = mown[row, :] + mrecv[0, row, :].astype(F32) + mrecv[1, row, :].astype(F32)
        mixed_v[row, :] = (xv + t + out_b + down_b).astype(BF)
        return carry

    lax.fori_loop(0, length // 32, mixed_rows, 0)
    mixed_out = pltpu.make_async_copy(mixed_v, mixed_o, io.at[9])
    mixed_out.start()

    spread_relay(DOWN)
    line_sum(IN, xri, zri, fi)
    spread(IN)
    def o_got(ref, k, cond):
        @pl.when(cond)
        def _():
            got(ref, ag_r.at[OUT, k])

    o_got(o_area(xn, 0), 0, at_home)
    start(rc(o_area(xn, 0), o_area(xn, 0), ag_s.at[OUT], ag_r.at[OUT, 3], dev_y), at_home)
    o_got(o_area(yn, 1), 1, away)
    start(rc(o_area(yn, 1), o_area(yn, 1), ag_s.at[OUT], ag_r.at[OUT, 3], dev_x), away)
    line_sum(UP, xru, zru, fu)
    spread(UP)

    spread_relay(IN)

    spread_near(DOWN)
    spread_far(DOWN)
    total = [vfull[zz * slots + k] for k in range(slots)]
    got(vz.at[pl.ds(0, s_n - 1)], one_r.at[1])
    for i in range(1, s_n):
        q, dev = line(i)
        total = [t + vz[q, k] for k, t in enumerate(total)]
    for k in range(slots):
        vu[k] = total[k]
        vr[r, k] = total[k]
    for i in range(1, 2 * n):
        start(rc(vu, vr.at[r], one_s.at[TOTALS], one_r.at[2], (lax.rem(r + i, 2 * n), zz)))

    got(erecv, e_r.at[2])

    def tgrad_rows(i, carry):
        step = 32
        row = pl.ds(mo(i * step, step), step)
        far = pl.ds(mo(p * length + i * step, step), step)
        inv = stat[far, 1:2]
        xh = (x_all[far, :].astype(F32) - stat[far, 0:1]) * inv
        e = eown[row, :] + erecv[0, row, :].astype(F32) + erecv[1, row, :].astype(F32)
        m0 = jnp.mean(e, axis=1, keepdims=True)
        m1 = jnp.mean(e * xh, axis=1, keepdims=True)
        tgrad_v[row, :] = g_all[far, :].astype(F32) + inv * (e - m0 - xh * m1)
        return carry

    lax.fori_loop(0, length // 32, tgrad_rows, 0)
    tgrad_out = pltpu.make_async_copy(tgrad_v, tgrad_o, io.at[10])
    tgrad_out.start()

    spread_relay(UP)
    o_got(o_area(xn, 1), 2, at_home)
    start(rc(o_whole(xn), o_whole(xn), agc_s.at[OUT], agc_r.at[OUT], partner), at_home)
    o_got(o_area(yn, 0), 2, away)
    start(rc(o_whole(yn), o_whole(yn), agc_s.at[OUT], agc_r.at[OUT], partner), away)
    o_got(o_whole(dg), 3, away)
    start(rc(o_whole(dg), o_whole(dg), agc_s.at[OUT], agc_r.at[OUT], partner), away)

    spread_near(IN)
    spread_far(IN)
    got(vr.at[pl.ds(0, 2 * n - 1)], one_r.at[2])
    for k in range(slots):
        t = vr[0, k]
        for q in range(1, 2 * n):
            t = t + vr[q, k]
        vec_v[k] = t
    vec_out = pltpu.make_async_copy(vec_v, vec_o, io.at[11])
    vec_out.start()
    spread_near(UP)
    spread_far(UP)
    for t in (DOWN, IN, UP):
        spread_end(t)
    two = wo.at[pl.ds(0, 2 * ohalf)]
    got(two, agc_r.at[OUT])

    for cond, cp in local_out:
        if cond is None:
            cp.wait()
        else:
            pl.when(cond)(cp.wait)
    for cp in (mixed_out, tgrad_out, vec_out):
        cp.wait()
    left(va.at[pl.ds(0, s_n - 1)], one_s.at[VECTORS])
    left(x_all.at[pl.ds(0, 3 * length)], one_s.at[TOKENS])
    left(g_all.at[pl.ds(0, 3 * length)], one_s.at[COTANGENTS])
    left(wo.at[pl.ds(0, 3 * ohalf)], one_s.at[ROWS], at_home)
    left(msend.at[pl.ds(0, 3)], one_s.at[OUTPUT])
    left(esend.at[pl.ds(0, 3)], one_s.at[INPUT])
    left(vz.at[pl.ds(0, s_n - 1)], one_s.at[SUMS])
    left(vr.at[pl.ds(0, 2 * n - 1)], one_s.at[TOTALS])
    for t in (IN, UP, DOWN):
        for h in range(cuts[t]):
            k = stream[t] + h
            left(pieces(t, 1), w_s.at[k], is_end)
            left(pieces(t, 5), w_s.at[k], inner)
            left(pieces(t, s_n - 1), wc_s.at[k])
    left(o_piece(0, 0), oc_s.at[0], away)
    left(o_piece(0, 0), oc_s.at[1])
    for t, xr in ((IN, xri), (UP, xru), (DOWN, xrd), (OUT, xro)):
        left(xr, xs_s.at[t])
    for t, xr in ((IN, xri), (UP, xru), (DOWN, xrd)):
        left(xr.at[pl.ds(0, 3)], zs_s.at[t])
        left(outs_of[t][0].at[pl.ds(0, 3), 0], ag_s.at[t])
        left(outs_of[t][0].at[:, 0], agc_s.at[t])
    left(xro.at[0], zo_s.at[0])
    left(xro.at[0], zo_s.at[1], away)
    left(wo.at[pl.ds(0, 5 * oq)], ag_s.at[OUT], at_home)
    left(wo.at[pl.ds(0, oq)], ag_s.at[OUT], away)
    left(two, agc_s.at[OUT])


def fused_call(z, tok, cot, inp, upp, outp, downp, vectors):
    n, s_n, length, width, span, hid = z.n, z.s, z.l, z.d, z.span, z.hid
    rs, hb, rows = z.rs, z.hb, z.rows
    iw = 3 * span
    nv = sum(v.shape[0] for v in vectors)
    slots = (3 * width // s_n + hb * n + 5 * rs) // 128
    V = pltpu.VMEM
    dma = lambda *shape: pltpu.SemaphoreType.DMA(shape)
    share = [
        V((n, length, width), BF), V((2, length, width), BF), V((2, length // 2, width), BF),
        V((length, width), F32),
    ]
    halves = [
        V((s_n, rs // 2, iw), BF), V((s_n, rs // 2, hid), BF), V((s_n, hb // 2, width), BF),
    ]
    scratch = [
        *[V((rows, width), BF)] * 4,
        V((width, iw), BF), V((width, hid), BF), V((span, width), BF), V((hid, width), BF),
        V((rows, iw), BF), V((n * span // HEAD_DIM, length, length), F32),
        V((rows, hid), F32), V((rows, hid), BF), V((rows, span), BF),
        V((rows, span), BF), V((rows, hid), BF), V((rows, iw), BF),
        *share, *share,
        V((s_n, rs, iw), BF), V((s_n, rs, hid), BF), V((s_n, hb, width), BF), V((2, span // 2, width), BF),
        *halves, V((2, span // 4, width), BF),
        *halves, V((3, span // 4, width), BF),
        V((rs // 2, iw), BF), V((rs // 2, hid), BF), V((hb // 2, width), BF), V((span // 4, width), BF),
        V((1, nv), F32), V((s_n, 1, nv), F32), V((1, 3 * width), F32), V((s_n * slots, 1, 128), F32),
        V((s_n, slots, 1, 128), F32), V((slots, 1, 128), F32), V((2 * n, slots, 1, 128), F32),
        V((rows, 2), F32), V((4, 1, width), F32), V((1, iw), F32), V((1, hid), F32),
        dma(6), dma(12), dma(8), dma(3), dma(4), dma(4), dma(4), dma(4, s_n), dma(4), dma(4), dma(2), dma(2), dma(2),
        dma(3), dma(3), dma(4), dma(4), dma(3), dma(3, 3), dma(2), dma(2), dma(4), dma(4, 4), dma(4), dma(4), dma(4),
        V((3, length, 128), F32), V((length, width), BF), V((length, width), F32), V((slots, 1, 128), F32),
        *[V(v.shape, BF) for v in vectors],
    ]
    any_ = pl.BlockSpec(memory_space=pl.ANY)
    outs = [
        jax.ShapeDtypeStruct((length, width), BF),
        jax.ShapeDtypeStruct((length, width), F32),
        jax.ShapeDtypeStruct((n, 2, rs // 2, iw), BF),
        jax.ShapeDtypeStruct((n, 2, rs // 2, hid), BF),
        jax.ShapeDtypeStruct((n, 2, hb // 2, width), BF),
        jax.ShapeDtypeStruct((2, 2, span // 4, width), BF),
        jax.ShapeDtypeStruct((slots, 1, 128), F32),
    ]
    return pl.pallas_call(
        functools.partial(fused, z),
        out_shape=outs,
        in_specs=[any_] * 15,
        out_specs=[any_] * 7,
        scratch_shapes=scratch,
        compiler_params=pltpu.CompilerParams(
            collective_id=0, has_side_effects=True, vmem_limit_bytes=VMEM_LIMIT
        ),
        name="block_step",
    )(tok, cot, inp, upp, outp, downp, *vectors, jnp.asarray(rotary_lanes(length)))


def finish(z, *refs):
    mixed, tgrad, g_in, g_up, g_down, g_out, vec = refs[:7]
    mixed_o, tgrad_o, in_o, up_o, down_o, out_o = refs[7:13]
    vec_o = refs[13:21]
    m_v, t_v, v_v, bi, bu, bd, bo, fi, fu, fd, fo = refs[21:32]
    vec_v, (io, r_sem, w_sem) = refs[32:40], refs[40:]
    n, s_n, width, span, hb, rs = z.n, z.s, z.d, z.span, z.hb, z.rs
    half, hhalf, quarter = rs // 2, hb // 2, span // 4
    through = [
        (pltpu.make_async_copy(a, b, io.at[i]), pltpu.make_async_copy(b, o, io.at[3 + i]))
        for i, (a, b, o) in enumerate(((mixed, m_v, mixed_o), (tgrad, t_v, tgrad_o)))
    ]
    vec_in = pltpu.make_async_copy(vec, v_v, io.at[2])
    blocks = []
    for q in range(n):
        blocks.append((1, g_up.at[q], bu.at[q], fu.at[q], [
            (core, up_o.at[core * half : (core + 1) * half, (k * n + q) * hb : (k * n + q + 1) * hb], slice(k * hb, (k + 1) * hb))
            for core in range(2) for k in range(s_n)
        ]))
    for q in range(n):
        blocks.append((2, g_down.at[q], bd.at[q], fd.at[q], [
            (core, down_o.at[q * hb + core * hhalf : q * hb + (core + 1) * hhalf], slice(None)) for core in range(2)
        ]))
    for q in range(n):
        blocks.append((0, g_in.at[q], bi.at[q], fi.at[q], [
            (core, in_o.at[core * half : (core + 1) * half, k * width + (q + n * h) * 128 : k * width + (q + n * h + 1) * 128],
             slice(k * span + h * 128, k * span + (h + 1) * 128))
            for core in range(2) for k in range(3) for h in range(2)
        ]))
    for j in range(2):
        blocks.append((3, g_out.at[j], bo.at[j], fo.at[j], [
            (core, out_o.at[(2 * j + core) * quarter : (2 * j + core + 1) * quarter], slice(None)) for core in range(2)
        ]))
    reads = [pltpu.make_async_copy(src, dst, r_sem.at[i]) for i, (_, src, dst, _, _) in enumerate(blocks)]
    for cp in [reads[0], *(a for a, _ in through), vec_in, *reads[1:]]:
        cp.start()
    for (t, _, low, wide, places), read in zip(blocks, reads):
        read.wait()
        for core in range(2):

            def body(i, carry, core=core, low=low, wide=wide):
                row = pl.ds(mo(i * 32, 32), 32)
                wide[core, row, :] = low[core, row, :].astype(F32)
                return carry

            lax.fori_loop(0, low.shape[1] // 32, body, 0)
        for core, place, col in places:
            pltpu.make_async_copy(wide.at[core, :, col], place, w_sem.at[t]).start()
    for a, b in through:
        a.wait()
        b.start()
    vec_in.wait()
    k = 0
    small = []
    for i, (ref, out) in enumerate(zip(vec_v, vec_o)):
        count = ref.shape[0] // 128
        if i == 3:
            k -= count
        for j in range(count):
            ref[j * 128 : (j + 1) * 128] = v_v[k + j].reshape(128)
        k += count
        small.append(pltpu.make_async_copy(ref, out, io.at[5 + i]))
        small[-1].start()
    for t, wide in enumerate((fi, fu, fd, fo)):
        pltpu.make_async_copy(wide, wide, w_sem.at[t]).wait()
    for cp in [b for _, b in through] + small:
        cp.wait()


def finish_call(z, pieces):
    n, width, span, rs = z.n, z.d, z.span, z.rs
    V = pltpu.VMEM
    S = jax.ShapeDtypeStruct
    any_ = pl.BlockSpec(memory_space=pl.ANY)
    small = [3 * width // z.s, z.hb * n] + [rs] * 6
    outs = [
        S((z.l, width), BF), S((z.l, width), F32), S((rs, 3 * width), F32), S((rs, z.ff), F32),
        S((z.hb * n, width), F32), S((span, width), F32), *[S((k,), F32) for k in small],
    ]
    shapes = [p.shape for p in pieces[2:6]]
    dma = lambda k: pltpu.SemaphoreType.DMA((k,))
    return pl.pallas_call(
        functools.partial(finish, z),
        out_shape=outs,
        in_specs=[any_] * 7,
        out_specs=[any_] * 14,
        scratch_shapes=[
            V((z.l, width), BF), V((z.l, width), F32), V(pieces[6].shape, F32),
            *[V(s, BF) for s in shapes], *[V(s, F32) for s in shapes],
            *[V((k,), F32) for k in small],
            dma(13), dma(3 * n + 2), dma(4),
        ],
        compiler_params=pltpu.CompilerParams(vmem_limit_bytes=VMEM_LIMIT),
        name="finish",
    )(*pieces)


def make_fused_body(z):
    def body(
        tokens, in_proj, in_bias, out_proj, out_bias, up_proj, up_bias, down_proj, down_bias,
        first_gain, first_shift, second_gain, second_shift, cotangent,
    ):
        vectors = (in_bias, up_bias, out_bias, down_bias, first_gain, first_shift, second_gain, second_shift)
        pieces = fused_call(z, tokens, cotangent, in_proj, up_proj, out_proj, down_proj, vectors)
        mixed, tgrad, g_in, g_up, g_down, g_out, b_in, b_up, b_out, b_down, *rest = finish_call(
            z, pieces
        )
        return (mixed, tgrad, g_in, b_in, g_out, b_out, g_up, b_up, g_down, b_down, *rest)

    return body


def solution(mesh):
    rows = P(("rep", "shard"), None)
    mat = P("shard", None)
    vec = P("shard")
    in_specs = (rows, mat, vec, mat, vec, mat, vec, mat, vec, vec, vec, vec, vec, rows)
    out_specs = (rows, rows, mat, vec, mat, vec, mat, vec, mat, vec, vec, vec, vec, vec)
    shape = dict(mesh.shape)

    def step(*args):
        tokens, up_proj = args[0], args[5]
        devices = shape["rep"] * shape["shard"]
        z = Sizes(shape, tokens.shape[0] // devices, tokens.shape[1], up_proj.shape[1])
        body = make_fused_body(z) if z.fits() else make_body(shape["shard"])
        return jax.shard_map(
            body, mesh=mesh, in_specs=in_specs, out_specs=out_specs, check_vma=False
        )(*args)

    return step
```

```python
import functools

import jax
import jax.numpy as jnp
import numpy as np
from jax import lax
from jax.experimental import pallas as pl
from jax.experimental.pallas import tpu as pltpu
from jax.sharding import PartitionSpec as P

HEAD_DIM = 64
ROT = 16
EPS = 1e-05
MASKED = -1e30


def rotary_tables(length):
    half = ROT // 2
    inverse = jnp.exp(-jnp.log(10000.0) * (2.0 * jnp.arange(half, dtype=jnp.float32) / ROT))
    angles = jnp.arange(length, dtype=jnp.float32)[:, None] * inverse[None, :]
    return (jnp.cos(angles)[:, None, :], jnp.sin(angles)[:, None, :])


def rotate(values, cosine, sine, sign):
    half = ROT // 2
    first = values[..., :half]
    second = values[..., half:ROT]
    return jnp.concatenate(
        [
            first * cosine - sign * second * sine,
            second * cosine + sign * first * sine,
            values[..., ROT:],
        ],
        axis=-1,
    )


def mm(left, right, dims=((1,), (0,))):
    return lax.dot_general(left, right, (dims, ((), ())), preferred_element_type=jnp.float32)


def make_body(parts):
    def body(
        tokens,
        in_proj,
        in_bias,
        out_proj,
        out_bias,
        up_proj,
        up_bias,
        down_proj,
        down_bias,
        first_gain,
        first_shift,
        second_gain,
        second_shift,
        cotangent,
    ):
        length, width = tokens.shape
        me = lax.axis_index("shard")
        heads = width // parts // HEAD_DIM
        span = width // parts
        rows = in_proj.shape[0]
        hidden = up_bias.shape[0]
        scale = HEAD_DIM ** (-0.5)
        vectors = jnp.concatenate(
            [in_bias, out_bias, down_bias, first_gain, first_shift, second_gain, second_shift]
        )
        vectors = lax.all_gather(vectors, "shard", axis=0).astype(jnp.float32)
        cuts = [in_bias.shape[0]] + [span] * 6
        offsets = [sum(cuts[:i]) for i in range(len(cuts))]
        whole = [vectors[:, o : o + c].reshape(-1) for o, c in zip(offsets, cuts)]
        in_b, out_b, down_b, gain1, shift1, gain2, shift2 = whole
        both = lax.all_gather(jnp.stack([tokens, cotangent]), "shard", axis=1, tiled=True)
        x_all, g_all = both[0], both[1]
        w_in = lax.all_to_all(
            in_proj.reshape(rows, 3, parts, span), "shard", 2, 0, tiled=True
        ).reshape(parts * rows, 3 * span)
        w_up = lax.all_to_all(up_proj, "shard", 1, 0, tiled=True)
        b_in = lax.dynamic_slice_in_dim(in_b.reshape(3, parts, span), me, 1, axis=1).reshape(-1)
        x = x_all.astype(jnp.float32)
        mean = jnp.mean(x, axis=1, keepdims=True)
        cen = x - mean
        inv = lax.rsqrt(jnp.mean(cen * cen, axis=1, keepdims=True) + EPS)
        xhat = cen * inv
        attn_in = (xhat * gain1 + shift1).astype(jnp.bfloat16)
        mlp_in = (xhat * gain2 + shift2).astype(jnp.bfloat16)
        total_rows = x.shape[0]
        qkv = (mm(attn_in, w_in) + b_in).reshape(parts, length, 3, heads, HEAD_DIM)
        cosine, sine = rotary_tables(length)
        query = rotate(qkv[:, :, 0], cosine, sine, 1.0).astype(jnp.bfloat16)
        keys = rotate(qkv[:, :, 1], cosine, sine, 1.0).astype(jnp.bfloat16)
        values = qkv[:, :, 2].astype(jnp.bfloat16)
        causal = jnp.arange(length)[:, None] >= jnp.arange(length)[None, :]

        def ein(eq, a, b):
            return jnp.einsum(eq, a, b, preferred_element_type=jnp.float32)

        scores = jnp.where(causal, ein("sqhd,skhd->shqk", query, keys) * scale, MASKED)
        expo = jnp.exp(scores)
        probs_full = expo / jnp.sum(expo, axis=-1, keepdims=True)
        probs = probs_full.astype(jnp.bfloat16)
        attended = ein("shqk,skhd->sqhd", probs, values).astype(jnp.bfloat16)
        attended = attended.reshape(total_rows, span)
        up = mm(mlp_in, w_up) + up_bias.astype(jnp.float32)
        activated, pull = jax.vjp(lambda t: jax.nn.gelu(t, approximate=False), up)
        activated = activated.astype(jnp.bfloat16)
        partial = mm(attended, out_proj) + mm(activated, down_proj)
        branch = lax.psum_scatter(
            partial.astype(jnp.bfloat16), "shard", scatter_dimension=0, tiled=True
        )
        mixed = (tokens.astype(jnp.float32) + branch.astype(jnp.float32) + out_b + down_b).astype(
            jnp.bfloat16
        )
        grad_att = mm(g_all, out_proj, ((1,), (1,))).astype(jnp.bfloat16)
        grad_att = grad_att.reshape(parts, length, heads, HEAD_DIM)
        grad_act = mm(g_all, down_proj, ((1,), (1,)))
        grad_up = pull(grad_act)[0].astype(jnp.bfloat16)
        d_probs = ein("sqhd,skhd->shqk", grad_att, values)
        d_values = ein("shqk,sqhd->skhd", probs, grad_att)
        inner = jnp.sum(d_probs * probs_full, axis=-1, keepdims=True)
        d_scores = (probs_full * (d_probs - inner)).astype(jnp.bfloat16)
        d_query = ein("shqk,skhd->sqhd", d_scores, keys) * scale
        d_keys = ein("shqk,sqhd->skhd", d_scores, query) * scale
        d_query = rotate(d_query, cosine, sine, -1.0)
        d_keys = rotate(d_keys, cosine, sine, -1.0)
        grad_qkv = jnp.stack([d_query, d_keys, d_values], axis=2).astype(jnp.bfloat16)
        grad_qkv = grad_qkv.reshape(total_rows, 3 * span)
        d1 = mm(grad_qkv, w_in, ((1,), (1,)))
        d2 = mm(grad_up, w_up, ((1,), (1,)))
        scaled = (d1 * gain1 + d2 * gain2).astype(jnp.bfloat16)
        e = lax.psum_scatter(scaled, "shard", scatter_dimension=0, tiled=True).astype(jnp.float32)
        own = lambda a: lax.dynamic_slice_in_dim(a, me * length, length, axis=0)
        xh, rv = own(xhat), own(inv)
        tokens_grad = cotangent.astype(jnp.float32) + rv * (
            e - jnp.mean(e, axis=1, keepdims=True) - xh * jnp.mean(e * xh, axis=1, keepdims=True)
        )
        left = ((0,), (0,))
        dw_in = mm(attn_in, grad_qkv, left).astype(jnp.bfloat16)
        dw_up = mm(mlp_in, grad_up, left).astype(jnp.bfloat16)
        dw_out = mm(attended, g_all, left).astype(jnp.bfloat16)
        dw_down = mm(activated, g_all, left).astype(jnp.bfloat16)
        dw_in, dw_up, dw_out, dw_down = lax.psum((dw_in, dw_up, dw_out, dw_down), "rep")
        dw_in = lax.all_to_all(
            dw_in.reshape(parts * rows, 3, 1, span), "shard", 0, 2, tiled=True
        ).reshape(rows, 3 * width)
        dw_up = lax.all_to_all(dw_up, "shard", 0, 1, tiled=True)
        f32 = jnp.float32
        place = lambda v: lax.dynamic_update_slice_in_dim(
            jnp.zeros((3, parts, span), f32), v.reshape(3, 1, span), me, axis=1
        ).reshape(-1)
        vec = [
            place(jnp.sum(grad_qkv, axis=0, dtype=f32)),
            jnp.sum(cotangent.astype(f32), axis=0),
            jnp.sum(d1 * xhat, axis=0),
            jnp.sum(d1, axis=0),
            jnp.sum(d2 * xhat, axis=0),
            jnp.sum(d2, axis=0),
        ]
        vec = jnp.concatenate([v.reshape(parts, -1) for v in vec], axis=1)
        vec = lax.psum_scatter(vec, "shard", scatter_dimension=0, tiled=True)[0]
        vec, up_vec = lax.psum((vec, jnp.sum(grad_up, axis=0, dtype=f32)), "rep")
        o = in_bias.shape[0]
        bias_grad = vec[o : o + span]
        rest = [vec[o + span * i : o + span * (i + 1)] for i in range(1, 5)]
        return (
            mixed,
            tokens_grad,
            dw_in.astype(f32),
            vec[:o],
            dw_out.astype(f32),
            bias_grad,
            dw_up.astype(f32),
            up_vec,
            dw_down.astype(f32),
            bias_grad,
            *rest,
        )

    return body


BF = jnp.bfloat16
F32 = jnp.float32
MESH = pl.DeviceIdType.MESH
VMEM_LIMIT = 67_000_000
NN = ((1,), (0,))
NT = ((1,), (1,))
TN = ((0,), (0,))
IN, UP, DOWN, OUT = range(4)
VECTORS, TOKENS, COTANGENTS, ROWS, OUTPUT, INPUT, SUMS, TOTALS = range(8)


class Sizes:
    def __init__(self, mesh_shape, length, width, hidden):
        self.copies = mesh_shape["rep"]
        self.n = self.copies // 2
        self.s = mesh_shape["shard"]
        self.l = length
        self.d = width
        self.ff = hidden
        self.span = width // self.n
        self.hid = hidden // self.n
        self.rs = width // self.s
        self.hb = hidden // self.s // self.n
        self.rows = self.n * length

    def fits(self):
        return (
            self.copies == 8
            and self.s == 4
            and self.rs == 256
            and self.span == 256
            and self.hb == 256
            and self.l % 256 == 0
        )


def rotary_lanes(length):
    half = ROT // 2
    inverse = np.exp(-np.log(10000.0) * (2.0 * np.arange(half) / ROT))
    angles = np.arange(length)[:, None] * inverse[None, :]
    cosine, sine = np.cos(angles), np.sin(angles)
    table = np.zeros((3, length, 128), np.float32)
    table[0] = 1.0
    for start in (0, HEAD_DIM):
        table[0, :, start : start + half] = cosine
        table[0, :, start + half : start + ROT] = cosine
        table[1, :, start : start + half] = -sine
        table[2, :, start + half : start + ROT] = sine
    return table


def dot(left, right, dims=NN):
    return lax.dot_general(left, right, (dims, ((), ())), preferred_element_type=F32)


def mo(value, m):
    return pl.multiple_of(value, m)


def fused(z, *refs):
    (tok, cot, inp, upp, outp, downp) = refs[:6]
    vectors_in, rot_in = refs[6:14], refs[14]
    (mixed_o, tgrad_o, gin_o, gup_o, gdown_o, gout_o, vec_o) = refs[15:22]
    (
        x_all, g_all, a1, a2, wi, wu, wo, wd, qkv, pt, der, act, att, gatt, gup, gqkv,
        msend, mrecv, mpre, mown, esend, erecv, epre, eown,
        dwi, dwu, dwd, dwo, xri, xru, xrd, xro, zri, zru, zrd, zro, fi, fu, fd, fo,
        vec, va, inb, vfull, vz, vu, vr, stat, vacc, bin_r, bup_r,
        loc, io, one_s, one_r, x_r, g_r, w_s, w_r, wc_s, wc_r, o_r, oc_s, oc_r,
        m_r, e_r, xs_s, xs_r, zs_s, zs_r, zo_s, zo_r, ag_s, ag_r, agc_s, agc_r, agl,
        rot, mixed_v, tgrad_v, vec_v, *vectors_v,
    ) = refs[22:]
    n, s_n, length, width = z.n, z.s, z.l, z.d
    span, hid, rs, hb = z.span, z.hid, z.rs, z.hb
    iw = 3 * span
    scale = HEAD_DIM**-0.5
    r = lax.axis_index("rep")
    zz = lax.axis_index("shard")
    p = lax.div(r, 2)
    c = lax.rem(r, 2)
    other = 1 - c
    partner = (2 * p + other, zz)
    py, px = lax.div(p, 2), lax.rem(p, 2)
    xn, yn, dg = 2 * py + 1 - px, 2 * (1 - py) + px, 2 * (1 - py) + 1 - px
    dev_x, dev_y = (2 * xn + c, zz), (2 * yn + c, zz)
    zp, zo = lax.div(zz, 2), lax.rem(zz, 2)
    is_end = zp == zo
    inner = zp != zo
    mate = 2 * zp + 1 - zo
    mate_dev = (r, mate)
    far_end, far_inner = 3 * (1 - zp), 2 - zp
    to_left, to_right = (r, zz - 1), (r, zz + 1)
    has_left, has_right = zz > 0, zz < s_n - 1

    def rc(src, dst, ss, rr, dev):
        return pltpu.make_async_remote_copy(
            src_ref=src, dst_ref=dst, send_sem=ss, recv_sem=rr, device_id=dev, device_id_type=MESH
        )

    def got(ref, rr):
        rc(ref, ref, rr, rr, partner).wait_recv()

    def seq(ref, s):
        return ref.at[pl.ds(mo(s * length, length), length)]

    def start(copy, cond=None):
        if cond is None:
            copy.start()
        else:
            pl.when(cond)(copy.start)

    def left(ref, ss, cond=None):
        cp = rc(ref, ref, ss, ss, partner)
        if cond is None:
            cp.wait_send()
        else:
            pl.when(cond)(cp.wait_send)

    own_rows = pl.ds(mo(zz * rs, rs), rs)
    own_hb = pl.ds(mo(zz * hb, hb), hb)
    local_u = [
        pltpu.make_async_copy(
            upp.at[:, pl.ds(mo(i * (hb * n) + p * hb, hb), hb)],
            wu.at[own_rows, pl.ds(i * hb, hb)],
            loc.at[1],
        )
        for i in range(s_n)
    ]
    local_i = [
        pltpu.make_async_copy(
            inp.at[:, pl.ds(mo(i * width + (p + n * k) * 128, 128), 128)],
            wi.at[own_rows, pl.ds(i * span + k * 128, 128)],
            loc.at[0],
        )
        for i in range(3)
        for k in range(2)
    ]
    local_d = pltpu.make_async_copy(
        downp.at[pl.ds(mo(p * hb, hb), hb)], wd.at[own_hb], loc.at[2]
    )
    local_x = pltpu.make_async_copy(tok, seq(x_all, p), loc.at[3])
    local_g = pltpu.make_async_copy(cot, seq(g_all, p), loc.at[4])
    local_o = pltpu.make_async_copy(
        outp.at[pl.ds(mo(px * 128, 128), 128)], wo.at[pl.ds(mo(zp * 128, 128), 128)], loc.at[5]
    )
    at_home = zo == py
    away = jnp.logical_not(at_home)
    local_v = [
        pltpu.make_async_copy(src, dst, io.at[i])
        for i, (src, dst) in enumerate(zip(vectors_in, vectors_v))
    ]
    local_r = pltpu.make_async_copy(rot_in, rot, io.at[8])
    for cp in local_v + local_i + [local_x] + local_u + [local_g, local_d, local_r]:
        cp.start()
    pl.when(at_home)(local_o.start)
    barrier = pltpu.get_barrier_semaphore()
    for i in range(1, 2 * n):
        pl.semaphore_signal(
            barrier, 1, device_id=(lax.rem(r + i, 2 * n), zz), device_id_type=MESH
        )
    for i in range(1, s_n):
        pl.semaphore_signal(barrier, 1, device_id=(r, lax.rem(zz + i, s_n)), device_id_type=MESH)
    off = 0
    for ref, cp in zip(vectors_v, local_v):
        cp.wait()
        size = ref.shape[0]
        vec[:, off : off + size] = ref[...].astype(F32).reshape(1, size)
        off += size
    pl.semaphore_wait(barrier, 2 * n - 1 + s_n - 1)

    def line(i):
        q = lax.rem(zz + i, s_n)
        return q, (r, q)

    def plane_send(src, dst, ss, rr, cond=None):
        start(rc(src(0), dst(p, 0), ss, rr(0), dev_x), cond)
        start(rc(src(1), dst(p, 1), ss, rr(1), dev_y), cond)
        start(rc(src(1), dst(p, 1), ss, rr(2), dev_x), cond)
        start(rc(src(0), dst(p, 0), ss, rr(2), dev_y), cond)

    def plane_relay(dst, ss, rr):
        got(dst(xn, 0), rr(0))
        start(rc(dst(xn, 0), dst(xn, 0), ss, rr(3), dev_y))
        got(dst(yn, 1), rr(1))
        start(rc(dst(yn, 1), dst(yn, 1), ss, rr(3), dev_x))

    def plane_near(block, rr):
        got(block, rr(2))

    def plane_far(block, rr):
        got(block, rr(3))

    lh = length // 2

    def part(ref):
        return lambda q, h: ref.at[pl.ds(mo(q * length + h * lh, lh), lh)]

    def sems(ref):
        return lambda i: ref.at[i]

    def rows_of(ref):
        return lambda h: ref.at[pl.ds(h * lh, lh)]

    for i in range(1, s_n):
        q, dev = line(i)
        start(rc(vec, va.at[zz], one_s.at[VECTORS], one_r.at[0], dev))
    plane_send(rows_of(tok), part(x_all), one_s.at[TOKENS], sems(x_r))

    half, hhalf, ohalf = rs // 2, hb // 2, span // 4
    cuts = {IN: 2, UP: 1, DOWN: 1}
    stream = {IN: 0, UP: 2, DOWN: 3}
    weight = {IN: wi, UP: wu, DOWN: wd}

    def piece(t, ref, block):
        rows = block // 2 // cuts[t]
        return lambda q, core, h: ref.at[pl.ds(mo(q * block + core * (block // 2) + h * rows, rows), rows)]

    u_piece, d_piece, i_piece = piece(UP, wu, rs), piece(DOWN, wd, hb), piece(IN, wi, rs)

    def own_sends(t, get):
        for h in range(cuts[t]):
            mine = get(zz, c, h)
            k = stream[t] + h
            start(rc(mine, mine, w_s.at[k], w_r.at[k, zz], to_left), has_left)
            start(rc(mine, mine, w_s.at[k], w_r.at[k, zz], to_right), has_right)

    def relay(t, get, d, who):
        def take(h, q, has, onward, more):
            ref = get(q, c, h)
            k = stream[t] + h

            @pl.when(has)
            def _():
                got(ref, w_r.at[k, q])

            start(rc(ref, ref, w_s.at[k], w_r.at[k, q], onward), jnp.logical_and(has, more))
            start(rc(ref, ref, wc_s.at[k], wc_r.at[k], partner), has)

        for h in range(cuts[t]):
            from_left = jnp.logical_and(who, zz - d >= 0)
            from_right = jnp.logical_and(who, zz + d <= s_n - 1)
            take(h, zz - d, from_left, to_right, has_right)
            take(h, zz + d, from_right, to_left, has_left)

    def pieces(t, count):
        rows = weight[t].shape[0] // s_n // 2 // cuts[t]
        return weight[t].at[pl.ds(0, count * rows)]

    def relay_done(t):
        for h in range(cuts[t]):
            got(pieces(t, s_n - 1), wc_r.at[stream[t] + h])

    pltpu.make_async_copy(wi.at[own_rows], wi.at[own_rows], loc.at[0]).wait()
    own_sends(IN, i_piece)

    got(va.at[pl.ds(0, s_n - 1)], one_r.at[0])
    va[zz] = vec[...]
    n_in = 3 * width // s_n
    n_up = hb * n
    at_up = n_in
    at_rest = n_in + n_up

    def vector(i):
        off = at_rest + i * rs
        return jnp.concatenate([va[q, :, off : off + rs] for q in range(s_n)], axis=1)

    out_b, down_b, gain1, shift1, gain2, shift2 = [vector(i) for i in range(6)]
    for q in range(s_n):
        inb[:, q * n_in : (q + 1) * n_in] = va[q, :, :n_in]

    def norm(s):
        step = 32

        def body(i, carry):
            row = pl.ds(mo(s * length + i * step, step), step)
            xv = x_all[row, :].astype(F32)
            mu = jnp.mean(xv, axis=1, keepdims=True)
            cen = xv - mu
            inv = lax.rsqrt(jnp.mean(cen * cen, axis=1, keepdims=True) + EPS)
            xh = cen * inv
            a1[row, :] = (xh * gain1 + shift1).astype(BF)
            a2[row, :] = (xh * gain2 + shift2).astype(BF)
            stat[row, 0:1] = mu
            stat[row, 1:2] = inv
            return carry

        lax.fori_loop(0, length // step, body, 0)

    local_r.wait()
    table = [rot[i] for i in range(3)]

    def turn(t, sign):
        fwd = pltpu.roll(t, 128 - ROT // 2, 1)
        back = pltpu.roll(t, ROT // 2, 1)
        return t * table[0] + (fwd * table[1] + back * table[2]) * sign

    def turn_of(k):
        return jnp.where(k == 0, p, jnp.where(k == 1, xn, jnp.where(k == 2, yn, dg)))

    def qkv_block(k, carry):
        row = pl.ds(mo(turn_of(k) * length, length), length)
        left_a = a1[row, :]
        for i in range(3):
            v = dot(left_a, wi[:, i * span : (i + 1) * span])
            for h in range(2):
                bias = inb[:, pl.ds(mo(i * width + (p + n * h) * 128, 128), 128)]
                cut = v[:, h * 128 : (h + 1) * 128] + bias
                if i < 2:
                    cut = turn(cut, 1.0)
                qkv[row, i * span + h * 128 : i * span + (h + 1) * 128] = cut.astype(BF)
        return carry

    relay(IN, i_piece, 1, inner)
    local_x.wait()
    norm(p)
    relay(IN, i_piece, 2, inner)
    pltpu.make_async_copy(wu.at[own_rows], wu.at[own_rows], loc.at[1]).wait()
    own_sends(UP, u_piece)
    plane_relay(part(x_all), one_s.at[TOKENS], sems(x_r))
    plane_send(rows_of(cot), part(g_all), one_s.at[COTANGENTS], sems(g_r))
    plane_near(seq(x_all, xn), sems(x_r))
    norm(xn)
    norm(yn)
    relay(UP, u_piece, 1, inner)
    for d in range(1, s_n):
        relay(IN, i_piece, d, is_end)
    relay_done(IN)
    lax.fori_loop(0, 3, qkv_block, 0)
    relay(UP, u_piece, 2, inner)
    local_d.wait()
    own_sends(DOWN, d_piece)
    def o_piece(block, core):
        return wo.at[pl.ds(mo(block * 128 + core * ohalf, ohalf), ohalf)]

    pl.when(at_home)(local_o.wait)
    near_first = (mate_dev, (r, far_inner), (r, far_end))
    for dev in near_first:
        start(rc(o_piece(zp, c), o_piece(zp, c), one_s.at[ROWS], o_r.at[zp], dev), at_home)
    plane_far(seq(x_all, dg), sems(x_r))
    norm(dg)
    lax.fori_loop(3, n, qkv_block, 0)
    plane_relay(part(g_all), one_s.at[COTANGENTS], sems(g_r))

    lane = lax.broadcasted_iota(jnp.int32, (1, 128), 1)
    first = lane < HEAD_DIM
    masks = [first.astype(F32).astype(BF), (1.0 - first.astype(F32)).astype(BF)]
    pairs = span // 128

    def att_forward(idx, carry):
        s = lax.div(idx, pairs)
        pr = lax.rem(idx, pairs)
        row = pl.ds(mo(s * length, length), length)
        q2 = qkv[row, pl.ds(mo(pr * 128, 128), 128)]
        k2 = qkv[row, pl.ds(mo(span + pr * 128, 128), 128)]
        v2 = qkv[row, pl.ds(mo(2 * span + pr * 128, 128), 128)]
        key_i = lax.broadcasted_iota(jnp.int32, (length, length), 0)
        query_i = lax.broadcasted_iota(jnp.int32, (length, length), 1)
        found = []
        for h in range(2):
            st = dot(k2, q2 * masks[h], NT) * scale
            ex = jnp.exp(jnp.where(key_i <= query_i, st, MASKED))
            pr_t = ex / jnp.sum(ex, axis=0, keepdims=True)
            pt[idx * 2 + h] = pr_t
            found.append(dot(pr_t.astype(BF), v2, TN))
        att[row, pl.ds(mo(pr * 128, 128), 128)] = jnp.where(first, found[0], found[1]).astype(BF)
        return carry

    lax.fori_loop(0, n * pairs // 2, att_forward, 0)
    relay(DOWN, d_piece, 1, inner)
    for d in range(1, s_n - 1):
        relay(UP, u_piece, d, is_end)
    lax.fori_loop(n * pairs // 2, n * pairs, att_forward, 0)
    relay(UP, u_piece, s_n - 1, is_end)
    relay_done(UP)

    def up_block(s, carry):
        row = pl.ds(mo(s * length, length), length)
        left_a = a2[row, :]
        for j in range(s_n):
            col = pl.ds(j * hb, hb)
            bias = va[j, :, pl.ds(mo(at_up + p * hb, hb), hb)]
            u = dot(left_a, wu[:, j * hb : (j + 1) * hb]) + bias
            phi = 0.5 * (1.0 + lax.erf(u * 0.7071067811865476))
            act[row, col] = (u * phi).astype(BF)
            der[row, col] = phi + u * (0.3989422804014327 * jnp.exp(-0.5 * u * u))
        return carry

    lax.fori_loop(0, n, up_block, 0)
    relay(DOWN, d_piece, 2, inner)

    def exchange(t, dw, xr, block_half):
        src = dw.at[:, pl.ds(mo(other * block_half, block_half), block_half)]
        start(rc(src, xr, xs_s.at[t], xs_r.at[t], partner))

    def core_sum(t, dw, xr, block_half):
        mine = pl.ds(mo(c * block_half, block_half), block_half)
        got(xr, xs_r.at[t])

        def body(q, carry):
            xr[q] = (dw[q, mine].astype(F32) + xr[q].astype(F32)).astype(BF)
            return carry

        lax.fori_loop(0, dw.shape[0], body, 0)

    def pair_sum(t, dw, xr, zr, block_half):
        core_sum(t, dw, xr, block_half)
        start(rc(xr.at[far_end], zr.at[2], zs_s.at[t], zs_r.at[t, 1], mate_dev), is_end)
        start(rc(xr.at[far_inner], zr.at[3], zs_s.at[t], zs_r.at[t, 2], mate_dev), is_end)
        start(rc(xr.at[mate], zr.at[0], zs_s.at[t], zs_r.at[t, 0], mate_dev))

    def pass_on(t, xr, zr):
        @pl.when(inner)
        def _():
            for slot, q in ((2, far_end), (3, far_inner)):
                got(zr.at[slot], zs_r.at[t, slot - 1])
                xr[q] = (xr[q].astype(F32) + zr[slot].astype(F32)).astype(BF)
                rc(xr.at[q], zr.at[1], zs_s.at[t], zs_r.at[t, 0], (r, q)).start()

    def line_sum(t, xr, zr, fin):
        got(zr.at[pl.ds(0, 2)], zs_r.at[t, 0])
        total = xr[zz].astype(F32) + zr[0].astype(F32) + zr[1].astype(F32)
        fin[...] = total.astype(BF)

    outs_of = {IN: (gin_o, fi), UP: (gup_o, fu), DOWN: (gdown_o, fd)}

    def area(t):
        o = outs_of[t][0]
        rows = o.shape[2] // 2
        return lambda q, h: o.at[q, c, pl.ds(h * rows, rows)]

    def fin_half(t):
        fin = outs_of[t][1]
        rows = fin.shape[0] // 2
        return lambda h: fin.at[pl.ds(h * rows, rows)]

    local_out = []

    def spread(t):
        o, fin = outs_of[t]
        plane_send(fin_half(t), area(t), ag_s.at[t], sems(ag_r.at[t]))
        start(rc(fin, o.at[p, c], agc_s.at[t], agc_r.at[t], partner))
        cp = pltpu.make_async_copy(fin, o.at[p, c], agl.at[t])
        cp.start()
        local_out.append((None, cp))

    def spread_relay(t):
        plane_relay(area(t), ag_s.at[t], sems(ag_r.at[t]))

    def across(t, q):
        o = outs_of[t][0]
        start(rc(o.at[q, c], o.at[q, c], agc_s.at[t], agc_r.at[t], partner))

    def spread_near(t):
        plane_near(outs_of[t][0].at[xn, c], sems(ag_r.at[t]))
        across(t, xn)
        across(t, yn)

    def spread_far(t):
        plane_far(outs_of[t][0].at[dg, c], sems(ag_r.at[t]))
        across(t, dg)

    def spread_end(t):
        got(outs_of[t][0].at[:, other], agc_r.at[t])

    local_g.wait()
    plane_near(seq(g_all, xn), sems(g_r))
    plane_far(seq(g_all, dg), sems(g_r))

    dwo_all = dot(att[...], g_all[...], TN).astype(BF)
    for i in range(2):
        dwo[i] = dwo_all[i * 128 : (i + 1) * 128]
    exchange(OUT, dwo, xro, ohalf)
    for j in range(s_n):
        dwd[j] = dot(act[:, j * hb : (j + 1) * hb], g_all[...], TN).astype(BF)
    exchange(DOWN, dwd, xrd, hhalf)
    core_sum(OUT, dwo, xro, ohalf)
    near_b, far_b = zp, 1 - zp
    start(rc(xro.at[far_b], zro.at[2], zo_s.at[0], zo_r.at[1], mate_dev), is_end)
    start(rc(xro.at[near_b], zro.at[0], zo_s.at[1], zo_r.at[0], mate_dev), away)
    pair_sum(DOWN, dwd, xrd, zrd, hhalf)

    def o_take(k, block, cond):
        ref = o_piece(block, c)

        @pl.when(cond)
        def _():
            got(ref, o_r.at[block])

        start(rc(ref, ref, oc_s.at[k], oc_r.at[k], partner), cond)

    def o_done(k, block, cond):
        @pl.when(cond)
        def _():
            got(o_piece(block, other), oc_r.at[k])

    always = zz >= 0
    o_take(0, near_b, away)
    o_take(1, far_b, always)
    o_done(0, near_b, away)
    o_done(1, far_b, always)

    bup_r[...] = jnp.zeros_like(bup_r)
    bin_r[...] = jnp.zeros_like(bin_r)

    def grad_att_block(s, carry):
        row = pl.ds(mo(s * length, length), length)
        gatt[row, :] = dot(g_all[row, :], wo[...], NT).astype(BF)
        return carry

    lax.fori_loop(0, n, grad_att_block, 0)

    def att_backward(idx, carry):
        s = lax.div(idx, pairs)
        pr = lax.rem(idx, pairs)
        row = pl.ds(mo(s * length, length), length)
        q_col = pl.ds(mo(pr * 128, 128), 128)
        k_col = pl.ds(mo(span + pr * 128, 128), 128)
        v_col = pl.ds(mo(2 * span + pr * 128, 128), 128)
        q2, k2, v2 = qkv[row, q_col], qkv[row, k_col], qkv[row, v_col]
        g2 = gatt[row, q_col]
        dq, dk, dv = [], [], []
        for h in range(2):
            pr_t = pt[idx * 2 + h]
            dp = dot(v2, g2 * masks[h], NT)
            total = jnp.sum(dp * pr_t, axis=0, keepdims=True)
            ds = (pr_t * (dp - total)).astype(BF)
            dv.append(dot(pr_t.astype(BF), g2))
            dk.append(dot(ds, q2))
            dq.append(dot(ds, k2, TN))
        dqv = turn(jnp.where(first, dq[0], dq[1]) * scale, -1.0).astype(BF)
        dkv = turn(jnp.where(first, dk[0], dk[1]) * scale, -1.0).astype(BF)
        dvv = jnp.where(first, dv[0], dv[1]).astype(BF)
        for col, val in ((q_col, dqv), (k_col, dkv), (v_col, dvv)):
            gqkv[row, col] = val
            bin_r[:, col] += jnp.sum(val.astype(F32), axis=0, keepdims=True)
        return carry

    lax.fori_loop(0, n * pairs - 4, att_backward, 0)
    on = rc(xro.at[far_b], zro.at[1], zo_s.at[0], zo_r.at[0], (r, 2 * (1 - zp) + py))

    @pl.when(inner)
    def _():
        got(zro.at[2], zo_r.at[1])
        xro[far_b] = (xro[far_b].astype(F32) + zro[2].astype(F32)).astype(BF)
        on.start()

    for d in range(1, s_n - 1):
        relay(DOWN, d_piece, d, is_end)
    lax.fori_loop(n * pairs - 4, n * pairs - 2, att_backward, 0)

    relay(DOWN, d_piece, s_n - 1, is_end)
    relay_done(DOWN)

    def shares(k, send, recv, pre, ss, rr):
        row = lambda h: pl.ds(h * lh, lh)

        @pl.when(k == 0)
        def _():
            rc(send.at[0, row(0)], pre.at[0], ss, rr.at[0], dev_x).start()
            rc(send.at[0, row(1)], pre.at[1], ss, rr.at[1], dev_y).start()

        @pl.when(k == 1)
        def _():
            rc(send.at[1, row(0)], recv.at[0, row(0)], ss, rr.at[2], dev_x).start()

        @pl.when(k == 2)
        def _():
            rc(send.at[2, row(1)], recv.at[1, row(1)], ss, rr.at[2], dev_y).start()

    def shares_on(send, recv, pre, ss, rr):
        for k, h, dev in ((1, 1, dev_x), (2, 0, dev_y)):
            got(pre.at[h], rr.at[h])
            row = pl.ds(h * lh, lh)
            send[k, row] = (send[k, row].astype(F32) + pre[h].astype(F32)).astype(BF)
            start(rc(send.at[k, row], recv.at[k - 1, row], ss, rr.at[2], dev))

    def share_of(k):
        return jnp.where(k == 0, dg, jnp.where(k == 1, xn, jnp.where(k == 2, yn, p)))

    m_refs = (msend, mrecv, mpre, one_s.at[OUTPUT], m_r)
    e_refs = (esend, erecv, epre, one_s.at[INPUT], e_r)

    def out_block(k, carry):
        row = pl.ds(mo(share_of(k) * length, length), length)
        for j in range(width // 256):
            col = slice(j * 256, (j + 1) * 256)
            v = dot(att[row, :], wo[:, col]) + dot(act[row, :], wd[:, col])
            msend[k, :, col] = v.astype(BF)
            mown[:, col] = v
        shares(k, *m_refs)
        return carry

    lax.fori_loop(0, n, out_block, 0)
    @pl.when(at_home)
    def _():
        got(zro.at[pl.ds(0, 2)], zo_r.at[0])
        total = xro[near_b].astype(F32) + zro[0].astype(F32) + zro[1].astype(F32)
        fo[...] = total.astype(BF)

    def o_whole(q):
        return gout_o.at[lax.rem(q, 2), c]

    start(rc(fo, o_whole(p), ag_s.at[OUT], ag_r.at[OUT, 0], dev_x), at_home)
    start(rc(fo, o_whole(p), ag_s.at[OUT], ag_r.at[OUT, 1], dev_y), at_home)
    start(rc(fo, o_whole(p), agc_s.at[OUT], agc_r.at[OUT], partner), at_home)
    cp = pltpu.make_async_copy(fo, o_whole(p), agl.at[OUT])
    pl.when(at_home)(cp.start)
    local_out.append((at_home, cp))

    pass_on(DOWN, xrd, zrd)
    lax.fori_loop(n * pairs - 2, n * pairs, att_backward, 0)
    shares_on(*m_refs)

    for j in range(s_n):
        dwi[j] = dot(a1[:, j * rs : (j + 1) * rs], gqkv[...], TN).astype(BF)
    exchange(IN, dwi, xri, half)

    def grad_up_block(s, carry):
        row = pl.ds(mo(s * length, length), length)
        gs = g_all[row, :]
        for j in range(s_n):
            col = pl.ds(j * hb, hb)
            gu = (dot(gs, wd[j * hb : (j + 1) * hb, :], NT) * der[row, col]).astype(BF)
            gup[row, col] = gu
            bup_r[:, col] += jnp.sum(gu.astype(F32), axis=0, keepdims=True)
        return carry

    lax.fori_loop(0, 2, grad_up_block, 0)
    pair_sum(IN, dwi, xri, zri, half)
    lax.fori_loop(2, n, grad_up_block, 0)
    for j in range(s_n):
        dwu[j] = dot(a2[:, j * rs : (j + 1) * rs], gup[...], TN).astype(BF)
    exchange(UP, dwu, xru, half)

    vacc[...] = jnp.zeros_like(vacc)

    def in_block(k, carry):
        row = pl.ds(mo(share_of(k) * length, length), length)
        gq = gqkv[row, :]
        gu = gup[row, :]
        mu = stat[row, 0:1]
        inv = stat[row, 1:2]
        for j in range(s_n):
            col = slice(j * rs, (j + 1) * rs)
            d1 = dot(gq, wi[col, :], NT)
            d2 = dot(gu, wu[col, :], NT)
            xh = (x_all[row, col].astype(F32) - mu) * inv
            vacc[0, :, col] += jnp.sum(d1 * xh, axis=0, keepdims=True)
            vacc[1, :, col] += jnp.sum(d1, axis=0, keepdims=True)
            vacc[2, :, col] += jnp.sum(d2 * xh, axis=0, keepdims=True)
            vacc[3, :, col] += jnp.sum(d2, axis=0, keepdims=True)
            e = d1 * gain1[:, col] + d2 * gain2[:, col]
            esend[k, :, col] = e.astype(BF)
            eown[:, col] = e
        shares(k, *e_refs)
        return carry

    lax.fori_loop(0, 1, in_block, 0)
    pair_sum(UP, dwu, xru, zru, half)
    lax.fori_loop(1, 3, in_block, 0)
    pass_on(IN, xri, zri)
    lax.fori_loop(3, n, in_block, 0)

    line_sum(DOWN, xrd, zrd, fd)
    spread(DOWN)

    shares_on(*e_refs)

    slots = vfull.shape[0] // s_n
    vfull[...] = jnp.zeros_like(vfull)
    per = n_in // 128
    for i in range(3):
        for h in range(2):
            b = i * 2 * n + p + n * h
            col = slice(i * span + h * 128, i * span + (h + 1) * 128)
            vfull[lax.div(b, per) * slots + lax.rem(b, per)] = bin_r[:, col]
    at_g = per + 2 * n
    for q in range(s_n):
        for h in range(2):
            up_col = slice(q * hb + h * 128, q * hb + (h + 1) * 128)
            vfull[q * slots + per + 2 * p + h] = bup_r[:, up_col]
            col = slice(q * rs + h * 128, q * rs + (h + 1) * 128)
            g_own = g_all[pl.ds(mo(p * length, length), length), col].astype(F32)
            vfull[q * slots + at_g + h] = jnp.sum(g_own, axis=0, keepdims=True)
            for i in range(4):
                vfull[q * slots + at_g + 2 + 2 * i + h] = vacc[i, :, col]
    for i in range(1, s_n):
        q, dev = line(i)
        start(rc(vfull.at[pl.ds(q * slots, slots)], vz.at[zz], one_s.at[SUMS], one_r.at[1], dev))

    pass_on(UP, xru, zru)

    got(mrecv, m_r.at[2])

    def mixed_rows(i, carry):
        step = 32
        row = pl.ds(mo(i * step, step), step)
        xv = x_all[pl.ds(mo(p * length + i * step, step), step), :].astype(F32)
        t = mown[row, :] + mrecv[0, row, :].astype(F32) + mrecv[1, row, :].astype(F32)
        mixed_v[row, :] = (xv + t + out_b + down_b).astype(BF)
        return carry

    lax.fori_loop(0, length // 32, mixed_rows, 0)
    mixed_out = pltpu.make_async_copy(mixed_v, mixed_o, io.at[9])
    mixed_out.start()

    spread_relay(DOWN)
    line_sum(IN, xri, zri, fi)
    spread(IN)
    def o_got(ref, k, cond):
        @pl.when(cond)
        def _():
            got(ref, ag_r.at[OUT, k])

    o_got(o_whole(yn), 1, away)
    start(rc(o_whole(yn), o_whole(yn), ag_s.at[OUT], ag_r.at[OUT, 2], dev_x), away)
    line_sum(UP, xru, zru, fu)
    spread(UP)

    spread_relay(IN)

    spread_near(DOWN)
    spread_far(DOWN)
    total = [vfull[zz * slots + k] for k in range(slots)]
    got(vz.at[pl.ds(0, s_n - 1)], one_r.at[1])
    for i in range(1, s_n):
        q, dev = line(i)
        total = [t + vz[q, k] for k, t in enumerate(total)]
    for k in range(slots):
        vu[k] = total[k]
        vr[r, k] = total[k]
    for i in range(1, 2 * n):
        start(rc(vu, vr.at[r], one_s.at[TOTALS], one_r.at[2], (lax.rem(r + i, 2 * n), zz)))

    got(erecv, e_r.at[2])

    def tgrad_rows(i, carry):
        step = 32
        row = pl.ds(mo(i * step, step), step)
        far = pl.ds(mo(p * length + i * step, step), step)
        inv = stat[far, 1:2]
        xh = (x_all[far, :].astype(F32) - stat[far, 0:1]) * inv
        e = eown[row, :] + erecv[0, row, :].astype(F32) + erecv[1, row, :].astype(F32)
        m0 = jnp.mean(e, axis=1, keepdims=True)
        m1 = jnp.mean(e * xh, axis=1, keepdims=True)
        tgrad_v[row, :] = g_all[far, :].astype(F32) + inv * (e - m0 - xh * m1)
        return carry

    lax.fori_loop(0, length // 32, tgrad_rows, 0)
    tgrad_out = pltpu.make_async_copy(tgrad_v, tgrad_o, io.at[10])
    tgrad_out.start()

    spread_relay(UP)
    o_got(o_whole(xn), 0, at_home)
    start(rc(o_whole(xn), o_whole(xn), agc_s.at[OUT], agc_r.at[OUT], partner), at_home)
    start(rc(o_whole(yn), o_whole(yn), agc_s.at[OUT], agc_r.at[OUT], partner), away)
    o_got(o_whole(dg), 2, away)
    start(rc(o_whole(dg), o_whole(dg), agc_s.at[OUT], agc_r.at[OUT], partner), away)

    spread_near(UP)
    spread_near(IN)
    spread_far(IN)
    got(vr.at[pl.ds(0, 2 * n - 1)], one_r.at[2])
    for k in range(slots):
        t = vr[0, k]
        for q in range(1, 2 * n):
            t = t + vr[q, k]
        vec_v[k] = t
    vec_out = pltpu.make_async_copy(vec_v, vec_o, io.at[11])
    vec_out.start()
    spread_far(UP)
    for t in (DOWN, IN, UP):
        spread_end(t)
    two = wo.at[pl.ds(0, 2 * ohalf)]
    got(two, agc_r.at[OUT])

    for cond, cp in local_out:
        if cond is None:
            cp.wait()
        else:
            pl.when(cond)(cp.wait)
    for cp in (mixed_out, tgrad_out, vec_out):
        cp.wait()
    left(va.at[pl.ds(0, s_n - 1)], one_s.at[VECTORS])
    left(x_all.at[pl.ds(0, 3 * length)], one_s.at[TOKENS])
    left(g_all.at[pl.ds(0, 3 * length)], one_s.at[COTANGENTS])
    left(wo.at[pl.ds(0, 3 * ohalf)], one_s.at[ROWS], at_home)
    left(msend.at[pl.ds(0, 3)], one_s.at[OUTPUT])
    left(esend.at[pl.ds(0, 3)], one_s.at[INPUT])
    left(vz.at[pl.ds(0, s_n - 1)], one_s.at[SUMS])
    left(vr.at[pl.ds(0, 2 * n - 1)], one_s.at[TOTALS])
    for t in (IN, UP, DOWN):
        for h in range(cuts[t]):
            k = stream[t] + h
            left(pieces(t, 1), w_s.at[k], is_end)
            left(pieces(t, 5), w_s.at[k], inner)
            left(pieces(t, s_n - 1), wc_s.at[k])
    left(o_piece(0, 0), oc_s.at[0], away)
    left(o_piece(0, 0), oc_s.at[1])
    for t, xr in ((IN, xri), (UP, xru), (DOWN, xrd), (OUT, xro)):
        left(xr, xs_s.at[t])
    for t, xr in ((IN, xri), (UP, xru), (DOWN, xrd)):
        left(xr.at[pl.ds(0, 3)], zs_s.at[t])
        left(outs_of[t][0].at[pl.ds(0, 3), 0], ag_s.at[t])
        left(outs_of[t][0].at[:, 0], agc_s.at[t])
    left(xro.at[0], zo_s.at[0])
    left(xro.at[0], zo_s.at[1], away)
    left(two, ag_s.at[OUT], at_home)
    left(wo.at[pl.ds(0, ohalf)], ag_s.at[OUT], away)
    left(two, agc_s.at[OUT])


def fused_call(z, tok, cot, inp, upp, outp, downp, vectors):
    n, s_n, length, width, span, hid = z.n, z.s, z.l, z.d, z.span, z.hid
    rs, hb, rows = z.rs, z.hb, z.rows
    iw = 3 * span
    nv = sum(v.shape[0] for v in vectors)
    slots = (3 * width // s_n + hb * n + 5 * rs) // 128
    V = pltpu.VMEM
    dma = lambda *shape: pltpu.SemaphoreType.DMA(shape)
    share = [
        V((n, length, width), BF), V((2, length, width), BF), V((2, length // 2, width), BF),
        V((length, width), F32),
    ]
    halves = [
        V((s_n, rs // 2, iw), BF), V((s_n, rs // 2, hid), BF), V((s_n, hb // 2, width), BF),
    ]
    scratch = [
        *[V((rows, width), BF)] * 4,
        V((width, iw), BF), V((width, hid), BF), V((span, width), BF), V((hid, width), BF),
        V((rows, iw), BF), V((n * span // HEAD_DIM, length, length), F32),
        V((rows, hid), F32), V((rows, hid), BF), V((rows, span), BF),
        V((rows, span), BF), V((rows, hid), BF), V((rows, iw), BF),
        *share, *share,
        V((s_n, rs, iw), BF), V((s_n, rs, hid), BF), V((s_n, hb, width), BF), V((2, span // 2, width), BF),
        *halves, V((2, span // 4, width), BF),
        *halves, V((3, span // 4, width), BF),
        V((rs // 2, iw), BF), V((rs // 2, hid), BF), V((hb // 2, width), BF), V((span // 4, width), BF),
        V((1, nv), F32), V((s_n, 1, nv), F32), V((1, 3 * width), F32), V((s_n * slots, 1, 128), F32),
        V((s_n, slots, 1, 128), F32), V((slots, 1, 128), F32), V((2 * n, slots, 1, 128), F32),
        V((rows, 2), F32), V((4, 1, width), F32), V((1, iw), F32), V((1, hid), F32),
        dma(6), dma(12), dma(8), dma(3), dma(4), dma(4), dma(4), dma(4, s_n), dma(4), dma(4), dma(2), dma(2), dma(2),
        dma(3), dma(3), dma(4), dma(4), dma(3), dma(3, 3), dma(2), dma(2), dma(4), dma(4, 4), dma(4), dma(4), dma(4),
        V((3, length, 128), F32), V((length, width), BF), V((length, width), F32), V((slots, 1, 128), F32),
        *[V(v.shape, BF) for v in vectors],
    ]
    any_ = pl.BlockSpec(memory_space=pl.ANY)
    outs = [
        jax.ShapeDtypeStruct((length, width), BF),
        jax.ShapeDtypeStruct((length, width), F32),
        jax.ShapeDtypeStruct((n, 2, rs // 2, iw), BF),
        jax.ShapeDtypeStruct((n, 2, rs // 2, hid), BF),
        jax.ShapeDtypeStruct((n, 2, hb // 2, width), BF),
        jax.ShapeDtypeStruct((2, 2, span // 4, width), BF),
        jax.ShapeDtypeStruct((slots, 1, 128), F32),
    ]
    return pl.pallas_call(
        functools.partial(fused, z),
        out_shape=outs,
        in_specs=[any_] * 15,
        out_specs=[any_] * 7,
        scratch_shapes=scratch,
        compiler_params=pltpu.CompilerParams(
            collective_id=0, has_side_effects=True, vmem_limit_bytes=VMEM_LIMIT
        ),
        name="block_step",
    )(tok, cot, inp, upp, outp, downp, *vectors, jnp.asarray(rotary_lanes(length)))


def finish(z, *refs):
    mixed, tgrad, g_in, g_up, g_down, g_out, vec = refs[:7]
    mixed_o, tgrad_o, in_o, up_o, down_o, out_o = refs[7:13]
    vec_o = refs[13:21]
    m_v, t_v, v_v, bi, bu, bd, bo, fi, fu, fd, fo = refs[21:32]
    vec_v, (io, r_sem, w_sem) = refs[32:40], refs[40:]
    n, s_n, width, span, hb, rs = z.n, z.s, z.d, z.span, z.hb, z.rs
    half, hhalf, quarter = rs // 2, hb // 2, span // 4
    through = [
        (pltpu.make_async_copy(a, b, io.at[i]), pltpu.make_async_copy(b, o, io.at[3 + i]))
        for i, (a, b, o) in enumerate(((mixed, m_v, mixed_o), (tgrad, t_v, tgrad_o)))
    ]
    vec_in = pltpu.make_async_copy(vec, v_v, io.at[2])
    blocks = []
    for q in range(n):
        blocks.append((1, g_up.at[q], bu.at[q], fu.at[q], [
            (core, up_o.at[core * half : (core + 1) * half, (k * n + q) * hb : (k * n + q + 1) * hb], slice(k * hb, (k + 1) * hb))
            for core in range(2) for k in range(s_n)
        ]))
    for q in range(n):
        blocks.append((2, g_down.at[q], bd.at[q], fd.at[q], [
            (core, down_o.at[q * hb + core * hhalf : q * hb + (core + 1) * hhalf], slice(None)) for core in range(2)
        ]))
    for q in range(n):
        blocks.append((0, g_in.at[q], bi.at[q], fi.at[q], [
            (core, in_o.at[core * half : (core + 1) * half, k * width + (q + n * h) * 128 : k * width + (q + n * h + 1) * 128],
             slice(k * span + h * 128, k * span + (h + 1) * 128))
            for core in range(2) for k in range(3) for h in range(2)
        ]))
    for j in range(2):
        blocks.append((3, g_out.at[j], bo.at[j], fo.at[j], [
            (core, out_o.at[(2 * j + core) * quarter : (2 * j + core + 1) * quarter], slice(None)) for core in range(2)
        ]))
    reads = [pltpu.make_async_copy(src, dst, r_sem.at[i]) for i, (_, src, dst, _, _) in enumerate(blocks)]
    for cp in [reads[0], *(a for a, _ in through), vec_in, *reads[1:]]:
        cp.start()
    for (t, _, low, wide, places), read in zip(blocks, reads):
        read.wait()
        for core in range(2):

            def body(i, carry, core=core, low=low, wide=wide):
                row = pl.ds(mo(i * 32, 32), 32)
                wide[core, row, :] = low[core, row, :].astype(F32)
                return carry

            lax.fori_loop(0, low.shape[1] // 32, body, 0)
        for core, place, col in places:
            pltpu.make_async_copy(wide.at[core, :, col], place, w_sem.at[t]).start()
    for a, b in through:
        a.wait()
        b.start()
    vec_in.wait()
    k = 0
    small = []
    for i, (ref, out) in enumerate(zip(vec_v, vec_o)):
        count = ref.shape[0] // 128
        if i == 3:
            k -= count
        for j in range(count):
            ref[j * 128 : (j + 1) * 128] = v_v[k + j].reshape(128)
        k += count
        small.append(pltpu.make_async_copy(ref, out, io.at[5 + i]))
        small[-1].start()
    for t, wide in enumerate((fi, fu, fd, fo)):
        pltpu.make_async_copy(wide, wide, w_sem.at[t]).wait()
    for cp in [b for _, b in through] + small:
        cp.wait()


def finish_call(z, pieces):
    n, width, span, rs = z.n, z.d, z.span, z.rs
    V = pltpu.VMEM
    S = jax.ShapeDtypeStruct
    any_ = pl.BlockSpec(memory_space=pl.ANY)
    small = [3 * width // z.s, z.hb * n] + [rs] * 6
    outs = [
        S((z.l, width), BF), S((z.l, width), F32), S((rs, 3 * width), F32), S((rs, z.ff), F32),
        S((z.hb * n, width), F32), S((span, width), F32), *[S((k,), F32) for k in small],
    ]
    shapes = [p.shape for p in pieces[2:6]]
    dma = lambda k: pltpu.SemaphoreType.DMA((k,))
    return pl.pallas_call(
        functools.partial(finish, z),
        out_shape=outs,
        in_specs=[any_] * 7,
        out_specs=[any_] * 14,
        scratch_shapes=[
            V((z.l, width), BF), V((z.l, width), F32), V(pieces[6].shape, F32),
            *[V(s, BF) for s in shapes], *[V(s, F32) for s in shapes],
            *[V((k,), F32) for k in small],
            dma(13), dma(3 * n + 2), dma(4),
        ],
        compiler_params=pltpu.CompilerParams(vmem_limit_bytes=VMEM_LIMIT),
        name="finish",
    )(*pieces)


def make_fused_body(z):
    def body(
        tokens, in_proj, in_bias, out_proj, out_bias, up_proj, up_bias, down_proj, down_bias,
        first_gain, first_shift, second_gain, second_shift, cotangent,
    ):
        vectors = (in_bias, up_bias, out_bias, down_bias, first_gain, first_shift, second_gain, second_shift)
        pieces = fused_call(z, tokens, cotangent, in_proj, up_proj, out_proj, down_proj, vectors)
        mixed, tgrad, g_in, g_up, g_down, g_out, b_in, b_up, b_out, b_down, *rest = finish_call(
            z, pieces
        )
        return (mixed, tgrad, g_in, b_in, g_out, b_out, g_up, b_up, g_down, b_down, *rest)

    return body


def solution(mesh):
    rows = P(("rep", "shard"), None)
    mat = P("shard", None)
    vec = P("shard")
    in_specs = (rows, mat, vec, mat, vec, mat, vec, mat, vec, vec, vec, vec, vec, rows)
    out_specs = (rows, rows, mat, vec, mat, vec, mat, vec, mat, vec, vec, vec, vec, vec)
    shape = dict(mesh.shape)

    def step(*args):
        tokens, up_proj = args[0], args[5]
        devices = shape["rep"] * shape["shard"]
        z = Sizes(shape, tokens.shape[0] // devices, tokens.shape[1], up_proj.shape[1])
        body = make_fused_body(z) if z.fits() else make_body(shape["shard"])
        return jax.shard_map(
            body, mesh=mesh, in_specs=in_specs, out_specs=out_specs, check_vma=False
        )(*args)

    return step
```
